32 devices in a mesh: frames: 8 (over y, x, core), pix: 4 (over z).
Axes of the slice: x: 2, y: 2, z: 4, core: 2. Of those that a mesh axis runs over, the one named last changes fastest.
Arguments:
- edge_frames: int32 [2, 1536], P(None, 'frames'), may hold values from 0 to 127, as said below
- rotvec: float32 [3, 128], replicated, may hold values from -0.06 to 0.06
- trans: float32 [3, 128], replicated, may hold values from -0.15 to 0.15
- inv_depth: float32 [128, 3072], P('frames', 'pix'), may hold values from 0.2 to 1
- depth_damping: float32 [128, 3072], P('frames', 'pix'), may hold values from 0.01 to 0.1
- flow: float32 [1536, 2, 3072], P('frames', None, 'pix'), may hold values from -0.3 to 0.3
- weight: float32 [1536, 2, 3072], P('frames', None, 'pix'), may hold values from 0.02 to 1
- mask: int32 [1536, 3072], P('frames', 'pix'), may hold values 0 or 1
Outputs:
- pose_step: float32 [6, 128], P(None, 'frames')
- depth_step: float32 [128, 3072], P('frames', 'pix')
The draws below stay inside these ranges and needn't reach their ends.
Inputs may be any that keep to these rules, and one draw needn't show every extreme that they name: Edge e of the block of 192 edges held by one index of frames has its target edge_frames[1, e] among that index's 16 keyframes; its source edge_frames[0, e] differs from the target by 1 to 8, and in every block some source lies exactly 8 away.
All inputs are finite; a program needn't handle non-finite values. No bound on the sum of `mask` on one device may be relied on, other than what follows from the above.
Results may differ from the reference program's by a relative error of at most 0.00015.
Values sent between devices are 32-bit elements; how exact they have to be, the bound alone decides.
A program may use at most 64 MiB of HBM per device.

```python
import math
import jax
import jax.numpy as jnp
from jax import lax

F_DEV = 16
EDGE_DEV = 192
ROWS = 48
COLS = 64
RADIUS = 8
ITERS = 6
FRAMES = 128
EDGES = 1536
PIX = 3072


def draw_edge_frames(key, part):
    keys = jax.random.split(jax.random.fold_in(key, 11), 4)
    index = jnp.arange(EDGES, dtype=jnp.int32)
    block = index // EDGE_DEV
    slot = index % EDGE_DEV
    first = jax.random.randint(keys[0], (EDGES,), 0, F_DEV)
    second = jax.random.randint(keys[1], (EDGES,), 0, F_DEV)
    local = jnp.minimum(first, second)
    local = jnp.where(slot == 0, 0, jnp.where(slot == 1, F_DEV - 1, local))
    offset = jax.random.randint(keys[2], (EDGES,), 1, RADIUS + 1)
    offset = jnp.where(slot < 2, RADIUS, offset)
    sign = 2 * jax.random.randint(keys[3], (EDGES,), 0, 2) - 1
    sign = jnp.where(slot == 0, -1, jnp.where(slot == 1, 1, sign))
    target = block * F_DEV + local
    source = target + sign * offset
    source = jnp.where((source < 0) | (source >= FRAMES), target - sign * offset, source)
    return jnp.stack([source, target]).astype(jnp.int32)


def draw_flow(key, part):
    keys = jax.random.split(jax.random.fold_in(key, 23), 2)
    shared = jnp.clip(0.06 * jax.random.normal(keys[0], (EDGES, 2, 1), jnp.float32), -0.2, 0.2)
    noise = jnp.clip(0.03 * jax.random.normal(keys[1], (EDGES, 2, PIX), jnp.float32), -0.1, 0.1)
    return shared + noise


def touch_ends(drawn, stream_key, low, high):
    place = [jax.random.randint(jax.random.fold_in(stream_key, axis), (), 0, length) for axis, length in enumerate(drawn.shape)]
    main_axis = drawn.shape.index(max(drawn.shape))
    neighbour = place[:main_axis] + [(place[main_axis] + 1) % drawn.shape[main_axis]] + place[main_axis + 1:]
    return drawn.at[tuple(place)].set(low).at[tuple(neighbour)].set(high)


def shard_levels(rng, shape, cuts, least, largest):
    gain = 1.0
    for axis_at, parts in cuts:
        steps = jax.random.uniform(jax.random.fold_in(jax.random.fold_in(rng, 6), axis_at), (parts,), jnp.float32, least / len(cuts), largest / len(cuts))
        gain = gain * jnp.repeat(jnp.exp(steps), shape[axis_at] // parts).reshape((-1,) + (1,) * (len(shape) - 1 - axis_at))
    return gain


def setup_inputs(seed: int = 0) -> dict:
    key_list = jax.random.split(jax.random.key(seed), 9)
    return {
        "edge_frames": draw_edge_frames(jax.random.fold_in(key_list[8], 71), 0),
        "rotvec": jnp.clip(jax.random.uniform(key_list[1], (3, FRAMES), jnp.float32, -0.06, 0.06), -0.06, 0.06),
        "trans": jnp.clip(jax.random.uniform(key_list[2], (3, FRAMES), jnp.float32, -0.15, 0.15), -0.15, 0.15),
        "inv_depth": jnp.clip(jnp.exp(math.log(1.0) - 1.609438 * jax.random.uniform(key_list[3], (FRAMES, PIX), jnp.float32) ** shard_levels(key_list[3], (FRAMES, PIX), ((0, 8), (1, 4)), -0.2, 0.2)), 0.2, 1.0),
        "depth_damping": jnp.clip(jnp.exp(math.log(0.1) - 2.3025851 * jax.random.uniform(key_list[4], (FRAMES, PIX), jnp.float32) ** shard_levels(key_list[4], (FRAMES, PIX), ((0, 8), (1, 4)), -0.2, 0.2)), 0.01, 0.1),
        "flow": draw_flow(jax.random.fold_in(key_list[8], 71), 0),
        "weight": jnp.clip(jnp.exp(math.log(1.0) - 3.912023 * jax.random.uniform(key_list[6], (EDGES, 2, PIX), jnp.float32) ** shard_levels(key_list[6], (EDGES, 2, PIX), ((0, 8), (2, 4)), -0.2, 0.2)), 0.02, 1.0),
        "mask": touch_ends((jax.random.randint(key_list[7], (EDGES, PIX), 0, 4) < 3).astype(jnp.int32), jax.random.fold_in(key_list[7], 1), 0, 1),
    }


exact = lax.Precision.HIGHEST
pose_regularizer = 100.0


def pixel_coords(pixel):
    row = pixel // COLS
    column = pixel % COLS
    col_coord = (column.astype(jnp.float32) - 0.5 * (COLS - 1)) / COLS
    row_coord = (row.astype(jnp.float32) - 0.5 * (ROWS - 1)) / COLS
    return col_coord, row_coord


def rotations(rotvec):
    omega_x, omega_y, omega_z = rotvec[0], rotvec[1], rotvec[2]
    zero = jnp.zeros_like(omega_x)
    cross = [[zero, -omega_z, omega_y], [omega_z, zero, -omega_x], [-omega_y, omega_x, zero]]
    theta_sq = omega_x * omega_x + omega_y * omega_y + omega_z * omega_z
    first_coef = 1.0 - theta_sq / 6.0 + theta_sq * theta_sq / 120.0
    second_coef = 0.5 - theta_sq / 24.0 + theta_sq * theta_sq / 720.0
    lines = []
    for row in range(3):
        entries = []
        for column in range(3):
            square = cross[row][0] * cross[0][column] + cross[row][1] * cross[1][column] + cross[row][2] * cross[2][column]
            entries.append(float(row == column) + first_coef * cross[row][column] + second_coef * square)
        lines.append(jnp.stack(entries))
    return jnp.stack(lines)


def relative(rot, trans, source, target):
    rot_source = jnp.take(rot, source, axis=2)
    rot_target = jnp.take(rot, target, axis=2)
    rel_rot = jnp.einsum('ike,jke->ije', rot_target, rot_source, precision=exact)
    rel_trans = jnp.take(trans, target, axis=1) - jnp.einsum('ije,je->ie', rel_rot, jnp.take(trans, source, axis=1), precision=exact)
    zero = jnp.zeros_like(rel_trans[0])
    skew = jnp.stack([jnp.stack([zero, -rel_trans[2], rel_trans[1]]),
                      jnp.stack([rel_trans[2], zero, -rel_trans[0]]),
                      jnp.stack([-rel_trans[1], rel_trans[0], zero])])
    corner = jnp.einsum('ike,kje->ije', skew, rel_rot, precision=exact)
    upper = jnp.concatenate([rel_rot, corner], axis=1)
    lower = jnp.concatenate([jnp.zeros_like(rel_rot), rel_rot], axis=1)
    return rel_rot, rel_trans, jnp.concatenate([upper, lower], axis=0)


def geometry(rel_rot, rel_trans, depth, flow, weight, mask, col_coord, row_coord):
    def coordinate(line):
        return (rel_rot[line, 0][:, None] * col_coord + rel_rot[line, 1][:, None] * row_coord
                + rel_rot[line, 2][:, None] + depth * rel_trans[line][:, None])
    inverse_z = 1.0 / coordinate(2)
    proj_u = coordinate(0) * inverse_z
    proj_v = coordinate(1) * inverse_z
    depth_scale = depth * inverse_z
    slope_u = inverse_z * (rel_trans[0][:, None] - proj_u * rel_trans[2][:, None])
    slope_v = inverse_z * (rel_trans[1][:, None] - proj_v * rel_trans[2][:, None])
    live = mask.astype(jnp.float32)
    conf_u = weight[:, 0] * live
    conf_v = weight[:, 1] * live
    error_u = col_coord + flow[:, 0] - proj_u
    error_v = row_coord + flow[:, 1] - proj_v
    return proj_u, proj_v, depth_scale, slope_u, slope_v, conf_u, conf_v, error_u, error_v


def apply_pose(geo, motion):
    proj_u, proj_v, depth_scale = geo[0], geo[1], geo[2]
    part = [motion[index][:, None] for index in range(6)]
    cross_uv = proj_u * proj_v
    lin_u = depth_scale * (part[0] - proj_u * part[2]) - cross_uv * part[3] + (1.0 + proj_u * proj_u) * part[4] - proj_v * part[5]
    lin_v = depth_scale * (part[1] - proj_v * part[2]) - (1.0 + proj_v * proj_v) * part[3] + cross_uv * part[4] + proj_u * part[5]
    return lin_u, lin_v


def pose_terms(geo, part_u, part_v):
    proj_u, proj_v, depth_scale = geo[0], geo[1], geo[2]
    heavy_u = geo[5] * part_u
    heavy_v = geo[6] * part_v
    cross_uv = proj_u * proj_v
    entries = [depth_scale * heavy_u, depth_scale * heavy_v,
               -depth_scale * (proj_u * heavy_u + proj_v * heavy_v),
               -cross_uv * heavy_u - (1.0 + proj_v * proj_v) * heavy_v,
               (1.0 + proj_u * proj_u) * heavy_u + cross_uv * heavy_v,
               -proj_v * heavy_u + proj_u * heavy_v]
    return jnp.stack([jnp.sum(entry, axis=1) for entry in entries])


def spread(motion, source, target, adjoint):
    return jnp.take(motion, target, axis=1) - jnp.einsum('jke,ke->je', adjoint, jnp.take(motion, source, axis=1), precision=exact)


def reference(edge_frames, rotvec, trans, inv_depth, depth_damping, flow, weight, mask):
    col_coord, row_coord = pixel_coords(jnp.arange(PIX, dtype=jnp.int32))
    rot = rotations(rotvec)
    blocks = EDGES // EDGE_DEV
    packed = (edge_frames[0].reshape(blocks, EDGE_DEV), edge_frames[1].reshape(blocks, EDGE_DEV),
              flow.reshape(blocks, EDGE_DEV, 2, PIX), weight.reshape(blocks, EDGE_DEV, 2, PIX),
              mask.reshape(blocks, EDGE_DEV, PIX))

    def sweep(update, init):
        def advance(carry, item):
            source, target, flow_block, weight_block, mask_block = item
            rel_rot, rel_trans, adjoint = relative(rot, trans, source, target)
            geo = geometry(rel_rot, rel_trans, jnp.take(inv_depth, source, axis=0), flow_block,
                           weight_block, mask_block, col_coord, row_coord)
            return update(carry, source, target, adjoint, geo), None
        return lax.scan(advance, init, packed)[0]

    def totals_update(carry, source, target, adjoint, geo):
        terms = jnp.stack([geo[5] * geo[3] * geo[3] + geo[6] * geo[4] * geo[4],
                           -(geo[3] * geo[5] * geo[7] + geo[4] * geo[6] * geo[8])])
        return carry.at[:, source].add(terms)

    totals = sweep(totals_update, jnp.zeros((2, FRAMES, PIX), jnp.float32))
    curvature = totals[0] + depth_damping
    base_step = totals[1] / curvature

    def pose_sweep(motion, image):
        def update(carry, source, target, adjoint, geo):
            at_source = jnp.take(image, source, axis=0)
            if motion is None:
                part_u = -geo[7] - geo[3] * at_source
                part_v = -geo[8] - geo[4] * at_source
            else:
                lin_u, lin_v = apply_pose(geo, spread(motion, source, target, adjoint))
                part_u = lin_u - geo[3] * at_source
                part_v = lin_v - geo[4] * at_source
            target_terms = pose_terms(geo, part_u, part_v)
            source_terms = -jnp.einsum('jke,je->ke', adjoint, target_terms, precision=exact)
            return carry.at[:, target].add(target_terms).at[:, source].add(source_terms)
        return sweep(update, jnp.zeros((6, FRAMES), jnp.float32))

    def depth_sweep(motion):
        def update(carry, source, target, adjoint, geo):
            lin_u, lin_v = apply_pose(geo, spread(motion, source, target, adjoint))
            return carry.at[source].add(geo[3] * geo[5] * lin_u + geo[4] * geo[6] * lin_v)
        return sweep(update, jnp.zeros((FRAMES, PIX), jnp.float32))

    def reduced(motion):
        image = depth_sweep(motion) / curvature
        return pose_sweep(motion, image) + pose_regularizer * motion

    rhs = pose_sweep(None, base_step)
    solution = jnp.zeros_like(rhs)
    residual = rhs
    direction = rhs
    norm_now = jnp.sum(residual * residual)
    for step in range(ITERS):
        product = reduced(direction)
        alpha = norm_now / jnp.sum(direction * product)
        solution = solution + alpha * direction
        residual = residual - alpha * product
        norm_next = jnp.sum(residual * residual)
        direction = residual + (norm_next / norm_now) * direction
        norm_now = norm_next
    depth_step = base_step - depth_sweep(solution) / curvature
    return solution, depth_step
```

```python
import functools
import jax
import jax.numpy as jnp
from jax import lax
from jax.experimental import pallas as pl
from jax.experimental.pallas import tpu as pltpu
from jax.sharding import PartitionSpec as P

ROWS = 48
COLS = 64
RADIUS = 8
ITERS = 6
REG = 100.0
F32 = jnp.float32
BF16 = jnp.bfloat16
L = 128
WIN = 32
SLOT = 24
BAND = 2 * RADIUS
PACKED = 160
VMEM_LIMIT = 60 * 1024 * 1024
UPPER = [(i, j) for i in range(6) for j in range(i, 6) if (i, j) != (0, 1)]


def split(x):
    high = x.astype(BF16)
    return high, (x - high.astype(F32)).astype(BF16)


def iota(shape, dim):
    return lax.broadcasted_iota(jnp.int32, shape, dim)


def destinations(edge_ref, own_rows, side, f_dev, me):
    start = me * f_dev
    source = edge_ref[0:1, :] - start + RADIUS
    target = edge_ref[1:2, :] - start + RADIUS
    s = source - RADIUS
    mine = s * SLOT + target - jnp.where(s >= RADIUS, RADIUS, 0)
    q = target - RADIUS
    tile = jnp.where(source <= 3, source, jnp.where(source == 7, 4, 6 - source))
    line = jnp.where((source > 3) & (source < 7), q + 7 - source, q)
    lowest = own_rows + tile * 8 + line
    i = source - f_dev - RADIUS
    q = target - f_dev
    tile = jnp.where(i == 0, 4, jnp.where(i <= 4, i - 1, 7 - i))
    line = jnp.where(i > 4, q - i, q)
    highest = own_rows + side + tile * 8 + line
    return jnp.where(source < RADIUS, lowest, jnp.where(source >= RADIUS + f_dev, highest, mine))


def fetch(flow_ref, weight_ref, mask_ref, flow3, weight3, mask3, sems):
    out = []
    for tile in range(flow3.shape[0]):
        cols = pl.ds(tile * L, L)
        pairs = [(mask_ref.at[:, cols], mask3.at[tile])]
        for comp in range(2):
            pairs.append((weight_ref.at[:, comp, cols], weight3.at[tile, comp]))
            pairs.append((flow_ref.at[:, comp, cols], flow3.at[tile, comp]))
        copies = [pltpu.make_async_copy(a, b, sems.at[tile, n]) for n, (a, b) in enumerate(pairs)]
        for copy in copies:
            copy.start()
        out.append(copies)
    return out


def aggregate(edge_ref, loads, flow3, weight3, mask3, own_ref, low_ref, high_ref, me, f_dev):
    edges = edge_ref.shape[1]
    own = own_ref.shape[1]
    side = low_ref.shape[1]
    rows = own + 2 * side
    dest = destinations(edge_ref, own, side, f_dev, me)
    pick = (iota((rows, edges), 0) == dest).astype(F32).astype(BF16)
    for tile, copies in enumerate(loads):
        cols = slice(tile * L, (tile + 1) * L)
        for copy in copies:
            copy.wait()
        live = mask3[tile].astype(F32)
        fields = []
        for comp in range(2):
            conf = weight3[tile, comp] * live
            fields += [conf, conf * flow3[tile, comp]]
        high, low = split(jnp.concatenate(fields, axis=1))
        out = jnp.dot(pick, high, preferred_element_type=F32) + jnp.dot(
            pick, low, preferred_element_type=F32
        )
        for field in range(4):
            part = out[:, field * L : (field + 1) * L]
            own_ref[field, :, cols] = part[:own]
            low_ref[field, :, cols] = part[own : own + side]
            high_ref[field, :, cols] = part[own + side :]


def window(load, me, f_dev, frames):
    tiles = frames // L
    first = lax.rem(me * f_dev - RADIUS + frames, frames)
    tile = first // L
    back = lax.rem(L - lax.rem(first, L), L)
    near = pltpu.roll(load(pl.ds(pl.multiple_of(tile * L, L), L)), back, 1)
    if tiles == 1:
        return near
    after = lax.rem(tile + 1, tiles)
    far = pltpu.roll(load(pl.ds(pl.multiple_of(after * L, L), L)), back, 1)
    return jnp.where(iota(near.shape, 1) + lax.rem(first, L) < L, near, far)


def spread_rows(x):
    return jnp.concatenate([x, jnp.zeros((L - x.shape[0], L), F32)], axis=0).T


def jac_sums(u, v, uu, vv, uv, ds, a, b):
    return [
        ds * a,
        ds * b,
        -ds * (u * a + v * b),
        -uv * a - vv * b,
        uu * a + uv * b,
        u * b - v * a,
    ]


def adj_t(rel, cor, vec):
    out = []
    for j in range(3):
        out.append(rel[j] * vec[0] + rel[3 + j] * vec[1] + rel[6 + j] * vec[2])
    for j in range(3):
        out.append(
            cor[j] * vec[0]
            + cor[3 + j] * vec[1]
            + cor[6 + j] * vec[2]
            + rel[j] * vec[3]
            + rel[3 + j] * vec[4]
            + rel[6 + j] * vec[5]
        )
    return out


def build(
    first, pose_ref, own_ref, low_ref, high_ref, depth_ref, damp_ref,
    matrix_ref, zh_ref, zl_ref, base_ref, scale_ref,
    frame_ref, pair_ref, hacc, racc, hc, rc, adc, wide, depth3, damp3,
):
    f_dev, pix = depth_ref.shape
    tiles = pix // L
    half = f_dev // 2
    ox, oy, oz = pose_ref[0], pose_ref[1], pose_ref[2]
    zero = jnp.zeros_like(ox)
    cross = [[zero, -oz, oy], [oz, zero, -ox], [-oy, ox, zero]]
    sq = ox * ox + oy * oy + oz * oz
    c1 = 1.0 - sq / 6.0 + sq * sq / 120.0
    c2 = 0.5 - sq / 24.0 + sq * sq / 720.0
    for r in range(3):
        for c in range(3):
            square = cross[r][0] * cross[0][c] + cross[r][1] * cross[1][c] + cross[r][2] * cross[2][c]
            frame_ref[3 * r + c] = float(r == c) + c1 * cross[r][c] + c2 * square
        frame_ref[9 + r] = pose_ref[3 + r]
    for tile in range(tiles):
        depth3[tile] = depth_ref[:, tile * L : (tile + 1) * L]
        damp3[tile] = damp_ref[:, tile * L : (tile + 1) * L]
    hc[...] = jnp.zeros_like(hc)
    rc[...] = jnp.zeros_like(rc)
    adc[...] = jnp.zeros_like(adc)
    lane = iota((SLOT, L), 1)
    row = iota((SLOT, L), 0)
    row8 = iota((8, L), 0)

    for part in range(2):
        base = part * half
        win = slice(base, base + SLOT)
        if part == 0:
            pad = lambda x: jnp.concatenate([x, jnp.zeros((WIN - SLOT, L), F32)], axis=0)
        else:
            pad = lambda x: jnp.concatenate([jnp.zeros((WIN - SLOT, L), F32), x], axis=0)

        @pl.loop(0, half)
        def per_source(i):
            s = i + base
            here = [frame_ref[k, pl.ds(s + RADIUS, 1), :] for k in range(12)]
            there = [frame_ref[k, win, :] for k in range(12)]
            rel = [
                there[3 * r] * here[3 * c]
                + there[3 * r + 1] * here[3 * c + 1]
                + there[3 * r + 2] * here[3 * c + 2]
                for r in range(3)
                for c in range(3)
            ]
            tr = [
                there[9 + r]
                - (rel[3 * r] * here[9] + rel[3 * r + 1] * here[10] + rel[3 * r + 2] * here[11])
                for r in range(3)
            ]
            cor = []
            for c in range(3):
                cor.append(tr[1] * rel[6 + c] - tr[2] * rel[3 + c])
            for c in range(3):
                cor.append(tr[2] * rel[c] - tr[0] * rel[6 + c])
            for c in range(3):
                cor.append(tr[0] * rel[3 + c] - tr[1] * rel[c])
            at = lane == s + RADIUS
            for k in range(9):
                pair_ref[k] = rel[k]
                pair_ref[12 + k] = cor[k]
                adc[k, win, :] = jnp.where(at, rel[k], adc[k, win, :])
                adc[9 + k, win, :] = jnp.where(at, cor[k], adc[9 + k, win, :])
            for k in range(3):
                pair_ref[9 + k] = tr[k]
            hacc[...] = jnp.zeros_like(hacc)
            racc[...] = jnp.zeros_like(racc)
            if part == 0:
                slot = jnp.where(i == 0, 4, jnp.where(i <= 4, i - 1, 7 - i))
                shift = jnp.where(i > 4, i, 0)
                keep = row8 >= i
            else:
                slot = jnp.where(i <= 3, i, jnp.where(i == 7, 4, 6 - i))
                shift = jnp.where((i > 3) & (i < 7), i + 1, 0)
                keep = row8 <= i
            is_source = row == s + RADIUS - base

            def per_tile(tile):
                cols = slice(tile * L, (tile + 1) * L)
                fields = []
                for k in range(4):
                    src = high_ref if part == 0 else low_ref
                    got = src[k, pl.ds(pl.multiple_of(slot * 8, 8), 8), cols]
                    got = jnp.where(keep, pltpu.roll(got, shift, 0), 0.0)
                    if part == 0:
                        mine = own_ref[k, pl.ds(pl.multiple_of(s * SLOT + 8, 8), 16), cols]
                        fields.append(jnp.concatenate([got, mine], axis=0))
                    else:
                        mine = own_ref[k, pl.ds(pl.multiple_of(s * SLOT, 8), 16), cols]
                        fields.append(jnp.concatenate([mine, got], axis=0))
                wu, fu, wv, fv = fields
                pixel = first + tile * L + iota((1, L), 1)
                prow = pixel // COLS
                pcol = pixel - prow * COLS
                col = (pcol.astype(F32) - 0.5 * (COLS - 1)) / COLS
                rowc = (prow.astype(F32) - 0.5 * (ROWS - 1)) / COLS
                depth = depth3[tile, pl.ds(s, 1), :]
                m = [pair_ref[k] for k in range(21)]
                point = [
                    m[3 * k] * col + m[3 * k + 1] * rowc + m[3 * k + 2] + depth * m[9 + k]
                    for k in range(3)
                ]
                iz = 1.0 / point[2]
                u = point[0] * iz
                v = point[1] * iz
                ds = depth * iz
                su = iz * (m[9] - u * m[11])
                sv = iz * (m[10] - v * m[11])
                au = wu * su
                av = wv * sv
                gu = wu * (col - u) + fu
                gv = wv * (rowc - v) + fv
                curv = jnp.sum(au * su + av * sv, axis=0, keepdims=True) + damp3[tile, pl.ds(s, 1), :]
                grad = -jnp.sum(su * gu + sv * gv, axis=0, keepdims=True)
                bstep = grad / curv
                scale = 1.0 / jnp.sqrt(curv)
                base_ref[tile, pl.ds(s, 1), :] = bstep
                scale_ref[tile, pl.ds(s, 1), :] = scale
                uu = 1.0 + u * u
                vv = 1.0 + v * v
                uv = u * v
                e = jac_sums(u, v, uu, vv, uv, ds, au, av)
                back = adj_t(m[0:9], m[12:21], e)
                zcols = pl.ds(pl.multiple_of(s * pix + tile * L, L), L)
                for j in range(6):
                    total = -jnp.sum(back[j], axis=0, keepdims=True)
                    full = jnp.where(is_source, total, e[j]) * scale
                    high, low = split(pad(full))
                    zh_ref[j * WIN : (j + 1) * WIN, zcols] = high
                    zl_ref[j * WIN : (j + 1) * WIN, zcols] = low
                r = jac_sums(u, v, uu, vv, uv, ds, -gu - au * bstep, -gv - av * bstep)
                for j in range(6):
                    racc[j] += r[j]
                ju = [ds, None, -ds * u, -uv, uu, -v]
                jv = [None, ds, -ds * v, -vv, uv, u]
                wju = [None if x is None else wu * x for x in ju]
                wjv = [None if x is None else wv * x for x in jv]
                for n, (a, b) in enumerate(UPPER):
                    terms = []
                    if ju[a] is not None and ju[b] is not None:
                        terms.append(wju[a] * ju[b])
                    if jv[a] is not None and jv[b] is not None:
                        terms.append(wjv[a] * jv[b])
                    hacc[n] += terms[0] if len(terms) == 1 else terms[0] + terms[1]

            for tile in range(tiles):
                per_tile(tile)
            for n in range(len(UPPER)):
                hc[n, win, :] = jnp.where(at, jnp.sum(hacc[n], axis=1, keepdims=True), hc[n, win, :])
            for j in range(6):
                rc[j, win, :] = jnp.where(at, jnp.sum(racc[j], axis=1, keepdims=True), rc[j, win, :])

    def accumulate(s, carry):
        hh, hl = carry
        cols = pl.ds(pl.multiple_of(s * pix, L), pix)
        zh = zh_ref[:, cols]
        zl = zl_ref[:, cols]
        nt = (((1,), (1,)), ((), ()))
        return (
            hh + lax.dot_general(zh, zh, nt, preferred_element_type=F32),
            hl + lax.dot_general(zh, zl, nt, preferred_element_type=F32),
        )

    none = jnp.zeros((6 * WIN, 6 * WIN), F32)
    hh, hl = lax.fori_loop(0, f_dev, accumulate, (none, none))

    h = [[None] * 6 for _ in range(6)]
    for n, (a, b) in enumerate(UPPER):
        h[a][b] = hc[n]
        h[b][a] = h[a][b]
    rel = [adc[k] for k in range(9)]
    cor = [adc[9 + k] for k in range(9)]
    ad = [[None] * 6 for _ in range(6)]
    for i in range(3):
        for j in range(3):
            ad[i][j] = rel[3 * i + j]
            ad[i][3 + j] = cor[3 * i + j]
            ad[3 + i][3 + j] = rel[3 * i + j]
    lane = iota((WIN, L), 1)
    row = iota((WIN, L), 0)
    eye = row == lane

    def total(terms):
        out = None
        for x, y in terms:
            if x is None or y is None:
                continue
            out = x * y if out is None else out + x * y
        return out

    had = [[total([(h[i][k], ad[k][j]) for k in range(6)]) for j in range(6)] for i in range(6)]
    wide[...] = jnp.zeros_like(wide)
    matrix_ref[...] = jnp.zeros_like(matrix_ref)
    for i in range(6):
        rows = slice(i * WIN, (i + 1) * WIN)
        for j in range(6):
            cols = slice(j * WIN, (j + 1) * WIN)
            wide[rows, cols] = -had[i][j][:, :WIN]
            both = jnp.sum(total([(ad[k][i], had[k][j]) for k in range(6)]), axis=0, keepdims=True)
            if h[i][j] is not None:
                both = both + jnp.sum(h[i][j], axis=1, keepdims=True)
            diag = jnp.where(eye, both, 0.0)
            matrix_ref[rows, cols] = diag[:, :WIN]
    wide[: 6 * WIN, : 6 * WIN] = wide[: 6 * WIN, : 6 * WIN] - hl
    flipped = wide[...].T
    matrix_ref[: 6 * WIN, : 6 * WIN] = (
        matrix_ref[: 6 * WIN, : 6 * WIN] - hh + wide[: 6 * WIN, : 6 * WIN] + flipped[: 6 * WIN, : 6 * WIN]
    )
    r = [rc[j] for j in range(6)]
    back = adj_t(rel, cor, r)
    for j in range(6):
        here = jnp.sum(jnp.where(eye, jnp.sum(r[j], axis=1, keepdims=True), 0.0) - back[j], axis=0, keepdims=True)
        matrix_ref[6 * WIN : 6 * WIN + 1, j * WIN : (j + 1) * WIN] = here[:, :WIN]


def remote(src, dst, sems, phase, which, axis, peer):
    return pltpu.make_async_remote_copy(
        src_ref=src,
        dst_ref=dst,
        send_sem=sems.at[0, phase, which],
        recv_sem=sems.at[1, phase, which],
        device_id={axis: peer},
        device_id_type=pl.DeviceIdType.MESH,
    )


def peers(axis):
    count = lax.axis_size(axis)
    me = lax.axis_index(axis)
    return [lax.rem(me + step, count) for step in range(1, count)]


def pack(matrix_ref, packed_ref):
    size = 6 * WIN
    lane = iota((WIN, L), 1) % WIN
    row = iota((WIN, L), 0)
    inside = row + lane < WIN
    left = iota((BAND, L), 1) < L // 2
    packed_ref[...] = jnp.zeros_like(packed_ref)

    def skew(x):
        for bit in (1, 2, 4, 8, 16):
            x = jnp.where((lane & bit) != 0, pltpu.roll(x, WIN - bit, 0), x)
        return jnp.where(inside, x, 0.0)

    rest = []
    for j in range(6):
        rows = slice(j * WIN, (j + 1) * WIN)
        main = skew(matrix_ref[rows, :L])
        packed_ref[j * BAND : (j + 1) * BAND, :] = main[:BAND]
        packed_ref[6 * BAND + j : 6 * BAND + j + 1, :] = main[BAND : BAND + 1]
        rest.append(skew(matrix_ref[rows, L:]))
    base = 6 * BAND + 8
    for j in range(3):
        near = rest[j]
        far = pltpu.roll(rest[j + 3], L // 2, 1)
        packed_ref[base + j * BAND : base + (j + 1) * BAND, :] = jnp.where(left, near[:BAND], far[:BAND])
        at = base + 3 * BAND + j
        packed_ref[at : at + 1, :] = jnp.where(left[:1], near[BAND : BAND + 1], far[BAND : BAND + 1])
    packed_ref[6 * BAND + 6 : 6 * BAND + 7, :] = matrix_ref[size : size + 1, :L]
    packed_ref[base + 3 * BAND + 3 : base + 3 * BAND + 4, :] = jnp.where(
        left[:1], matrix_ref[size : size + 1, L:], 0.0
    )


def exchange(src, dst, sems, phase, axis):
    sent = []
    for peer in peers(axis):
        copy = remote(src(peer), dst, sems, phase, len(sent), axis, peer)
        copy.start()
        sent.append(copy)
    return sent


def operator(packed_ref, land, reduced_ref, gathered, diag_ref, ahead_ref, back_ref, far_ref, pix_sem, round_sem, f_dev, frames):
    zcount = lax.axis_size("pix")
    z = lax.axis_index("pix")
    count = lax.axis_size("frames")
    me = lax.axis_index("frames")
    chunk = land.shape[1]
    tiles = frames // L

    def piece(which):
        return pl.ds(pl.multiple_of(which * chunk, 8), chunk)

    sent = exchange(lambda peer: packed_ref.at[piece(peer)], land.at[z], pix_sem, 0, "pix")
    land[z] = packed_ref[piece(z), :]
    for copy in sent:
        copy.wait_recv()
    total = land[0]
    for k in range(1, zcount):
        total = total + land[k]
    reduced_ref[...] = total
    more = exchange(lambda peer: reduced_ref, gathered.at[me], round_sem, 0, "frames")
    gathered[me] = total
    for copy in more:
        copy.wait_recv()
    lane = iota((chunk, L), 1)
    sums = [[None] * tiles for _ in range(4)]
    for w in range(count):
        first = (w * f_dev - RADIUS) % frames
        start = first % L
        for k in range(4):
            part = pltpu.roll(gathered[w], (start - WIN * k) % L, 1)
            spans = [(first // L, start, min(start + WIN, L))]
            if start + WIN > L:
                spans.append(((first // L + 1) % tiles, 0, start + WIN - L))
            for tile, low, high in spans:
                term = jnp.where((lane >= low) & (lane < high), part, 0.0)
                sums[k][tile] = term if sums[k][tile] is None else sums[k][tile] + term
    for k in range(4):
        for tile in range(tiles):
            diag_ref[z, k, :, tile * L : (tile + 1) * L] = sums[k][tile]
    for copy in sent + more:
        copy.wait_send()
    sent = exchange(lambda peer: diag_ref.at[z], diag_ref.at[z], pix_sem, 1, "pix")
    for copy in sent:
        copy.wait_recv()
    for copy in sent:
        copy.wait_send()

    def block(k, at):
        return [
            diag_ref[at // chunk, k, at % chunk : at % chunk + 8, t * L : (t + 1) * L]
            for t in range(tiles)
        ]

    def entry(i, j, half):
        if i < 4:
            return block(i, BAND * j + 8 * half)
        return block(i - 4 + 2 * (j // 3), 6 * BAND + 8 + BAND * (j % 3) + 8 * half)

    row = iota((8, L), 0)
    lanes = iota((8, L), 1)

    def later(x, half):
        turned = [pltpu.roll(v, 8 * half, 1, stride=1, stride_axis=0) for v in x]
        if tiles == 1:
            return turned
        mine = lanes >= 8 * half + row
        return [jnp.where(mine, turned[t], turned[t - 1]) for t in range(tiles)]

    def flip(x):
        for bit in (4, 2, 1):
            x = jnp.where((row & bit) != 0, pltpu.roll(x, bit, 0), pltpu.roll(x, 8 - bit, 0))
        return x

    for i in range(6):
        for j in range(6):
            for half in range(2):
                front = entry(i, j, half)
                moved = later(entry(j, i, half), half)
                for t in range(tiles):
                    ahead_ref[i, 2 * j + half, :, t * L : (t + 1) * L] = flip(front[t])
                    value = jnp.where(row > 0, moved[t], 0.0) if half == 0 else moved[t]
                    back_ref[i, 2 * j + half, :, t * L : (t + 1) * L] = value
    edge = 6 * BAND
    last = edge + 8 + 3 * BAND
    for i in range(6):
        if i < 4:
            ends = block(i, edge)
        else:
            near, far = block(i - 4, last), block(i - 2, last)
            ends = [jnp.where(row < 3, a, pltpu.roll(b, 3, 0)) for a, b in zip(near, far)]
        for t in range(tiles):
            far_ref[i, :, t * L : (t + 1) * L] = jnp.where(row < 6, ends[t], 0.0)
    sources = [block(k, edge) for k in range(4)] + [block(k, last) for k in range(2)]
    rhs = []
    for t in range(tiles):
        out = jnp.zeros((8, L), F32)
        for i in range(6):
            at = 6 if i < 4 else 3
            out = jnp.where(row == i, sources[i][t][at : at + 1, :], out)
        rhs.append(out)
    return rhs, later


def conjugate(rhs, later, ahead_ref, back_ref, far_ref):
    tiles = len(rhs)
    row = iota((8, L), 0)
    lanes = iota((8, L), 1)

    def sooner(x, half):
        turned = [pltpu.roll(v, L - 8 * half - 7, 1, stride=1, stride_axis=0) for v in x]
        if tiles == 1:
            return turned
        mine = lanes + 8 * half + 7 - row < L
        return [jnp.where(mine, turned[t], turned[(t + 1) % tiles]) for t in range(tiles)]

    def moved(x, steps):
        turned = [pltpu.roll(v, steps % L, 1) for v in x]
        if tiles == 1:
            return turned
        if steps > 0:
            return [jnp.where(lanes >= steps, turned[t], turned[t - 1]) for t in range(tiles)]
        return [jnp.where(lanes < L + steps, turned[t], turned[(t + 1) % tiles]) for t in range(tiles)]

    def dot(x, y):
        total = x[0] * y[0]
        for t in range(1, tiles):
            total = total + x[t] * y[t]
        return jnp.sum(total, keepdims=True)

    def product(p):
        ahead = moved(p, -BAND)
        acc = [[far_ref[i, :, t * L : (t + 1) * L] * ahead[t] for t in range(tiles)] for i in range(6)]
        tail = [None] * tiles
        for j in range(6):
            wide = [jnp.broadcast_to(v[j : j + 1, :], (8, L)) for v in p]
            for t in range(tiles):
                term = far_ref[j, :, t * L : (t + 1) * L] * wide[t]
                tail[t] = term if tail[t] is None else tail[t] + term
            for half in range(2):
                plus = sooner(wide, half)
                minus = later(wide, half)
                for i in range(6):
                    for t in range(tiles):
                        acc[i][t] = (
                            acc[i][t]
                            + ahead_ref[i, 2 * j + half, :, t * L : (t + 1) * L] * plus[t]
                            + back_ref[i, 2 * j + half, :, t * L : (t + 1) * L] * minus[t]
                        )
        tail = moved(tail, BAND)
        out = []
        for t in range(tiles):
            y = tail[t] + REG * p[t]
            for i in range(6):
                y = y + jnp.where(row == i, jnp.sum(acc[i][t], axis=0, keepdims=True), 0.0)
            out.append(y)
        return out

    def step(_, carry):
        x, residual, direction, rr = carry
        image = product(direction)
        alpha = rr / dot(direction, image)
        x = [a + alpha * b for a, b in zip(x, direction)]
        residual = [a - alpha * b for a, b in zip(residual, image)]
        new = dot(residual, residual)
        beta = new / rr
        direction = [a + beta * b for a, b in zip(residual, direction)]
        return x, residual, direction, new

    zero = [jnp.zeros((8, L), F32)] * tiles
    return lax.fori_loop(0, ITERS, step, (zero, rhs, rhs, dot(rhs, rhs)))[0]


def finish(
    matrix_ref, zh_ref, zl_ref, base_ref, scale_ref, pose_ref, step_ref, frames,
    cols_ref, step3, packed_ref, land, reduced_ref, gathered, diag_ref, ahead_ref, back_ref, far_ref, x_ref,
    pix_sem, round_sem,
):
    me = lax.axis_index("frames")
    f_dev, pix = step_ref.shape
    pack(matrix_ref, packed_ref)
    rhs, later = operator(
        packed_ref, land, reduced_ref, gathered, diag_ref, ahead_ref, back_ref, far_ref,
        pix_sem, round_sem, f_dev, frames,
    )
    x = conjugate(rhs, later, ahead_ref, back_ref, far_ref)
    for t, value in enumerate(x):
        x_ref[:, t * L : (t + 1) * L] = value
    mine = window(lambda at: x_ref[:, at], me, f_dev, frames)
    pose_ref[...] = mine[:6, RADIUS : RADIUS + f_dev]
    turned = spread_rows(mine)
    for i in range(6):
        cols_ref[i * WIN : (i + 1) * WIN, :] = jnp.broadcast_to(turned[:WIN, i : i + 1], (WIN, L))

    @pl.loop(0, f_dev)
    def per_source(s):
        for tile in range(pix // L):
            zcols = pl.ds(pl.multiple_of(s * pix + tile * L, L), L)
            z = zh_ref[:, zcols].astype(F32) + zl_ref[:, zcols].astype(F32)
            image = jnp.sum(z * cols_ref[...], axis=0, keepdims=True)
            here = (tile, pl.ds(s, 1), slice(None))
            step3[here] = base_ref[here] - scale_ref[here] * image

    for tile in range(pix // L):
        step_ref[:, tile * L : (tile + 1) * L] = step3[tile]


def swap_edges(low_out, high_out, low_ref, high_ref, sems):
    count = lax.axis_size("frames")
    me = lax.axis_index("frames")
    down = remote(low_out, low_ref, sems, 0, 0, "frames", lax.rem(me + count - 1, count))
    up = remote(high_out, high_ref, sems, 1, 0, "frames", lax.rem(me + 1, count))

    @pl.when(me > 0)
    def _():
        down.start()

    @pl.when(me < count - 1)
    def _():
        up.start()

    def receive():
        @pl.when(me < count - 1)
        def _():
            down.wait_recv()

        @pl.when(me == count - 1)
        def _():
            low_ref[...] = jnp.zeros_like(low_ref)

        @pl.when(me > 0)
        def _():
            up.wait_recv()

        @pl.when(me == 0)
        def _():
            high_ref[...] = jnp.zeros_like(high_ref)

    def drain():
        @pl.when(me > 0)
        def _():
            down.wait_send()

        @pl.when(me < count - 1)
        def _():
            up.wait_send()

    return receive, drain


def solve(
    edge_ref, rot_ref, trans_ref, depth_ref, damp_ref, flow_ref, weight_ref, mask_ref,
    x_ref, step_ref, flow3, weight3, mask3, load_sem, pose_ref,
    own_ref, low_out, high_out, low_ref, high_ref, edge_sem, *scratch,
):
    matrix, zh, zl, base, scale = scratch[:5]
    me = lax.axis_index("frames")
    f_dev, pix = depth_ref.shape
    frames = rot_ref.shape[1]
    loads = fetch(flow_ref, weight_ref, mask_ref, flow3, weight3, mask3, load_sem)
    barrier = pltpu.get_barrier_semaphore()
    total = 0
    for axis in ("frames", "pix"):
        for peer in peers(axis):
            pl.semaphore_signal(
                barrier, inc=1, device_id={axis: peer}, device_id_type=pl.DeviceIdType.MESH
            )
            total += 1
    poses = []
    for ref in (rot_ref, trans_ref):
        poses.append(window(lambda at: ref[:, at], me, f_dev, frames))
    turned = spread_rows(jnp.concatenate(poses, axis=0))
    for k in range(6):
        pose_ref[k] = jnp.broadcast_to(turned[:WIN, k : k + 1], (WIN, L))
    aggregate(edge_ref, loads, flow3, weight3, mask3, own_ref, low_out, high_out, me, f_dev)
    pl.semaphore_wait(barrier, total)
    receive, drain = swap_edges(low_out, high_out, low_ref, high_ref, edge_sem)
    receive()
    drain()
    build(
        lax.axis_index("pix") * pix, pose_ref, own_ref, low_ref, high_ref, depth_ref, damp_ref,
        matrix, zh, zl, base, scale, *scratch[5:15],
    )
    finish(matrix, zh, zl, base, scale, x_ref, step_ref, frames, *scratch[15:])


def call(body, out, scratch, vmem, hbm, **params):
    vm = pl.BlockSpec(memory_space=pltpu.VMEM)
    far = pl.BlockSpec(memory_space=pl.ANY)
    return pl.pallas_call(
        body,
        out_shape=[jax.ShapeDtypeStruct(s, t) for s, t in out],
        in_specs=[vm] * vmem + [far] * hbm,
        out_specs=[vm] * len(out),
        scratch_shapes=scratch,
        compiler_params=pltpu.CompilerParams(vmem_limit_bytes=VMEM_LIMIT, **params),
    )


def per_device(edge_frames, rotvec, trans, inv_depth, depth_damping, flow, weight, mask):
    f_dev, pix = inv_depth.shape
    edges = mask.shape[0]
    frames = rotvec.shape[1]
    tiles = pix // L
    own_rows = f_dev * SLOT
    side = 40
    n = len(UPPER)
    width = 256
    count = lax.axis_size("frames")
    zcount = lax.axis_size("pix")
    chunk = -(-PACKED // (8 * zcount)) * 8
    x, step = call(
        solve,
        [((6, f_dev), F32), ((f_dev, pix), F32)],
        [
            pltpu.VMEM((tiles, 2, edges, L), F32),
            pltpu.VMEM((tiles, 2, edges, L), F32),
            pltpu.VMEM((tiles, edges, L), jnp.int32),
            pltpu.SemaphoreType.DMA((tiles, 5)),
            pltpu.VMEM((6, WIN, L), F32),
            pltpu.VMEM((4, own_rows, pix), F32),
            pltpu.VMEM((4, side, pix), F32),
            pltpu.VMEM((4, side, pix), F32),
            pltpu.VMEM((4, side, pix), F32),
            pltpu.VMEM((4, side, pix), F32),
            pltpu.SemaphoreType.DMA((2, 2, 1)),
            pltpu.VMEM((6 * WIN + 8, width), F32),
            pltpu.VMEM((6 * WIN, f_dev * pix), BF16),
            pltpu.VMEM((6 * WIN, f_dev * pix), BF16),
            pltpu.VMEM((tiles, f_dev, L), F32),
            pltpu.VMEM((tiles, f_dev, L), F32),
            pltpu.VMEM((12, WIN, L), F32),
            pltpu.VMEM((21, SLOT, L), F32),
            pltpu.VMEM((n, SLOT, L), F32),
            pltpu.VMEM((6, SLOT, L), F32),
            pltpu.VMEM((n, WIN, L), F32),
            pltpu.VMEM((6, WIN, L), F32),
            pltpu.VMEM((18, WIN, L), F32),
            pltpu.VMEM((256, 256), F32),
            pltpu.VMEM((tiles, f_dev, L), F32),
            pltpu.VMEM((tiles, f_dev, L), F32),
            pltpu.VMEM((6 * WIN, L), F32),
            pltpu.VMEM((tiles, f_dev, L), F32),
            pltpu.VMEM((chunk * zcount, L), F32),
            pltpu.VMEM((zcount, chunk, L), F32),
            pltpu.VMEM((chunk, L), F32),
            pltpu.VMEM((count, chunk, L), F32),
            pltpu.VMEM((zcount, 4, chunk, frames), F32),
            pltpu.VMEM((6, 12, 8, frames), F32),
            pltpu.VMEM((6, 12, 8, frames), F32),
            pltpu.VMEM((6, 8, frames), F32),
            pltpu.VMEM((8, frames), F32),
            pltpu.SemaphoreType.DMA((2, 2, zcount)),
            pltpu.SemaphoreType.DMA((2, 1, count)),
        ],
        5, 3, collective_id=0, has_side_effects=True,
    )(edge_frames, rotvec, trans, inv_depth, depth_damping, flow, weight, mask)
    return x, step


def solution(mesh):
    return jax.shard_map(
        per_device,
        mesh=mesh,
        in_specs=(
            P(None, "frames"),
            P(),
            P(),
            P("frames", "pix"),
            P("frames", "pix"),
            P("frames", None, "pix"),
            P("frames", None, "pix"),
            P("frames", "pix"),
        ),
        out_specs=(P(None, "frames"), P("frames", "pix")),
        check_vma=False,
    )
```

```python
import jax
import jax.numpy as jnp
from jax import lax
from jax.experimental import pallas as pl
from jax.experimental.pallas import tpu as pltpu
from jax.sharding import PartitionSpec as P

ROWS = 48
COLS = 64
RADIUS = 8
ITERS = 6
REG = 100.0
F32 = jnp.float32
BF16 = jnp.bfloat16
L = 128
WIN = 32
BAND = 2 * RADIUS
PACKED = 160
VMEM_LIMIT = 60 * 1024 * 1024
UPPER = [(i, j) for i in range(6) for j in range(i, 6) if (i, j) != (0, 1)]


def split(x):
    high = x.astype(BF16)
    return high, (x - high.astype(F32)).astype(BF16)


def iota(shape, dim):
    return lax.broadcasted_iota(jnp.int32, shape, dim)


def destinations(edge_ref, own_rows, side, f_dev, me):
    start = me * f_dev
    source = edge_ref[0:1, :] - start + RADIUS
    target = edge_ref[1:2, :] - start + RADIUS
    s = source - RADIUS
    low = jnp.where(s < f_dev // 2, 1, 0)
    above = jnp.where(target > source, 1, 0)
    mine = jnp.where(low == above, 0, f_dev * 8) + s * 8 + (target & 7)
    q = target - RADIUS
    tile = jnp.where(source <= 3, source, jnp.where(source == 7, 4, 6 - source))
    line = jnp.where((source > 3) & (source < 7), q + 7 - source, q)
    lowest = own_rows + tile * 8 + line
    i = source - f_dev - RADIUS
    q = target - f_dev
    tile = jnp.where(i == 0, 4, jnp.where(i <= 4, i - 1, 7 - i))
    line = jnp.where(i > 4, q - i, q)
    highest = own_rows + side + tile * 8 + line
    return jnp.where(source < RADIUS, lowest, jnp.where(source >= RADIUS + f_dev, highest, mine))


def fetch(flow_ref, weight_ref, mask_ref, flow3, weight3, mask3, sems):
    out = []
    for tile in range(flow3.shape[0]):
        cols = pl.ds(tile * L, L)
        pairs = [(mask_ref.at[:, cols], mask3.at[tile])]
        for comp in range(2):
            pairs.append((weight_ref.at[:, comp, cols], weight3.at[tile, comp]))
            pairs.append((flow_ref.at[:, comp, cols], flow3.at[tile, comp]))
        copies = [pltpu.make_async_copy(a, b, sems.at[tile, n]) for n, (a, b) in enumerate(pairs)]
        for copy in copies:
            copy.start()
        out.append(copies)
    return out


def aggregate(edge_ref, loads, flow3, weight3, mask3, own_ref, low_ref, high_ref, me, f_dev):
    edges = edge_ref.shape[1]
    own = own_ref.shape[1]
    side = low_ref.shape[2]
    rows = own + 2 * side
    dest = destinations(edge_ref, own, side, f_dev, me)
    pick = (iota((rows, edges), 0) == dest).astype(F32).astype(BF16)
    for tile, copies in enumerate(loads):
        cols = slice(tile * L, (tile + 1) * L)
        for copy in copies:
            copy.wait()
        live = mask3[tile].astype(F32)
        fields = []
        for comp in range(2):
            conf = weight3[tile, comp] * live
            fields += [conf, conf * flow3[tile, comp]]
        high, low = split(jnp.concatenate(fields, axis=1))
        out = jnp.dot(pick, high, preferred_element_type=F32) + jnp.dot(
            pick, low, preferred_element_type=F32
        )
        for field in range(4):
            part = out[:, field * L : (field + 1) * L]
            own_ref[field, :, cols] = part[:own]
            low_ref[tile, field] = part[own : own + side]
            high_ref[tile, field] = part[own + side :]


def window(load, me, f_dev, frames):
    tiles = frames // L
    first = lax.rem(me * f_dev - RADIUS + frames, frames)
    tile = first // L
    back = lax.rem(L - lax.rem(first, L), L)
    near = pltpu.roll(load(pl.ds(pl.multiple_of(tile * L, L), L)), back, 1)
    if tiles == 1:
        return near
    after = lax.rem(tile + 1, tiles)
    far = pltpu.roll(load(pl.ds(pl.multiple_of(after * L, L), L)), back, 1)
    return jnp.where(iota(near.shape, 1) + lax.rem(first, L) < L, near, far)


def spread_rows(x):
    return jnp.concatenate([x, jnp.zeros((L - x.shape[0], L), F32)], axis=0).T


def motion_sums(u, v, uu, vv, a, b, ds):
    va, ub = v * a, u * b
    e0, e1 = ds * a, ds * b
    return [e0, e1, -(u * e0 + v * e1), -(u * va + vv * b), uu * a + v * ub, ub - va]


def curvature_sums(u, v, uu, vv, uv, ds, wu, wv):
    a1, b1 = wu * v, wv * u
    a2, b2 = a1 * u, b1 * v
    a3, b3 = wu * uu, wv * vv
    h00, h11 = wu * ds * ds, wv * ds * ds
    h02, h12 = h00 * u, h11 * v
    x1, x2, x3 = ds * a1, ds * a2, ds * a3
    y1, y2, y3 = ds * b1, ds * b2, ds * b3
    return [
        h00, h02, x2, x3, x1,
        h11, h12, y3, y2, y1,
        h02 * u + h12 * v, u * x2 + v * y3, u * x3 + v * y2, u * x1 - v * y1,
        a2 * uv + b3 * vv, a2 * uu + b3 * uv, a2 * v - b3 * u,
        a3 * uu + b2 * uv, b2 * u - a3 * v,
        a1 * v + b1 * u,
    ]


SIGNS = [1, -1, -1, 1, -1, 1, -1, -1, 1, 1, 1, 1, -1, 1, 1, -1, 1, 1, 1, 1]


def adj_t(rel, tr, vec):
    turn = [
        vec[3] - (tr[1] * vec[2] - tr[2] * vec[1]),
        vec[4] - (tr[2] * vec[0] - tr[0] * vec[2]),
        vec[5] - (tr[0] * vec[1] - tr[1] * vec[0]),
    ]
    out = [rel[j] * vec[0] + rel[3 + j] * vec[1] + rel[6 + j] * vec[2] for j in range(3)]
    return out + [rel[j] * turn[0] + rel[3 + j] * turn[1] + rel[6 + j] * turn[2] for j in range(3)]


def fold(x):
    row = iota((8, L), 0)

    def merge(a, b, bit):
        other = (row & bit) != 0
        return jnp.where(other, b, a) + pltpu.roll(jnp.where(other, a, b), bit, 0)

    first, second, third = merge(x[0], x[1], 1), merge(x[2], x[3], 1), merge(x[4], x[5], 1)
    return merge(merge(first, second, 2), third + pltpu.roll(third, 2, 0), 4)


def pair_pose(frame_ref, s, first, after):
    here = [frame_ref[k, pl.ds(s + RADIUS, 1), :] for k in range(12)]
    there = [
        jnp.where(after, frame_ref[k, first : first + 8, :], frame_ref[k, first + 8 : first + 16, :])
        for k in range(12)
    ]
    rel = [
        there[3 * r] * here[3 * c] + there[3 * r + 1] * here[3 * c + 1] + there[3 * r + 2] * here[3 * c + 2]
        for r in range(3)
        for c in range(3)
    ]
    tr = [
        there[9 + r] - (rel[3 * r] * here[9] + rel[3 * r + 1] * here[10] + rel[3 * r + 2] * here[11])
        for r in range(3)
    ]
    return rel, tr


def octet(fields, depth, col, rowc, rel, tr):
    wu, fu, wv, fv = fields
    point = [
        rel[3 * k] * col + rel[3 * k + 1] * rowc + rel[3 * k + 2] + depth * tr[k] for k in range(3)
    ]
    iz = 1.0 / point[2]
    u = point[0] * iz
    v = point[1] * iz
    ds = depth * iz
    su = iz * (tr[0] - u * tr[2])
    sv = iz * (tr[1] - v * tr[2])
    au = wu * su
    av = wv * sv
    gu = wu * (col - u) + fu
    gv = wv * (rowc - v) + fv
    uu = 1.0 + u * u
    vv = 1.0 + v * v
    uv = u * v
    e = motion_sums(u, v, uu, vv, au, av, ds)
    back = fold(adj_t(rel, tr, e))
    sums = curvature_sums(u, v, uu, vv, uv, ds, wu, wv) + motion_sums(u, v, uu, vv, gu, gv, ds)
    return e, back, au * su + av * sv, su * gu + sv * gv, sums


def prepare(pose_ref, frame_ref, coord_ref, depth_ref, damp_ref, depth3, damp3):
    tiles = depth3.shape[0]
    ox, oy, oz = pose_ref[0], pose_ref[1], pose_ref[2]
    zero = jnp.zeros_like(ox)
    cross = [[zero, -oz, oy], [oz, zero, -ox], [-oy, ox, zero]]
    sq = ox * ox + oy * oy + oz * oz
    c1 = 1.0 - sq / 6.0 + sq * sq / 120.0
    c2 = 0.5 - sq / 24.0 + sq * sq / 720.0
    for r in range(3):
        for c in range(3):
            square = cross[r][0] * cross[0][c] + cross[r][1] * cross[1][c] + cross[r][2] * cross[2][c]
            frame_ref[3 * r + c] = float(r == c) + c1 * cross[r][c] + c2 * square
        frame_ref[9 + r] = pose_ref[3 + r]
    first = lax.axis_index("pix") * (tiles * L)
    for tile in range(tiles):
        depth3[tile] = depth_ref[:, tile * L : (tile + 1) * L]
        damp3[tile] = damp_ref[:, tile * L : (tile + 1) * L]
        pixel = first + tile * L + iota((8, L), 1)
        prow = pixel // COLS
        pcol = pixel - prow * COLS
        coord_ref[tile, 0] = (pcol.astype(F32) - 0.5 * (COLS - 1)) / COLS
        coord_ref[tile, 1] = (prow.astype(F32) - 0.5 * (ROWS - 1)) / COLS


def note(at, sums, pose, sum_ref, pair_ref):
    for n, x in enumerate(sums):
        sum_ref[n] = jnp.where(at, jnp.sum(x, axis=1, keepdims=True), sum_ref[n])
    for n, x in enumerate(pose):
        pair_ref[n] = jnp.where(at, x, pair_ref[n])


def near_pairs(own_ref, frame_ref, coord_ref, depth3, e_ref, part_ref, sum_ref, pair_ref):
    tiles, f_dev = depth3.shape[:2]
    half = f_dev // 2
    row = iota((8, L), 0)
    lane = iota((8, L), 1)
    sum_ref[...] = jnp.zeros_like(sum_ref)
    pair_ref[...] = jnp.zeros_like(pair_ref)
    for part in range(2):

        @pl.loop(0, half)
        def per_source(i):
            s = i + part * half
            rel, tr = pair_pose(frame_ref, s, 8, row > i if part == 0 else row >= i)
            sums = None
            for tile in range(tiles):
                cols = slice(tile * L, (tile + 1) * L)
                at = pl.ds(pl.multiple_of(s * 8, 8), 8)
                fields = [own_ref[k, at, cols] for k in range(4)]
                e, back, curv, grad, new = octet(
                    fields, depth3[tile, pl.ds(s, 1), :], coord_ref[tile, 0], coord_ref[tile, 1], rel, tr
                )
                slot = s * tiles + tile
                for j in range(6):
                    e_ref[slot, j] = e[j]
                part_ref[slot, 0] = back
                part_ref[slot, 1] = curv
                part_ref[slot, 2] = grad
                sums = new if sums is None else [a + b for a, b in zip(sums, new)]
            note(lane == s + RADIUS, sums, rel + tr, sum_ref, pair_ref)


def far_pairs(
    own_ref, low_ref, high_ref, frame_ref, coord_ref, depth3, damp3, e_ref, part_ref, sum_ref, pair_ref,
    base_ref, inv_ref, zs, gram_ref,
):
    tiles, f_dev = depth3.shape[:2]
    half = f_dev // 2
    row = iota((8, L), 0)
    lane = iota((8, L), 1)
    pair = iota((16, L), 0)
    size = 6 * WIN
    sum_ref[...] = jnp.zeros_like(sum_ref)
    pair_ref[...] = jnp.zeros_like(pair_ref)
    gram_ref[...] = jnp.zeros_like(gram_ref)
    for ref in zs[2:]:
        ref[...] = jnp.zeros_like(ref)
    none = jnp.zeros((8, L), F32)

    def gram(which):
        zh = zs[2 * which][...]
        zl = zs[2 * which + 1][...]
        nt = (((1,), (1,)), ((), ()))
        gram_ref[0] += lax.dot_general(zh[:size], zh, nt, preferred_element_type=F32)
        gram_ref[1] += lax.dot_general(zl, zh, nt, preferred_element_type=F32)

    for part in range(2):

        def per_source(i, which):
            s = i + part * half
            after = row >= i if part == 0 else row > i
            rel, tr = pair_pose(frame_ref, s, 0 if part == 0 else 16, after)
            if part == 0:
                slot = jnp.where(i == 0, 4, jnp.where(i <= 4, i - 1, 7 - i))
                shift = jnp.where(i > 4, i, 0)
                keep = row >= i
                src = high_ref
            else:
                slot = jnp.where(i <= 3, i, jnp.where(i == 7, 4, 6 - i))
                shift = jnp.where((i > 3) & (i < 7), i + 1, 0)
                keep = row <= i
                src = low_ref
            sums = None
            for tile in range(tiles):
                cols = slice(tile * L, (tile + 1) * L)
                at = pl.ds(pl.multiple_of(f_dev * 8 + s * 8, 8), 8)
                fields = []
                for k in range(4):
                    got = src[tile, k, pl.ds(pl.multiple_of(slot * 8, 8), 8), :]
                    fields.append(jnp.where(keep, pltpu.roll(got, shift, 0), own_ref[k, at, cols]))
                e, back, curv, grad, new = octet(
                    fields, depth3[tile, pl.ds(s, 1), :], coord_ref[tile, 0], coord_ref[tile, 1], rel, tr
                )
                sums = new if sums is None else [a + b for a, b in zip(sums, new)]
                here = s * tiles + tile
                for j in range(6):
                    e_ref[here, 6 + j] = e[j]
                back = -(back + part_ref[here, 0])
                e_ref[here, 12] = back
                curv = jnp.sum(curv + part_ref[here, 1], axis=0, keepdims=True) + damp3[tile, pl.ds(s, 1), :]
                grad = -jnp.sum(grad + part_ref[here, 2], axis=0, keepdims=True)
                inv = 1.0 / curv
                scale = 1.0 / jnp.sqrt(curv)
                base_ref[tile, pl.ds(s, 1), :] = grad * inv
                inv_ref[tile, pl.ds(s, 1), :] = inv
                zh, zl = zs[2 * which], zs[2 * which + 1]
                source = back * scale
                for j in range(6):
                    mine = e[j] * scale
                    other = e_ref[here, j] * scale
                    below, over = (mine, other) if part == 0 else (other, mine)
                    mid = jnp.where(row < i, below, jnp.where(row > i, over, source[j : j + 1, :]))
                    groups = [jnp.where(row >= i, below, 0.0), mid, jnp.where(row <= i, over, 0.0)]
                    groups = groups + [none] if part == 0 else [none] + groups
                    high, low = split(jnp.concatenate(groups, axis=0))
                    zh[j * WIN : (j + 1) * WIN, cols] = high
                    zl[j * WIN : (j + 1) * WIN, cols] = low
                y = grad * scale
                rest = y - y.astype(BF16).astype(F32)
                lines = jnp.where(pair == 0, y, jnp.where(pair == 1, rest, 0.0))
                zh[size : size + 16, cols] = lines.astype(BF16)
            note(lane == s + RADIUS, sums, rel + tr, sum_ref, pair_ref)

        @pl.loop(0, half // 2)
        def per_two(k):
            gram(1)
            per_source(2 * k, 0)
            gram(0)
            per_source(2 * k + 1, 1)

    gram(1)


def assemble(near_sum, near_pair, far_sum, far_pair, gram_ref, matrix_ref, wide):
    size = 6 * WIN
    row = iota((8, L), 0)
    lane = iota((8, L), 1)
    i = lane & 7
    first = lane < 16

    def sides(near, far):
        return jnp.where(first, far, near), jnp.where(first, near, far)

    def expand(x):
        low, high = x
        mid = jnp.where(row < i, low, jnp.where(row > i, high, 0.0))
        start = jnp.where(row >= i, low, 0.0)
        end = jnp.where(row <= i, high, 0.0)
        return jnp.concatenate(
            [
                jnp.where(first, start, 0.0),
                jnp.where(first, mid, start),
                jnp.where(first, end, mid),
                jnp.where(first, 0.0, end),
            ],
            axis=0,
        )

    pose = [sides(near_pair[k], far_pair[k]) for k in range(12)]
    h = [[None] * 6 for _ in range(6)]
    wholes = [[None] * 6 for _ in range(6)]
    for n, (a, b) in enumerate(UPPER):
        pair = sides(near_sum[n], far_sum[n])
        h[a][b] = h[b][a] = pair if SIGNS[n] > 0 else tuple(-x for x in pair)
    count = len(UPPER)
    r = [tuple(-x for x in sides(near_sum[count + j], far_sum[count + j])) for j in range(6)]
    eye = iota((WIN, L), 0) == iota((WIN, L), 1)

    def total(terms):
        out = None
        for x, y in terms:
            if x is None or y is None:
                continue
            out = x * y if out is None else out + x * y
        return out

    had = [[[None, None] for _ in range(6)] for _ in range(6)]
    source = [[0.0] * 6 for _ in range(6)]
    lines = [0.0] * 6
    for side in range(2):
        rel = [pose[k][side] for k in range(9)]
        tr = [pose[9 + k][side] for k in range(3)]
        ad = [[None] * 6 for _ in range(6)]
        for c in range(3):
            corner = [
                tr[1] * rel[6 + c] - tr[2] * rel[3 + c],
                tr[2] * rel[c] - tr[0] * rel[6 + c],
                tr[0] * rel[3 + c] - tr[1] * rel[c],
            ]
            for a in range(3):
                ad[a][c] = ad[3 + a][3 + c] = rel[3 * a + c]
                ad[a][3 + c] = corner[a]
        for a in range(6):
            for b in range(6):
                had[a][b][side] = total(
                    [(None if h[a][k] is None else h[a][k][side], ad[k][b]) for k in range(6)]
                )
        for a in range(6):
            for b in range(6):
                source[a][b] = source[a][b] + total([(ad[k][a], had[k][b][side]) for k in range(6)])
        back = adj_t(rel, tr, [x[side] for x in r])
        lines = [x + y for x, y in zip(lines, back)]
    wide[...] = jnp.zeros_like(wide)
    matrix_ref[...] = jnp.zeros_like(matrix_ref)
    for a in range(6):
        rows = slice(a * WIN, (a + 1) * WIN)
        for b in range(6):
            cols = slice(b * WIN, (b + 1) * WIN)
            wide[rows, cols] = -expand(had[a][b])[:, :WIN]
            both = jnp.sum(source[a][b], axis=0, keepdims=True)
            if h[a][b] is not None:
                both = both + jnp.sum(expand(h[a][b]), axis=1, keepdims=True)
            matrix_ref[rows, cols] = jnp.where(eye, both, 0.0)[:, :WIN]
    high, low = gram_ref[0], gram_ref[1]
    wide[:size, :size] = wide[:size, :size] - low[:, :size]
    wide[:size, size : size + 1] = -(
        high[:, size : size + 1] + high[:, size + 1 : size + 2] + low[:, size : size + 1]
    )
    flipped = wide[...].T
    matrix_ref[:size, :size] = (
        matrix_ref[:size, :size] - high[:, :size] + wide[:size, :size] + flipped[:size, :size]
    )
    for j in range(6):
        cols = slice(j * WIN, (j + 1) * WIN)
        whole = jnp.sum(expand(r[j]), axis=1, keepdims=True)
        here = jnp.sum(jnp.where(eye, whole, 0.0), axis=0, keepdims=True)
        here = here - jnp.sum(lines[j], axis=0, keepdims=True)
        matrix_ref[size : size + 1, cols] = here[:, :WIN] + flipped[size : size + 1, cols]


def remote(src, dst, sems, phase, which, axis, peer):
    return pltpu.make_async_remote_copy(
        src_ref=src,
        dst_ref=dst,
        send_sem=sems.at[0, phase, which],
        recv_sem=sems.at[1, phase, which],
        device_id={axis: peer},
        device_id_type=pl.DeviceIdType.MESH,
    )


def peers(axis):
    count = lax.axis_size(axis)
    me = lax.axis_index(axis)
    return [lax.rem(me + step, count) for step in range(1, count)]


def pack(matrix_ref, packed_ref):
    size = 6 * WIN
    lane = iota((WIN, L), 1) % WIN
    row = iota((WIN, L), 0)
    inside = row + lane < WIN
    left = iota((BAND, L), 1) < L // 2
    packed_ref[...] = jnp.zeros_like(packed_ref)

    def skew(x):
        for bit in (1, 2, 4, 8, 16):
            x = jnp.where((lane & bit) != 0, pltpu.roll(x, WIN - bit, 0), x)
        return jnp.where(inside, x, 0.0)

    rest = []
    for j in range(6):
        rows = slice(j * WIN, (j + 1) * WIN)
        main = skew(matrix_ref[rows, :L])
        packed_ref[j * BAND : (j + 1) * BAND, :] = main[:BAND]
        packed_ref[6 * BAND + j : 6 * BAND + j + 1, :] = main[BAND : BAND + 1]
        rest.append(skew(matrix_ref[rows, L:]))
    base = 6 * BAND + 8
    for j in range(3):
        near = rest[j]
        far = pltpu.roll(rest[j + 3], L // 2, 1)
        packed_ref[base + j * BAND : base + (j + 1) * BAND, :] = jnp.where(left, near[:BAND], far[:BAND])
        at = base + 3 * BAND + j
        packed_ref[at : at + 1, :] = jnp.where(left[:1], near[BAND : BAND + 1], far[BAND : BAND + 1])
    packed_ref[6 * BAND + 6 : 6 * BAND + 7, :] = matrix_ref[size : size + 1, :L]
    packed_ref[base + 3 * BAND + 3 : base + 3 * BAND + 4, :] = jnp.where(
        left[:1], matrix_ref[size : size + 1, L:], 0.0
    )


def exchange(src, dst, sems, phase, axis):
    sent = []
    for peer in peers(axis):
        copy = remote(src(peer), dst, sems, phase, len(sent), axis, peer)
        copy.start()
        sent.append(copy)
    return sent


def operator(packed_ref, land, reduced_ref, gathered, diag_ref, ahead_ref, back_ref, far_ref, pix_sem, round_sem, f_dev, frames):
    zcount = lax.axis_size("pix")
    z = lax.axis_index("pix")
    count = lax.axis_size("frames")
    me = lax.axis_index("frames")
    chunk = land.shape[1]
    tiles = frames // L

    def piece(which):
        return pl.ds(pl.multiple_of(which * chunk, 8), chunk)

    sent = exchange(lambda peer: packed_ref.at[piece(peer)], land.at[z], pix_sem, 0, "pix")
    land[z] = packed_ref[piece(z), :]
    for copy in sent:
        copy.wait_recv()
    total = land[0]
    for k in range(1, zcount):
        total = total + land[k]
    reduced_ref[...] = total
    more = exchange(lambda peer: reduced_ref, gathered.at[me], round_sem, 0, "frames")
    gathered[me] = total
    for copy in more:
        copy.wait_recv()
    lane = iota((chunk, L), 1)
    sums = [[None] * tiles for _ in range(4)]
    for w in range(count):
        first = (w * f_dev - RADIUS) % frames
        start = first % L
        for k in range(4):
            part = pltpu.roll(gathered[w], (start - WIN * k) % L, 1)
            spans = [(first // L, start, min(start + WIN, L))]
            if start + WIN > L:
                spans.append(((first // L + 1) % tiles, 0, start + WIN - L))
            for tile, low, high in spans:
                term = jnp.where((lane >= low) & (lane < high), part, 0.0)
                sums[k][tile] = term if sums[k][tile] is None else sums[k][tile] + term
    for k in range(4):
        for tile in range(tiles):
            diag_ref[z, k, :, tile * L : (tile + 1) * L] = sums[k][tile]
    for copy in sent + more:
        copy.wait_send()
    sent = exchange(lambda peer: diag_ref.at[z], diag_ref.at[z], pix_sem, 1, "pix")
    for copy in sent:
        copy.wait_recv()
    for copy in sent:
        copy.wait_send()

    def block(k, at):
        return [
            diag_ref[at // chunk, k, at % chunk : at % chunk + 8, t * L : (t + 1) * L]
            for t in range(tiles)
        ]

    def entry(i, j, half):
        if i < 4:
            return block(i, BAND * j + 8 * half)
        return block(i - 4 + 2 * (j // 3), 6 * BAND + 8 + BAND * (j % 3) + 8 * half)

    row = iota((8, L), 0)
    lanes = iota((8, L), 1)

    def later(x, half):
        turned = [pltpu.roll(v, 8 * half, 1, stride=1, stride_axis=0) for v in x]
        if tiles == 1:
            return turned
        mine = lanes >= 8 * half + row
        return [jnp.where(mine, turned[t], turned[t - 1]) for t in range(tiles)]

    def flip(x):
        for bit in (4, 2, 1):
            x = jnp.where((row & bit) != 0, pltpu.roll(x, bit, 0), pltpu.roll(x, 8 - bit, 0))
        return x

    for i in range(6):
        for j in range(6):
            for half in range(2):
                front = entry(i, j, half)
                moved = later(entry(j, i, half), half)
                for t in range(tiles):
                    ahead_ref[i, 2 * j + half, :, t * L : (t + 1) * L] = flip(front[t])
                    value = jnp.where(row > 0, moved[t], 0.0) if half == 0 else moved[t]
                    back_ref[i, 2 * j + half, :, t * L : (t + 1) * L] = value
    edge = 6 * BAND
    last = edge + 8 + 3 * BAND
    for i in range(6):
        if i < 4:
            ends = block(i, edge)
        else:
            near, far = block(i - 4, last), block(i - 2, last)
            ends = [jnp.where(row < 3, a, pltpu.roll(b, 3, 0)) for a, b in zip(near, far)]
        for t in range(tiles):
            far_ref[i, :, t * L : (t + 1) * L] = jnp.where(row < 6, ends[t], 0.0)
    sources = [block(k, edge) for k in range(4)] + [block(k, last) for k in range(2)]
    rhs = []
    for t in range(tiles):
        out = jnp.zeros((8, L), F32)
        for i in range(6):
            at = 6 if i < 4 else 3
            out = jnp.where(row == i, sources[i][t][at : at + 1, :], out)
        rhs.append(out)
    return rhs, later


def conjugate(rhs, later, ahead_ref, back_ref, far_ref):
    tiles = len(rhs)
    row = iota((8, L), 0)
    lanes = iota((8, L), 1)

    def sooner(x, half):
        turned = [pltpu.roll(v, L - 8 * half - 7, 1, stride=1, stride_axis=0) for v in x]
        if tiles == 1:
            return turned
        mine = lanes + 8 * half + 7 - row < L
        return [jnp.where(mine, turned[t], turned[(t + 1) % tiles]) for t in range(tiles)]

    def moved(x, steps):
        turned = [pltpu.roll(v, steps % L, 1) for v in x]
        if tiles == 1:
            return turned
        if steps > 0:
            return [jnp.where(lanes >= steps, turned[t], turned[t - 1]) for t in range(tiles)]
        return [jnp.where(lanes < L + steps, turned[t], turned[(t + 1) % tiles]) for t in range(tiles)]

    def dot(x, y):
        total = x[0] * y[0]
        for t in range(1, tiles):
            total = total + x[t] * y[t]
        return jnp.sum(total, keepdims=True)

    def product(p):
        ahead = moved(p, -BAND)
        acc = [[far_ref[i, :, t * L : (t + 1) * L] * ahead[t] for t in range(tiles)] for i in range(6)]
        tail = [None] * tiles
        for j in range(6):
            wide = [jnp.broadcast_to(v[j : j + 1, :], (8, L)) for v in p]
            for t in range(tiles):
                term = far_ref[j, :, t * L : (t + 1) * L] * wide[t]
                tail[t] = term if tail[t] is None else tail[t] + term
            for half in range(2):
                plus = sooner(wide, half)
                minus = later(wide, half)
                for i in range(6):
                    for t in range(tiles):
                        acc[i][t] = (
                            acc[i][t]
                            + ahead_ref[i, 2 * j + half, :, t * L : (t + 1) * L] * plus[t]
                            + back_ref[i, 2 * j + half, :, t * L : (t + 1) * L] * minus[t]
                        )
        tail = moved(tail, BAND)
        out = []
        for t in range(tiles):
            y = tail[t] + REG * p[t]
            for i in range(6):
                y = y + jnp.where(row == i, jnp.sum(acc[i][t], axis=0, keepdims=True), 0.0)
            out.append(y)
        return out

    def step(_, carry):
        x, residual, direction, rr = carry
        image = product(direction)
        alpha = rr / dot(direction, image)
        x = [a + alpha * b for a, b in zip(x, direction)]
        residual = [a - alpha * b for a, b in zip(residual, image)]
        new = dot(residual, residual)
        beta = new / rr
        direction = [a + beta * b for a, b in zip(residual, direction)]
        return x, residual, direction, new

    zero = [jnp.zeros((8, L), F32)] * tiles
    return lax.fori_loop(0, ITERS, step, (zero, rhs, rhs, dot(rhs, rhs)))[0]


def finish(
    matrix_ref, e_ref, base_ref, inv_ref, pose_ref, step_ref, frames,
    cols_ref, step3, packed_ref, land, reduced_ref, gathered, diag_ref, ahead_ref, back_ref, far_ref, x_ref,
    pix_sem, round_sem,
):
    me = lax.axis_index("frames")
    tiles, f_dev = step3.shape[:2]
    half = f_dev // 2
    pack(matrix_ref, packed_ref)
    rhs, later = operator(
        packed_ref, land, reduced_ref, gathered, diag_ref, ahead_ref, back_ref, far_ref,
        pix_sem, round_sem, f_dev, frames,
    )
    x = conjugate(rhs, later, ahead_ref, back_ref, far_ref)
    for t, value in enumerate(x):
        x_ref[:, t * L : (t + 1) * L] = value
    mine = window(lambda at: x_ref[:, at], me, f_dev, frames)
    pose_ref[...] = mine[:6, RADIUS : RADIUS + f_dev]
    turned = spread_rows(mine)
    for i in range(6):
        cols_ref[i] = jnp.broadcast_to(turned[:WIN, i : i + 1], (WIN, L))
    row = iota((8, L), 0)
    lane = iota((8, L), 1)
    for part in range(2):

        @pl.loop(0, half)
        def per_source(i):
            s = i + part * half
            group = [[cols_ref[j, 8 * g : 8 * g + 8, :] for g in range(part, part + 3)] for j in range(6)]
            below = [jnp.where(row >= i, group[j][0], group[j][1]) for j in range(6)]
            over = [jnp.where(row > i, group[j][1], group[j][2]) for j in range(6)]
            near, far = (over, below) if part == 0 else (below, over)
            at = jnp.sum(jnp.where(lane == s + RADIUS, mine, 0.0), axis=1, keepdims=True)
            terms = near + far + [jnp.broadcast_to(at, (8, L))]
            for tile in range(tiles):
                slot = s * tiles + tile
                image = e_ref[slot, 0] * terms[0]
                for n in range(1, 13):
                    image = image + e_ref[slot, n] * terms[n]
                image = jnp.sum(image, axis=0, keepdims=True)
                here = (tile, pl.ds(s, 1), slice(None))
                step3[here] = base_ref[here] - inv_ref[here] * image

    for tile in range(tiles):
        step_ref[:, tile * L : (tile + 1) * L] = step3[tile]


def swap_edges(low_out, high_out, low_ref, high_ref, sems):
    count = lax.axis_size("frames")
    me = lax.axis_index("frames")
    below = lax.rem(me + count - 1, count)
    over = lax.rem(me + 1, count)
    tiles = low_out.shape[0]
    down = [remote(low_out.at[t], low_ref.at[t], sems, 0, t, "frames", below) for t in range(tiles)]
    up = [remote(high_out.at[t], high_ref.at[t], sems, 1, t, "frames", over) for t in range(tiles)]

    @pl.when(me > 0)
    def _():
        for copy in down:
            copy.start()

    @pl.when(me < count - 1)
    def _():
        for copy in up:
            copy.start()

    def receive():
        @pl.when(me < count - 1)
        def _():
            for copy in down:
                copy.wait_recv()

        @pl.when(me == count - 1)
        def _():
            low_ref[...] = jnp.zeros_like(low_ref)

        @pl.when(me > 0)
        def _():
            for copy in up:
                copy.wait_recv()

        @pl.when(me == 0)
        def _():
            high_ref[...] = jnp.zeros_like(high_ref)

    def drain():
        @pl.when(me > 0)
        def _():
            for copy in down:
                copy.wait_send()

        @pl.when(me < count - 1)
        def _():
            for copy in up:
                copy.wait_send()

    return receive, drain


def solve(
    edge_ref, rot_ref, trans_ref, depth_ref, damp_ref, flow_ref, weight_ref, mask_ref,
    x_ref, step_ref, flow3, weight3, mask3, load_sem, pose_ref,
    own_ref, low_out, high_out, low_ref, high_ref, edge_sem,
    frame_ref, coord_ref, depth3, damp3, e_ref, part_ref, near_sum, near_pair, far_sum, far_pair,
    base_ref, inv_ref, zh0, zl0, zh1, zl1, gram_ref, matrix_ref, wide, *scratch,
):
    me = lax.axis_index("frames")
    f_dev, pix = depth_ref.shape
    frames = rot_ref.shape[1]
    loads = fetch(flow_ref, weight_ref, mask_ref, flow3, weight3, mask3, load_sem)
    barrier = pltpu.get_barrier_semaphore()
    total = 0
    for axis in ("frames", "pix"):
        for peer in peers(axis):
            pl.semaphore_signal(
                barrier, inc=1, device_id={axis: peer}, device_id_type=pl.DeviceIdType.MESH
            )
            total += 1
    poses = []
    for ref in (rot_ref, trans_ref):
        poses.append(window(lambda at: ref[:, at], me, f_dev, frames))
    turned = spread_rows(jnp.concatenate(poses, axis=0))
    for k in range(6):
        pose_ref[k] = jnp.broadcast_to(turned[:WIN, k : k + 1], (WIN, L))
    prepare(pose_ref, frame_ref, coord_ref, depth_ref, damp_ref, depth3, damp3)
    aggregate(edge_ref, loads, flow3, weight3, mask3, own_ref, low_out, high_out, me, f_dev)
    pl.semaphore_wait(barrier, total)
    receive, drain = swap_edges(low_out, high_out, low_ref, high_ref, edge_sem)
    near_pairs(own_ref, frame_ref, coord_ref, depth3, e_ref, part_ref, near_sum, near_pair)
    receive()
    far_pairs(
        own_ref, low_ref, high_ref, frame_ref, coord_ref, depth3, damp3, e_ref, part_ref,
        far_sum, far_pair, base_ref, inv_ref, (zh0, zl0, zh1, zl1), gram_ref,
    )
    assemble(near_sum, near_pair, far_sum, far_pair, gram_ref, matrix_ref, wide)
    finish(matrix_ref, e_ref, base_ref, inv_ref, x_ref, step_ref, frames, *scratch)
    drain()


def call(body, out, scratch, vmem, hbm, **params):
    vm = pl.BlockSpec(memory_space=pltpu.VMEM)
    far = pl.BlockSpec(memory_space=pl.ANY)
    return pl.pallas_call(
        body,
        out_shape=[jax.ShapeDtypeStruct(s, t) for s, t in out],
        in_specs=[vm] * vmem + [far] * hbm,
        out_specs=[vm] * len(out),
        scratch_shapes=scratch,
        compiler_params=pltpu.CompilerParams(vmem_limit_bytes=VMEM_LIMIT, **params),
    )


def per_device(edge_frames, rotvec, trans, inv_depth, depth_damping, flow, weight, mask):
    f_dev, pix = inv_depth.shape
    edges = mask.shape[0]
    frames = rotvec.shape[1]
    tiles = pix // L
    own_rows = f_dev * 16
    side = 40
    sums = len(UPPER) + 6
    width = 256
    size = 6 * WIN
    count = lax.axis_size("frames")
    zcount = lax.axis_size("pix")
    chunk = -(-PACKED // (8 * zcount)) * 8
    x, step = call(
        solve,
        [((6, f_dev), F32), ((f_dev, pix), F32)],
        [
            pltpu.VMEM((tiles, 2, edges, L), F32),
            pltpu.VMEM((tiles, 2, edges, L), F32),
            pltpu.VMEM((tiles, edges, L), jnp.int32),
            pltpu.SemaphoreType.DMA((tiles, 5)),
            pltpu.VMEM((6, WIN, L), F32),
            pltpu.VMEM((4, own_rows, pix), F32),
            pltpu.VMEM((tiles, 4, side, L), F32),
            pltpu.VMEM((tiles, 4, side, L), F32),
            pltpu.VMEM((tiles, 4, side, L), F32),
            pltpu.VMEM((tiles, 4, side, L), F32),
            pltpu.SemaphoreType.DMA((2, 2, tiles)),
            pltpu.VMEM((12, WIN, L), F32),
            pltpu.VMEM((tiles, 2, 8, L), F32),
            pltpu.VMEM((tiles, f_dev, L), F32),
            pltpu.VMEM((tiles, f_dev, L), F32),
            pltpu.VMEM((f_dev * tiles, 13, 8, L), F32),
            pltpu.VMEM((f_dev * tiles, 3, 8, L), F32),
            pltpu.VMEM((sums, 8, L), F32),
            pltpu.VMEM((12, 8, L), F32),
            pltpu.VMEM((sums, 8, L), F32),
            pltpu.VMEM((12, 8, L), F32),
            pltpu.VMEM((tiles, f_dev, L), F32),
            pltpu.VMEM((tiles, f_dev, L), F32),
            pltpu.VMEM((size + 16, pix), BF16),
            pltpu.VMEM((size, pix), BF16),
            pltpu.VMEM((size + 16, pix), BF16),
            pltpu.VMEM((size, pix), BF16),
            pltpu.VMEM((2, size, size + 16), F32),
            pltpu.VMEM((size + 8, width), F32),
            pltpu.VMEM((256, 256), F32),
            pltpu.VMEM((6, WIN, L), F32),
            pltpu.VMEM((tiles, f_dev, L), F32),
            pltpu.VMEM((chunk * zcount, L), F32),
            pltpu.VMEM((zcount, chunk, L), F32),
            pltpu.VMEM((chunk, L), F32),
            pltpu.VMEM((count, chunk, L), F32),
            pltpu.VMEM((zcount, 4, chunk, frames), F32),
            pltpu.VMEM((6, 12, 8, frames), F32),
            pltpu.VMEM((6, 12, 8, frames), F32),
            pltpu.VMEM((6, 8, frames), F32),
            pltpu.VMEM((8, frames), F32),
            pltpu.SemaphoreType.DMA((2, 2, zcount)),
            pltpu.SemaphoreType.DMA((2, 1, count)),
        ],
        5, 3, collective_id=0, has_side_effects=True,
    )(edge_frames, rotvec, trans, inv_depth, depth_damping, flow, weight, mask)
    return x, step


def solution(mesh):
    return jax.shard_map(
        per_device,
        mesh=mesh,
        in_specs=(
            P(None, "frames"),
            P(),
            P(),
            P("frames", "pix"),
            P("frames", "pix"),
            P("frames", None, "pix"),
            P("frames", None, "pix"),
            P("frames", "pix"),
        ),
        out_specs=(P(None, "frames"), P("frames", "pix")),
        check_vma=False,
    )
```

```python
import jax
import jax.numpy as jnp
from jax import lax
from jax.experimental import pallas as pl
from jax.experimental.pallas import tpu as pltpu
from jax.sharding import PartitionSpec as P

ROWS = 48
COLS = 64
RADIUS = 8
ITERS = 6
REG = 100.0
F32 = jnp.float32
BF16 = jnp.bfloat16
L = 128
WIN = 32
BAND = 2 * RADIUS
PACKED = 160
SENT = RADIUS * (RADIUS + 1) // 2
VMEM_LIMIT = 60 * 1024 * 1024
UPPER = [(i, j) for i in range(6) for j in range(i, 6) if (i, j) != (0, 1)]


def split(x):
    high = x.astype(BF16)
    return high, (x - high.astype(F32)).astype(BF16)


def iota(shape, dim):
    return lax.broadcasted_iota(jnp.int32, shape, dim)


def destinations(edge_ref, own_rows, side, f_dev, me):
    start = me * f_dev
    source = edge_ref[0:1, :] - start + RADIUS
    target = edge_ref[1:2, :] - start + RADIUS
    s = source - RADIUS
    low = jnp.where(s < f_dev // 2, 1, 0)
    above = jnp.where(target > source, 1, 0)
    mine = jnp.where(low == above, 0, f_dev * 8) + s * 8 + (target & 7)
    q = target - RADIUS
    tile = jnp.where(source < 3, source, jnp.where(source == 3, 4, jnp.where(source == 7, 3, 6 - source)))
    line = jnp.where((source > 3) & (source < 7), q + 7 - source, q)
    lowest = own_rows + tile * 8 + line
    i = source - f_dev - RADIUS
    q = target - f_dev
    tile = jnp.where(i == 0, 3, jnp.where(i < 4, i - 1, jnp.where(i == 4, 4, 7 - i)))
    line = jnp.where(i >= 4, q - i, q)
    highest = own_rows + side + tile * 8 + line
    return jnp.where(source < RADIUS, lowest, jnp.where(source >= RADIUS + f_dev, highest, mine))


def fetch(flow_ref, weight_ref, mask_ref, flow3, weight3, mask3, sems):
    out = []
    for tile in range(flow3.shape[0]):
        cols = pl.ds(tile * L, L)
        pairs = [(mask_ref.at[:, cols], mask3.at[tile])]
        for comp in range(2):
            pairs.append((weight_ref.at[:, comp, cols], weight3.at[tile, comp]))
            pairs.append((flow_ref.at[:, comp, cols], flow3.at[tile, comp]))
        copies = [pltpu.make_async_copy(a, b, sems.at[tile, n]) for n, (a, b) in enumerate(pairs)]
        for copy in copies:
            copy.start()
        out.append(copies)
    return out


def aggregate(edge_ref, loads, flow3, weight3, mask3, own_ref, low_ref, high_ref, me, f_dev):
    edges = edge_ref.shape[1]
    own = own_ref.shape[1]
    side = low_ref.shape[2]
    rows = own + 2 * side
    dest = destinations(edge_ref, own, side, f_dev, me)
    pick = (iota((rows, edges), 0) == dest).astype(F32).astype(BF16)
    for tile, copies in enumerate(loads):
        cols = slice(tile * L, (tile + 1) * L)
        for copy in copies:
            copy.wait()
        live = mask3[tile].astype(F32)
        fields = []
        for comp in range(2):
            conf = weight3[tile, comp] * live
            fields += [conf, conf * flow3[tile, comp]]
        high, low = split(jnp.concatenate(fields, axis=1))
        out = jnp.dot(pick, high, preferred_element_type=F32) + jnp.dot(
            pick, low, preferred_element_type=F32
        )
        for field in range(4):
            part = out[:, field * L : (field + 1) * L]
            own_ref[field, :, cols] = part[:own]
            low_ref[tile, field] = part[own : own + side]
            high_ref[tile, field] = part[own + side :]


def window(load, me, f_dev, frames):
    tiles = frames // L
    first = lax.rem(me * f_dev - RADIUS + frames, frames)
    tile = first // L
    back = lax.rem(L - lax.rem(first, L), L)
    near = pltpu.roll(load(pl.ds(pl.multiple_of(tile * L, L), L)), back, 1)
    if tiles == 1:
        return near
    after = lax.rem(tile + 1, tiles)
    far = pltpu.roll(load(pl.ds(pl.multiple_of(after * L, L), L)), back, 1)
    return jnp.where(iota(near.shape, 1) + lax.rem(first, L) < L, near, far)


def spread_rows(x):
    return jnp.concatenate([x, jnp.zeros((L - x.shape[0], L), F32)], axis=0).T


def motion_sums(u, v, uu, vv, a, b, ds):
    va, ub = v * a, u * b
    e0, e1 = ds * a, ds * b
    return [e0, e1, -(u * e0 + v * e1), -(u * va + vv * b), uu * a + v * ub, ub - va]


def curvature_sums(u, v, uu, vv, uv, ds, wu, wv):
    a1, b1 = wu * v, wv * u
    a2, b2 = a1 * u, b1 * v
    a3, b3 = wu * uu, wv * vv
    h00, h11 = wu * ds * ds, wv * ds * ds
    h02, h12 = h00 * u, h11 * v
    x1, x2, x3 = ds * a1, ds * a2, ds * a3
    y1, y2, y3 = ds * b1, ds * b2, ds * b3
    return [
        h00, h02, x2, x3, x1,
        h11, h12, y3, y2, y1,
        h02 * u + h12 * v, u * x2 + v * y3, u * x3 + v * y2, u * x1 - v * y1,
        a2 * uv + b3 * vv, a2 * uu + b3 * uv, a2 * v - b3 * u,
        a3 * uu + b2 * uv, b2 * u - a3 * v,
        a1 * v + b1 * u,
    ]


SIGNS = [1, -1, -1, 1, -1, 1, -1, -1, 1, 1, 1, 1, -1, 1, 1, -1, 1, 1, 1, 1]


def adj_t(rel, tr, vec):
    turn = [
        vec[3] - (tr[1] * vec[2] - tr[2] * vec[1]),
        vec[4] - (tr[2] * vec[0] - tr[0] * vec[2]),
        vec[5] - (tr[0] * vec[1] - tr[1] * vec[0]),
    ]
    out = [rel[j] * vec[0] + rel[3 + j] * vec[1] + rel[6 + j] * vec[2] for j in range(3)]
    return out + [rel[j] * turn[0] + rel[3 + j] * turn[1] + rel[6 + j] * turn[2] for j in range(3)]


def fold(x):
    row = iota((8, L), 0)

    def merge(a, b, bit):
        other = (row & bit) != 0
        return jnp.where(other, b, a) + pltpu.roll(jnp.where(other, a, b), bit, 0)

    first, second, third = merge(x[0], x[1], 1), merge(x[2], x[3], 1), merge(x[4], x[5], 1)
    return merge(merge(first, second, 2), third + pltpu.roll(third, 2, 0), 4)


def pair_pose(frame_ref, s, first, after):
    here = [frame_ref[k, pl.ds(s + RADIUS, 1), :] for k in range(12)]
    there = [
        jnp.where(after, frame_ref[k, first : first + 8, :], frame_ref[k, first + 8 : first + 16, :])
        for k in range(12)
    ]
    rel = [
        there[3 * r] * here[3 * c] + there[3 * r + 1] * here[3 * c + 1] + there[3 * r + 2] * here[3 * c + 2]
        for r in range(3)
        for c in range(3)
    ]
    tr = [
        there[9 + r] - (rel[3 * r] * here[9] + rel[3 * r + 1] * here[10] + rel[3 * r + 2] * here[11])
        for r in range(3)
    ]
    return rel, tr


def octet(fields, depth, col, rowc, rel, tr):
    wu, fu, wv, fv = fields
    point = [
        rel[3 * k] * col + rel[3 * k + 1] * rowc + rel[3 * k + 2] + depth * tr[k] for k in range(3)
    ]
    iz = 1.0 / point[2]
    u = point[0] * iz
    v = point[1] * iz
    ds = depth * iz
    su = iz * (tr[0] - u * tr[2])
    sv = iz * (tr[1] - v * tr[2])
    au = wu * su
    av = wv * sv
    gu = wu * (col - u) + fu
    gv = wv * (rowc - v) + fv
    uu = 1.0 + u * u
    vv = 1.0 + v * v
    uv = u * v
    e = motion_sums(u, v, uu, vv, au, av, ds)
    back = fold(adj_t(rel, tr, e))
    sums = curvature_sums(u, v, uu, vv, uv, ds, wu, wv) + motion_sums(u, v, uu, vv, gu, gv, ds)
    return e, back, au * su + av * sv, su * gu + sv * gv, sums


def prepare(pose_ref, frame_ref, coord_ref, depth_ref, damp_ref, depth3, damp3):
    tiles = depth3.shape[0]
    ox, oy, oz = pose_ref[0], pose_ref[1], pose_ref[2]
    zero = jnp.zeros_like(ox)
    cross = [[zero, -oz, oy], [oz, zero, -ox], [-oy, ox, zero]]
    sq = ox * ox + oy * oy + oz * oz
    c1 = 1.0 - sq / 6.0 + sq * sq / 120.0
    c2 = 0.5 - sq / 24.0 + sq * sq / 720.0
    for r in range(3):
        for c in range(3):
            square = cross[r][0] * cross[0][c] + cross[r][1] * cross[1][c] + cross[r][2] * cross[2][c]
            frame_ref[3 * r + c] = float(r == c) + c1 * cross[r][c] + c2 * square
        frame_ref[9 + r] = pose_ref[3 + r]
    first = lax.axis_index("pix") * (tiles * L)
    for tile in range(tiles):
        depth3[tile] = depth_ref[:, tile * L : (tile + 1) * L]
        damp3[tile] = damp_ref[:, tile * L : (tile + 1) * L]
        pixel = first + tile * L + iota((8, L), 1)
        prow = pixel // COLS
        pcol = pixel - prow * COLS
        coord_ref[tile, 0] = (pcol.astype(F32) - 0.5 * (COLS - 1)) / COLS
        coord_ref[tile, 1] = (prow.astype(F32) - 0.5 * (ROWS - 1)) / COLS


def note(at, sums, pose, sum_ref, pair_ref):
    for n, x in enumerate(sums):
        sum_ref[n] = jnp.where(at, jnp.sum(x, axis=1, keepdims=True), sum_ref[n])
    for n, x in enumerate(pose):
        pair_ref[n] = jnp.where(at, x, pair_ref[n])


def near_pairs(own_ref, frame_ref, coord_ref, depth3, e_ref, part_ref, sum_ref, pair_ref, descend):
    tiles, f_dev = depth3.shape[:2]
    half = f_dev // 2
    row = iota((8, L), 0)
    lane = iota((8, L), 1)
    sum_ref[...] = jnp.zeros_like(sum_ref)
    pair_ref[...] = jnp.zeros_like(pair_ref)
    for part in range(2):

        @pl.loop(0, half)
        def per_source(i):
            s = i + part * half
            rel, tr = pair_pose(frame_ref, s, 8, row > i if part == 0 else row >= i)
            sums = None
            for tile in range(tiles):
                cols = slice(tile * L, (tile + 1) * L)
                at = pl.ds(pl.multiple_of(s * 8, 8), 8)
                fields = [own_ref[k, at, cols] for k in range(4)]
                e, back, curv, grad, new = octet(
                    fields, depth3[tile, pl.ds(s, 1), :], coord_ref[tile, 0], coord_ref[tile, 1], rel, tr
                )
                slot = s * tiles + tile
                for j in range(6):
                    e_ref[slot, j] = e[j]
                part_ref[slot, 0] = back
                part_ref[slot, 1] = curv
                part_ref[slot, 2] = grad
                sums = new if sums is None else [a + b for a, b in zip(sums, new)]
            note(lane == s + RADIUS, sums, rel + tr, sum_ref, pair_ref)

        if part == 1:
            descend()


def far_pairs(
    own_ref, low_ref, high_ref, frame_ref, coord_ref, depth3, damp3, e_ref, part_ref, sum_ref, pair_ref,
    base_ref, inv_ref, zs, gram_ref, receive,
):
    tiles, f_dev = depth3.shape[:2]
    half = f_dev // 2
    row = iota((8, L), 0)
    lane = iota((8, L), 1)
    pair = iota((16, L), 0)
    size = 6 * WIN
    sum_ref[...] = jnp.zeros_like(sum_ref)
    pair_ref[...] = jnp.zeros_like(pair_ref)
    gram_ref[...] = jnp.zeros_like(gram_ref)
    for ref in zs[2:]:
        ref[...] = jnp.zeros_like(ref)
    none = jnp.zeros((8, L), F32)

    def gram(which):
        zh = zs[2 * which][...]
        zl = zs[2 * which + 1][...]
        nt = (((1,), (1,)), ((), ()))
        gram_ref[0] += lax.dot_general(zh[:size], zh, nt, preferred_element_type=F32)
        gram_ref[1] += lax.dot_general(zl, zh, nt, preferred_element_type=F32)

    for part in range(2):
        receive(part)

        def per_source(i, which):
            s = i + part * half
            after = row >= i if part == 0 else row > i
            rel, tr = pair_pose(frame_ref, s, 0 if part == 0 else 16, after)
            if part == 0:
                slot = jnp.where(i == 0, 3, jnp.where(i < 4, i - 1, jnp.where(i == 4, 4, 7 - i)))
                shift = jnp.where(i >= 4, i, 0)
                keep = row >= i
                src = high_ref
            else:
                slot = jnp.where(i < 3, i, jnp.where(i == 3, 4, jnp.where(i == 7, 3, 6 - i)))
                shift = jnp.where((i > 3) & (i < 7), i + 1, 0)
                keep = row <= i
                src = low_ref
            sums = None
            for tile in range(tiles):
                cols = slice(tile * L, (tile + 1) * L)
                at = pl.ds(pl.multiple_of(f_dev * 8 + s * 8, 8), 8)
                fields = []
                for k in range(4):
                    got = src[tile, k, pl.ds(pl.multiple_of(slot * 8, 8), 8), :]
                    fields.append(jnp.where(keep, pltpu.roll(got, shift, 0), own_ref[k, at, cols]))
                e, back, curv, grad, new = octet(
                    fields, depth3[tile, pl.ds(s, 1), :], coord_ref[tile, 0], coord_ref[tile, 1], rel, tr
                )
                sums = new if sums is None else [a + b for a, b in zip(sums, new)]
                here = s * tiles + tile
                for j in range(6):
                    e_ref[here, 6 + j] = e[j]
                back = -(back + part_ref[here, 0])
                e_ref[here, 12] = back
                curv = jnp.sum(curv + part_ref[here, 1], axis=0, keepdims=True) + damp3[tile, pl.ds(s, 1), :]
                grad = -jnp.sum(grad + part_ref[here, 2], axis=0, keepdims=True)
                inv = 1.0 / curv
                scale = 1.0 / jnp.sqrt(curv)
                base_ref[tile, pl.ds(s, 1), :] = grad * inv
                inv_ref[tile, pl.ds(s, 1), :] = inv
                zh, zl = zs[2 * which], zs[2 * which + 1]
                source = back * scale
                for j in range(6):
                    mine = e[j] * scale
                    other = e_ref[here, j] * scale
                    below, over = (mine, other) if part == 0 else (other, mine)
                    mid = jnp.where(row < i, below, jnp.where(row > i, over, source[j : j + 1, :]))
                    groups = [jnp.where(row >= i, below, 0.0), mid, jnp.where(row <= i, over, 0.0)]
                    groups = groups + [none] if part == 0 else [none] + groups
                    high, low = split(jnp.concatenate(groups, axis=0))
                    zh[j * WIN : (j + 1) * WIN, cols] = high
                    zl[j * WIN : (j + 1) * WIN, cols] = low
                y = grad * scale
                rest = y - y.astype(BF16).astype(F32)
                lines = jnp.where(pair == 0, y, jnp.where(pair == 1, rest, 0.0))
                zh[size : size + 16, cols] = lines.astype(BF16)
            note(lane == s + RADIUS, sums, rel + tr, sum_ref, pair_ref)

        @pl.loop(0, half // 2)
        def per_two(k):
            gram(1)
            per_source(2 * k, 0)
            gram(0)
            per_source(2 * k + 1, 1)

    gram(1)


def assemble(near_sum, near_pair, far_sum, far_pair, gram_ref, matrix_ref, wide):
    size = 6 * WIN
    row = iota((8, L), 0)
    lane = iota((8, L), 1)
    i = lane & 7
    first = lane < 16

    def sides(near, far):
        return jnp.where(first, far, near), jnp.where(first, near, far)

    def expand(x):
        low, high = x
        mid = jnp.where(row < i, low, jnp.where(row > i, high, 0.0))
        start = jnp.where(row >= i, low, 0.0)
        end = jnp.where(row <= i, high, 0.0)
        return jnp.concatenate(
            [
                jnp.where(first, start, 0.0),
                jnp.where(first, mid, start),
                jnp.where(first, end, mid),
                jnp.where(first, 0.0, end),
            ],
            axis=0,
        )

    pose = [sides(near_pair[k], far_pair[k]) for k in range(12)]
    h = [[None] * 6 for _ in range(6)]
    wholes = [[None] * 6 for _ in range(6)]
    for n, (a, b) in enumerate(UPPER):
        pair = sides(near_sum[n], far_sum[n])
        h[a][b] = h[b][a] = pair if SIGNS[n] > 0 else tuple(-x for x in pair)
    count = len(UPPER)
    r = [tuple(-x for x in sides(near_sum[count + j], far_sum[count + j])) for j in range(6)]
    eye = iota((WIN, L), 0) == iota((WIN, L), 1)

    def total(terms):
        out = None
        for x, y in terms:
            if x is None or y is None:
                continue
            out = x * y if out is None else out + x * y
        return out

    had = [[[None, None] for _ in range(6)] for _ in range(6)]
    source = [[0.0] * 6 for _ in range(6)]
    lines = [0.0] * 6
    for side in range(2):
        rel = [pose[k][side] for k in range(9)]
        tr = [pose[9 + k][side] for k in range(3)]
        ad = [[None] * 6 for _ in range(6)]
        for c in range(3):
            corner = [
                tr[1] * rel[6 + c] - tr[2] * rel[3 + c],
                tr[2] * rel[c] - tr[0] * rel[6 + c],
                tr[0] * rel[3 + c] - tr[1] * rel[c],
            ]
            for a in range(3):
                ad[a][c] = ad[3 + a][3 + c] = rel[3 * a + c]
                ad[a][3 + c] = corner[a]
        for a in range(6):
            for b in range(6):
                had[a][b][side] = total(
                    [(None if h[a][k] is None else h[a][k][side], ad[k][b]) for k in range(6)]
                )
        for a in range(6):
            for b in range(6):
                source[a][b] = source[a][b] + total([(ad[k][a], had[k][b][side]) for k in range(6)])
        back = adj_t(rel, tr, [x[side] for x in r])
        lines = [x + y for x, y in zip(lines, back)]
    wide[...] = jnp.zeros_like(wide)
    matrix_ref[...] = jnp.zeros_like(matrix_ref)
    for a in range(6):
        rows = slice(a * WIN, (a + 1) * WIN)
        for b in range(6):
            cols = slice(b * WIN, (b + 1) * WIN)
            wide[rows, cols] = -expand(had[a][b])[:, :WIN]
            both = jnp.sum(source[a][b], axis=0, keepdims=True)
            if h[a][b] is not None:
                both = both + jnp.sum(expand(h[a][b]), axis=1, keepdims=True)
            matrix_ref[rows, cols] = jnp.where(eye, both, 0.0)[:, :WIN]
    high, low = gram_ref[0], gram_ref[1]
    wide[:size, :size] = wide[:size, :size] - low[:, :size]
    wide[:size, size : size + 1] = -(
        high[:, size : size + 1] + high[:, size + 1 : size + 2] + low[:, size : size + 1]
    )
    flipped = wide[...].T
    matrix_ref[:size, :size] = (
        matrix_ref[:size, :size] - high[:, :size] + wide[:size, :size] + flipped[:size, :size]
    )
    for j in range(6):
        cols = slice(j * WIN, (j + 1) * WIN)
        whole = jnp.sum(expand(r[j]), axis=1, keepdims=True)
        here = jnp.sum(jnp.where(eye, whole, 0.0), axis=0, keepdims=True)
        here = here - jnp.sum(lines[j], axis=0, keepdims=True)
        matrix_ref[size : size + 1, cols] = here[:, :WIN] + flipped[size : size + 1, cols]


def remote(src, dst, sems, phase, which, axis, peer):
    return pltpu.make_async_remote_copy(
        src_ref=src,
        dst_ref=dst,
        send_sem=sems.at[0, phase, which],
        recv_sem=sems.at[1, phase, which],
        device_id={axis: peer},
        device_id_type=pl.DeviceIdType.MESH,
    )


def peers(axis):
    count = lax.axis_size(axis)
    me = lax.axis_index(axis)
    return [lax.rem(me + step, count) for step in range(1, count)]


def pack(matrix_ref, packed_ref):
    size = 6 * WIN
    lane = iota((WIN, L), 1) % WIN
    row = iota((WIN, L), 0)
    inside = row + lane < WIN
    left = iota((BAND, L), 1) < L // 2
    packed_ref[...] = jnp.zeros_like(packed_ref)

    def skew(x):
        for bit in (1, 2, 4, 8, 16):
            x = jnp.where((lane & bit) != 0, pltpu.roll(x, WIN - bit, 0), x)
        return jnp.where(inside, x, 0.0)

    rest = []
    for j in range(6):
        rows = slice(j * WIN, (j + 1) * WIN)
        main = skew(matrix_ref[rows, :L])
        packed_ref[j * BAND : (j + 1) * BAND, :] = main[:BAND]
        packed_ref[6 * BAND + j : 6 * BAND + j + 1, :] = main[BAND : BAND + 1]
        rest.append(skew(matrix_ref[rows, L:]))
    base = 6 * BAND + 8
    for j in range(3):
        near = rest[j]
        far = pltpu.roll(rest[j + 3], L // 2, 1)
        packed_ref[base + j * BAND : base + (j + 1) * BAND, :] = jnp.where(left, near[:BAND], far[:BAND])
        at = base + 3 * BAND + j
        packed_ref[at : at + 1, :] = jnp.where(left[:1], near[BAND : BAND + 1], far[BAND : BAND + 1])
    packed_ref[6 * BAND + 6 : 6 * BAND + 7, :] = matrix_ref[size : size + 1, :L]
    packed_ref[base + 3 * BAND + 3 : base + 3 * BAND + 4, :] = jnp.where(
        left[:1], matrix_ref[size : size + 1, L:], 0.0
    )


def exchange(src, dst, sems, phase, axis):
    sent = []
    for peer in peers(axis):
        copy = remote(src(peer), dst, sems, phase, len(sent), axis, peer)
        copy.start()
        sent.append(copy)
    return sent


def operator(packed_ref, land, reduced_ref, gathered, diag_ref, ahead_ref, back_ref, far_ref, pix_sem, round_sem, f_dev, frames):
    zcount = lax.axis_size("pix")
    z = lax.axis_index("pix")
    count = lax.axis_size("frames")
    me = lax.axis_index("frames")
    chunk = land.shape[1]
    tiles = frames // L

    def piece(which):
        return pl.ds(pl.multiple_of(which * chunk, 8), chunk)

    sent = exchange(lambda peer: packed_ref.at[piece(peer)], land.at[z], pix_sem, 0, "pix")
    land[z] = packed_ref[piece(z), :]
    for copy in sent:
        copy.wait_recv()
    total = land[0]
    for k in range(1, zcount):
        total = total + land[k]
    reduced_ref[...] = total
    more = exchange(lambda peer: reduced_ref, gathered.at[me], round_sem, 0, "frames")
    gathered[me] = total
    for copy in more:
        copy.wait_recv()
    lane = iota((chunk, L), 1)
    sums = [[None] * tiles for _ in range(4)]
    for w in range(count):
        first = (w * f_dev - RADIUS) % frames
        start = first % L
        for k in range(4):
            part = pltpu.roll(gathered[w], (start - WIN * k) % L, 1)
            spans = [(first // L, start, min(start + WIN, L))]
            if start + WIN > L:
                spans.append(((first // L + 1) % tiles, 0, start + WIN - L))
            for tile, low, high in spans:
                term = jnp.where((lane >= low) & (lane < high), part, 0.0)
                sums[k][tile] = term if sums[k][tile] is None else sums[k][tile] + term
    for k in range(4):
        for tile in range(tiles):
            diag_ref[z, k, :, tile * L : (tile + 1) * L] = sums[k][tile]
    for copy in sent + more:
        copy.wait_send()
    sent = exchange(lambda peer: diag_ref.at[z], diag_ref.at[z], pix_sem, 1, "pix")
    for copy in sent:
        copy.wait_recv()
    for copy in sent:
        copy.wait_send()

    def block(k, at):
        return [
            diag_ref[at // chunk, k, at % chunk : at % chunk + 8, t * L : (t + 1) * L]
            for t in range(tiles)
        ]

    def entry(i, j, half):
        if i < 4:
            return block(i, BAND * j + 8 * half)
        return block(i - 4 + 2 * (j // 3), 6 * BAND + 8 + BAND * (j % 3) + 8 * half)

    row = iota((8, L), 0)
    lanes = iota((8, L), 1)

    def later(x, half):
        turned = [pltpu.roll(v, 8 * half, 1, stride=1, stride_axis=0) for v in x]
        if tiles == 1:
            return turned
        mine = lanes >= 8 * half + row
        return [jnp.where(mine, turned[t], turned[t - 1]) for t in range(tiles)]

    def flip(x):
        for bit in (4, 2, 1):
            x = jnp.where((row & bit) != 0, pltpu.roll(x, bit, 0), pltpu.roll(x, 8 - bit, 0))
        return x

    for i in range(6):
        for j in range(6):
            for half in range(2):
                front = entry(i, j, half)
                moved = later(entry(j, i, half), half)
                for t in range(tiles):
                    ahead_ref[i, 2 * j + half, :, t * L : (t + 1) * L] = flip(front[t])
                    value = jnp.where(row > 0, moved[t], 0.0) if half == 0 else moved[t]
                    back_ref[i, 2 * j + half, :, t * L : (t + 1) * L] = value
    edge = 6 * BAND
    last = edge + 8 + 3 * BAND
    for i in range(6):
        if i < 4:
            ends = block(i, edge)
        else:
            near, far = block(i - 4, last), block(i - 2, last)
            ends = [jnp.where(row < 3, a, pltpu.roll(b, 3, 0)) for a, b in zip(near, far)]
        for t in range(tiles):
            far_ref[i, :, t * L : (t + 1) * L] = jnp.where(row < 6, ends[t], 0.0)
    sources = [block(k, edge) for k in range(4)] + [block(k, last) for k in range(2)]
    rhs = []
    for t in range(tiles):
        out = jnp.zeros((8, L), F32)
        for i in range(6):
            at = 6 if i < 4 else 3
            out = jnp.where(row == i, sources[i][t][at : at + 1, :], out)
        rhs.append(out)
    return rhs, later


def conjugate(rhs, later, ahead_ref, back_ref, far_ref):
    tiles = len(rhs)
    row = iota((8, L), 0)
    lanes = iota((8, L), 1)

    def sooner(x, half):
        turned = [pltpu.roll(v, L - 8 * half - 7, 1, stride=1, stride_axis=0) for v in x]
        if tiles == 1:
            return turned
        mine = lanes + 8 * half + 7 - row < L
        return [jnp.where(mine, turned[t], turned[(t + 1) % tiles]) for t in range(tiles)]

    def moved(x, steps):
        turned = [pltpu.roll(v, steps % L, 1) for v in x]
        if tiles == 1:
            return turned
        if steps > 0:
            return [jnp.where(lanes >= steps, turned[t], turned[t - 1]) for t in range(tiles)]
        return [jnp.where(lanes < L + steps, turned[t], turned[(t + 1) % tiles]) for t in range(tiles)]

    def dot(x, y):
        total = x[0] * y[0]
        for t in range(1, tiles):
            total = total + x[t] * y[t]
        return jnp.sum(total, keepdims=True)

    def product(p):
        ahead = moved(p, -BAND)
        acc = [[far_ref[i, :, t * L : (t + 1) * L] * ahead[t] for t in range(tiles)] for i in range(6)]
        tail = [None] * tiles
        for j in range(6):
            wide = [jnp.broadcast_to(v[j : j + 1, :], (8, L)) for v in p]
            for t in range(tiles):
                term = far_ref[j, :, t * L : (t + 1) * L] * wide[t]
                tail[t] = term if tail[t] is None else tail[t] + term
            for half in range(2):
                plus = sooner(wide, half)
                minus = later(wide, half)
                for i in range(6):
                    for t in range(tiles):
                        acc[i][t] = (
                            acc[i][t]
                            + ahead_ref[i, 2 * j + half, :, t * L : (t + 1) * L] * plus[t]
                            + back_ref[i, 2 * j + half, :, t * L : (t + 1) * L] * minus[t]
                        )
        tail = moved(tail, BAND)
        out = []
        for t in range(tiles):
            y = tail[t] + REG * p[t]
            for i in range(6):
                y = y + jnp.where(row == i, jnp.sum(acc[i][t], axis=0, keepdims=True), 0.0)
            out.append(y)
        return out

    def step(_, carry):
        x, residual, direction, rr = carry
        image = product(direction)
        alpha = rr / dot(direction, image)
        x = [a + alpha * b for a, b in zip(x, direction)]
        residual = [a - alpha * b for a, b in zip(residual, image)]
        new = dot(residual, residual)
        beta = new / rr
        direction = [a + beta * b for a, b in zip(residual, direction)]
        return x, residual, direction, new

    zero = [jnp.zeros((8, L), F32)] * tiles
    return lax.fori_loop(0, ITERS, step, (zero, rhs, rhs, dot(rhs, rhs)))[0]


def finish(
    matrix_ref, e_ref, base_ref, inv_ref, pose_ref, step_ref, frames,
    cols_ref, step3, packed_ref, land, reduced_ref, gathered, diag_ref, ahead_ref, back_ref, far_ref, x_ref,
    pix_sem, round_sem,
):
    me = lax.axis_index("frames")
    tiles, f_dev = step3.shape[:2]
    half = f_dev // 2
    pack(matrix_ref, packed_ref)
    rhs, later = operator(
        packed_ref, land, reduced_ref, gathered, diag_ref, ahead_ref, back_ref, far_ref,
        pix_sem, round_sem, f_dev, frames,
    )
    x = conjugate(rhs, later, ahead_ref, back_ref, far_ref)
    for t, value in enumerate(x):
        x_ref[:, t * L : (t + 1) * L] = value
    mine = window(lambda at: x_ref[:, at], me, f_dev, frames)
    pose_ref[...] = mine[:6, RADIUS : RADIUS + f_dev]
    turned = spread_rows(mine)
    for i in range(6):
        cols_ref[i] = jnp.broadcast_to(turned[:WIN, i : i + 1], (WIN, L))
    row = iota((8, L), 0)
    lane = iota((8, L), 1)
    for part in range(2):

        @pl.loop(0, half)
        def per_source(i):
            s = i + part * half
            group = [[cols_ref[j, 8 * g : 8 * g + 8, :] for g in range(part, part + 3)] for j in range(6)]
            below = [jnp.where(row >= i, group[j][0], group[j][1]) for j in range(6)]
            over = [jnp.where(row > i, group[j][1], group[j][2]) for j in range(6)]
            near, far = (over, below) if part == 0 else (below, over)
            at = jnp.sum(jnp.where(lane == s + RADIUS, mine, 0.0), axis=1, keepdims=True)
            terms = near + far + [jnp.broadcast_to(at, (8, L))]
            for tile in range(tiles):
                slot = s * tiles + tile
                image = e_ref[slot, 0] * terms[0]
                for n in range(1, 13):
                    image = image + e_ref[slot, n] * terms[n]
                image = jnp.sum(image, axis=0, keepdims=True)
                here = (tile, pl.ds(s, 1), slice(None))
                step3[here] = base_ref[here] - inv_ref[here] * image

    for tile in range(tiles):
        step_ref[:, tile * L : (tile + 1) * L] = step3[tile]


def swap_edges(low_out, high_out, low_ref, high_ref, sems):
    count = lax.axis_size("frames")
    me = lax.axis_index("frames")
    below = lax.rem(me + count - 1, count)
    over = lax.rem(me + 1, count)
    tiles = low_out.shape[0]
    down = [remote(low_out.at[t, :, :SENT], low_ref.at[t, :, :SENT], sems, 0, t, "frames", below) for t in range(tiles)]
    up = [remote(high_out.at[t, :, :SENT], high_ref.at[t, :, :SENT], sems, 1, t, "frames", over) for t in range(tiles)]

    @pl.when(me < count - 1)
    def _():
        for copy in up:
            copy.start()

    def descend():
        @pl.when(me > 0)
        def _():
            for copy in down:
                copy.start()

    def receive(part):
        if part == 0:

            @pl.when(me > 0)
            def _():
                for copy in up:
                    copy.wait_recv()

            @pl.when(me == 0)
            def _():
                high_ref[...] = jnp.zeros_like(high_ref)

        else:

            @pl.when(me < count - 1)
            def _():
                for copy in down:
                    copy.wait_recv()

            @pl.when(me == count - 1)
            def _():
                low_ref[...] = jnp.zeros_like(low_ref)

    def drain():
        @pl.when(me > 0)
        def _():
            for copy in down:
                copy.wait_send()

        @pl.when(me < count - 1)
        def _():
            for copy in up:
                copy.wait_send()

    return descend, receive, drain


def solve(
    edge_ref, rot_ref, trans_ref, depth_ref, damp_ref, flow_ref, weight_ref, mask_ref,
    x_ref, step_ref, flow3, weight3, mask3, load_sem, pose_ref,
    own_ref, low_out, high_out, low_ref, high_ref, edge_sem,
    frame_ref, coord_ref, depth3, damp3, e_ref, part_ref, near_sum, near_pair, far_sum, far_pair,
    base_ref, inv_ref, zh0, zl0, zh1, zl1, gram_ref, matrix_ref, wide, *scratch,
):
    me = lax.axis_index("frames")
    f_dev, pix = depth_ref.shape
    frames = rot_ref.shape[1]
    loads = fetch(flow_ref, weight_ref, mask_ref, flow3, weight3, mask3, load_sem)
    barrier = pltpu.get_barrier_semaphore()
    total = 0
    for axis in ("frames", "pix"):
        for peer in peers(axis):
            pl.semaphore_signal(
                barrier, inc=1, device_id={axis: peer}, device_id_type=pl.DeviceIdType.MESH
            )
            total += 1
    poses = []
    for ref in (rot_ref, trans_ref):
        poses.append(window(lambda at: ref[:, at], me, f_dev, frames))
    turned = spread_rows(jnp.concatenate(poses, axis=0))
    for k in range(6):
        pose_ref[k] = jnp.broadcast_to(turned[:WIN, k : k + 1], (WIN, L))
    prepare(pose_ref, frame_ref, coord_ref, depth_ref, damp_ref, depth3, damp3)
    aggregate(edge_ref, loads, flow3, weight3, mask3, own_ref, low_out, high_out, me, f_dev)
    pl.semaphore_wait(barrier, total)
    descend, receive, drain = swap_edges(low_out, high_out, low_ref, high_ref, edge_sem)
    near_pairs(own_ref, frame_ref, coord_ref, depth3, e_ref, part_ref, near_sum, near_pair, descend)
    far_pairs(
        own_ref, low_ref, high_ref, frame_ref, coord_ref, depth3, damp3, e_ref, part_ref,
        far_sum, far_pair, base_ref, inv_ref, (zh0, zl0, zh1, zl1), gram_ref, receive,
    )
    assemble(near_sum, near_pair, far_sum, far_pair, gram_ref, matrix_ref, wide)
    finish(matrix_ref, e_ref, base_ref, inv_ref, x_ref, step_ref, frames, *scratch)
    drain()


def call(body, out, scratch, vmem, hbm, **params):
    vm = pl.BlockSpec(memory_space=pltpu.VMEM)
    far = pl.BlockSpec(memory_space=pl.ANY)
    return pl.pallas_call(
        body,
        out_shape=[jax.ShapeDtypeStruct(s, t) for s, t in out],
        in_specs=[vm] * vmem + [far] * hbm,
        out_specs=[vm] * len(out),
        scratch_shapes=scratch,
        compiler_params=pltpu.CompilerParams(vmem_limit_bytes=VMEM_LIMIT, **params),
    )


def per_device(edge_frames, rotvec, trans, inv_depth, depth_damping, flow, weight, mask):
    f_dev, pix = inv_depth.shape
    edges = mask.shape[0]
    frames = rotvec.shape[1]
    tiles = pix // L
    own_rows = f_dev * 16
    side = 40
    sums = len(UPPER) + 6
    width = 256
    size = 6 * WIN
    count = lax.axis_size("frames")
    zcount = lax.axis_size("pix")
    chunk = -(-PACKED // (8 * zcount)) * 8
    x, step = call(
        solve,
        [((6, f_dev), F32), ((f_dev, pix), F32)],
        [
            pltpu.VMEM((tiles, 2, edges, L), F32),
            pltpu.VMEM((tiles, 2, edges, L), F32),
            pltpu.VMEM((tiles, edges, L), jnp.int32),
            pltpu.SemaphoreType.DMA((tiles, 5)),
            pltpu.VMEM((6, WIN, L), F32),
            pltpu.VMEM((4, own_rows, pix), F32),
            pltpu.VMEM((tiles, 4, side, L), F32),
            pltpu.VMEM((tiles, 4, side, L), F32),
            pltpu.VMEM((tiles, 4, side, L), F32),
            pltpu.VMEM((tiles, 4, side, L), F32),
            pltpu.SemaphoreType.DMA((2, 2, tiles)),
            pltpu.VMEM((12, WIN, L), F32),
            pltpu.VMEM((tiles, 2, 8, L), F32),
            pltpu.VMEM((tiles, f_dev, L), F32),
            pltpu.VMEM((tiles, f_dev, L), F32),
            pltpu.VMEM((f_dev * tiles, 13, 8, L), F32),
            pltpu.VMEM((f_dev * tiles, 3, 8, L), F32),
            pltpu.VMEM((sums, 8, L), F32),
            pltpu.VMEM((12, 8, L), F32),
            pltpu.VMEM((sums, 8, L), F32),
            pltpu.VMEM((12, 8, L), F32),
            pltpu.VMEM((tiles, f_dev, L), F32),
            pltpu.VMEM((tiles, f_dev, L), F32),
            pltpu.VMEM((size + 16, pix), BF16),
            pltpu.VMEM((size, pix), BF16),
            pltpu.VMEM((size + 16, pix), BF16),
            pltpu.VMEM((size, pix), BF16),
            pltpu.VMEM((2, size, size + 16), F32),
            pltpu.VMEM((size + 8, width), F32),
            pltpu.VMEM((256, 256), F32),
            pltpu.VMEM((6, WIN, L), F32),
            pltpu.VMEM((tiles, f_dev, L), F32),
            pltpu.VMEM((chunk * zcount, L), F32),
            pltpu.VMEM((zcount, chunk, L), F32),
            pltpu.VMEM((chunk, L), F32),
            pltpu.VMEM((count, chunk, L), F32),
            pltpu.VMEM((zcount, 4, chunk, frames), F32),
            pltpu.VMEM((6, 12, 8, frames), F32),
            pltpu.VMEM((6, 12, 8, frames), F32),
            pltpu.VMEM((6, 8, frames), F32),
            pltpu.VMEM((8, frames), F32),
            pltpu.SemaphoreType.DMA((2, 2, zcount)),
            pltpu.SemaphoreType.DMA((2, 1, count)),
        ],
        5, 3, collective_id=0, has_side_effects=True,
    )(edge_frames, rotvec, trans, inv_depth, depth_damping, flow, weight, mask)
    return x, step


def solution(mesh):
    return jax.shard_map(
        per_device,
        mesh=mesh,
        in_specs=(
            P(None, "frames"),
            P(),
            P(),
            P("frames", "pix"),
            P("frames", "pix"),
            P("frames", None, "pix"),
            P("frames", None, "pix"),
            P("frames", "pix"),
        ),
        out_specs=(P(None, "frames"), P("frames", "pix")),
        check_vma=False,
    )
```

```python
import jax
import jax.numpy as jnp
from jax import lax
from jax.experimental import pallas as pl
from jax.experimental.pallas import tpu as pltpu
from jax.sharding import PartitionSpec as P

ROWS = 48
COLS = 64
RADIUS = 8
ITERS = 6
REG = 100.0
F32 = jnp.float32
BF16 = jnp.bfloat16
L = 128
WIN = 32
BAND = 2 * RADIUS
PACKED = 160
SENT = RADIUS * (RADIUS + 1) // 2
VMEM_LIMIT = 60 * 1024 * 1024
UPPER = [(i, j) for i in range(6) for j in range(i, 6) if (i, j) != (0, 1)]


def split(x):
    high = x.astype(BF16)
    return high, (x - high.astype(F32)).astype(BF16)


def iota(shape, dim):
    return lax.broadcasted_iota(jnp.int32, shape, dim)


def destinations(edge_ref, own_rows, side, f_dev, me):
    start = me * f_dev
    source = edge_ref[0:1, :] - start + RADIUS
    target = edge_ref[1:2, :] - start + RADIUS
    s = source - RADIUS
    low = jnp.where(s < f_dev // 2, 1, 0)
    above = jnp.where(target > source, 1, 0)
    mine = jnp.where(low == above, 0, f_dev * 8) + s * 8 + (target & 7)
    q = target - RADIUS
    tile = jnp.where(source < 3, source, jnp.where(source == 3, 4, jnp.where(source == 7, 3, 6 - source)))
    line = jnp.where((source > 3) & (source < 7), q + 7 - source, q)
    lowest = own_rows + tile * 8 + line
    i = source - f_dev - RADIUS
    q = target - f_dev
    tile = jnp.where(i == 0, 3, jnp.where(i < 4, i - 1, jnp.where(i == 4, 4, 7 - i)))
    line = jnp.where(i >= 4, q - i, q)
    highest = own_rows + side + tile * 8 + line
    return jnp.where(source < RADIUS, lowest, jnp.where(source >= RADIUS + f_dev, highest, mine))


def fetch(flow_ref, weight_ref, mask_ref, flow3, weight3, mask3, sems):
    out = []
    for tile in range(flow3.shape[0]):
        cols = pl.ds(tile * L, L)
        pairs = [(mask_ref.at[:, cols], mask3.at[tile])]
        for comp in range(2):
            pairs.append((weight_ref.at[:, comp, cols], weight3.at[tile, comp]))
            pairs.append((flow_ref.at[:, comp, cols], flow3.at[tile, comp]))
        copies = [pltpu.make_async_copy(a, b, sems.at[tile, n]) for n, (a, b) in enumerate(pairs)]
        for copy in copies:
            copy.start()
        out.append(copies)
    return out


def aggregate(edge_ref, loads, flow3, weight3, mask3, own_ref, low_ref, high_ref, me, f_dev):
    edges = edge_ref.shape[1]
    own = own_ref.shape[1]
    side = low_ref.shape[2]
    rows = own + 2 * side
    dest = destinations(edge_ref, own, side, f_dev, me)
    pick = (iota((rows, edges), 0) == dest).astype(F32).astype(BF16)
    for tile, copies in enumerate(loads):
        cols = slice(tile * L, (tile + 1) * L)
        for copy in copies:
            copy.wait()
        live = mask3[tile].astype(F32)
        fields = []
        for comp in range(2):
            conf = weight3[tile, comp] * live
            fields += [conf, conf * flow3[tile, comp]]
        high, low = split(jnp.concatenate(fields, axis=1))
        out = jnp.dot(pick, high, preferred_element_type=F32) + jnp.dot(
            pick, low, preferred_element_type=F32
        )
        for field in range(4):
            part = out[:, field * L : (field + 1) * L]
            own_ref[field, :, cols] = part[:own]
            low_ref[tile, field] = part[own : own + side]
            high_ref[tile, field] = part[own + side :]


def window(load, me, f_dev, frames):
    tiles = frames // L
    first = lax.rem(me * f_dev - RADIUS + frames, frames)
    tile = first // L
    back = lax.rem(L - lax.rem(first, L), L)
    near = pltpu.roll(load(pl.ds(pl.multiple_of(tile * L, L), L)), back, 1)
    if tiles == 1:
        return near
    after = lax.rem(tile + 1, tiles)
    far = pltpu.roll(load(pl.ds(pl.multiple_of(after * L, L), L)), back, 1)
    return jnp.where(iota(near.shape, 1) + lax.rem(first, L) < L, near, far)


def spread_rows(x):
    return jnp.concatenate([x, jnp.zeros((L - x.shape[0], L), F32)], axis=0).T


def motion_sums(u, v, uu, vv, a, b, ds):
    va, ub = v * a, u * b
    e0, e1 = ds * a, ds * b
    return [e0, e1, -(u * e0 + v * e1), -(u * va + vv * b), uu * a + v * ub, ub - va]


def curvature_sums(u, v, uu, vv, uv, ds, wu, wv):
    a1, b1 = wu * v, wv * u
    a2, b2 = a1 * u, b1 * v
    a3, b3 = wu * uu, wv * vv
    h00, h11 = wu * ds * ds, wv * ds * ds
    h02, h12 = h00 * u, h11 * v
    x1, x2, x3 = ds * a1, ds * a2, ds * a3
    y1, y2, y3 = ds * b1, ds * b2, ds * b3
    return [
        h00, h02, x2, x3, x1,
        h11, h12, y3, y2, y1,
        h02 * u + h12 * v, u * x2 + v * y3, u * x3 + v * y2, u * x1 - v * y1,
        a2 * uv + b3 * vv, a2 * uu + b3 * uv, a2 * v - b3 * u,
        a3 * uu + b2 * uv, b2 * u - a3 * v,
        a1 * v + b1 * u,
    ]


SIGNS = [1, -1, -1, 1, -1, 1, -1, -1, 1, 1, 1, 1, -1, 1, 1, -1, 1, 1, 1, 1]


def adj_t(rel, tr, vec):
    turn = [
        vec[3] - (tr[1] * vec[2] - tr[2] * vec[1]),
        vec[4] - (tr[2] * vec[0] - tr[0] * vec[2]),
        vec[5] - (tr[0] * vec[1] - tr[1] * vec[0]),
    ]
    out = [rel[j] * vec[0] + rel[3 + j] * vec[1] + rel[6 + j] * vec[2] for j in range(3)]
    return out + [rel[j] * turn[0] + rel[3 + j] * turn[1] + rel[6 + j] * turn[2] for j in range(3)]


def fold(x):
    row = iota((8, L), 0)

    def merge(a, b, bit):
        other = (row & bit) != 0
        return jnp.where(other, b, a) + pltpu.roll(jnp.where(other, a, b), bit, 0)

    first, second, third = merge(x[0], x[1], 1), merge(x[2], x[3], 1), merge(x[4], x[5], 1)
    return merge(merge(first, second, 2), third + pltpu.roll(third, 2, 0), 4)


def pair_pose(frame_ref, s, first, after):
    here = [frame_ref[k, pl.ds(s + RADIUS, 1), :] for k in range(12)]
    there = [
        jnp.where(after, frame_ref[k, first : first + 8, :], frame_ref[k, first + 8 : first + 16, :])
        for k in range(12)
    ]
    rel = [
        there[3 * r] * here[3 * c] + there[3 * r + 1] * here[3 * c + 1] + there[3 * r + 2] * here[3 * c + 2]
        for r in range(3)
        for c in range(3)
    ]
    tr = [
        there[9 + r] - (rel[3 * r] * here[9] + rel[3 * r + 1] * here[10] + rel[3 * r + 2] * here[11])
        for r in range(3)
    ]
    return rel, tr


def octet(fields, depth, col, rowc, rel, tr):
    wu, fu, wv, fv = fields
    point = [
        rel[3 * k] * col + rel[3 * k + 1] * rowc + rel[3 * k + 2] + depth * tr[k] for k in range(3)
    ]
    iz = 1.0 / point[2]
    u = point[0] * iz
    v = point[1] * iz
    ds = depth * iz
    su = iz * (tr[0] - u * tr[2])
    sv = iz * (tr[1] - v * tr[2])
    au = wu * su
    av = wv * sv
    gu = wu * (col - u) + fu
    gv = wv * (rowc - v) + fv
    uu = 1.0 + u * u
    vv = 1.0 + v * v
    uv = u * v
    e = motion_sums(u, v, uu, vv, au, av, ds)
    back = fold(adj_t(rel, tr, e))
    sums = curvature_sums(u, v, uu, vv, uv, ds, wu, wv) + motion_sums(u, v, uu, vv, gu, gv, ds)
    return e, back, au * su + av * sv, su * gu + sv * gv, sums


def prepare(pose_ref, frame_ref, coord_ref, depth_ref, damp_ref, depth3, damp3):
    tiles = depth3.shape[0]
    ox, oy, oz = pose_ref[0], pose_ref[1], pose_ref[2]
    zero = jnp.zeros_like(ox)
    cross = [[zero, -oz, oy], [oz, zero, -ox], [-oy, ox, zero]]
    sq = ox * ox + oy * oy + oz * oz
    c1 = 1.0 - sq / 6.0 + sq * sq / 120.0
    c2 = 0.5 - sq / 24.0 + sq * sq / 720.0
    for r in range(3):
        for c in range(3):
            square = cross[r][0] * cross[0][c] + cross[r][1] * cross[1][c] + cross[r][2] * cross[2][c]
            frame_ref[3 * r + c] = float(r == c) + c1 * cross[r][c] + c2 * square
        frame_ref[9 + r] = pose_ref[3 + r]
    first = lax.axis_index("pix") * (tiles * L)
    for tile in range(tiles):
        depth3[tile] = depth_ref[:, tile * L : (tile + 1) * L]
        damp3[tile] = damp_ref[:, tile * L : (tile + 1) * L]
        pixel = first + tile * L + iota((8, L), 1)
        prow = pixel // COLS
        pcol = pixel - prow * COLS
        coord_ref[tile, 0] = (pcol.astype(F32) - 0.5 * (COLS - 1)) / COLS
        coord_ref[tile, 1] = (prow.astype(F32) - 0.5 * (ROWS - 1)) / COLS


def note(at, sums, pose, sum_ref, pair_ref):
    for n, x in enumerate(sums):
        sum_ref[n] = jnp.where(at, jnp.sum(x, axis=1, keepdims=True), sum_ref[n])
    for n, x in enumerate(pose):
        pair_ref[n] = jnp.where(at, x, pair_ref[n])


def near_pairs(own_ref, frame_ref, coord_ref, depth3, e_ref, part_ref, sum_ref, pair_ref, descend):
    tiles, f_dev = depth3.shape[:2]
    half = f_dev // 2
    row = iota((8, L), 0)
    lane = iota((8, L), 1)
    sum_ref[...] = jnp.zeros_like(sum_ref)
    pair_ref[...] = jnp.zeros_like(pair_ref)
    for part in range(2):

        @pl.loop(0, half)
        def per_source(i):
            s = i + part * half
            rel, tr = pair_pose(frame_ref, s, 8, row > i if part == 0 else row >= i)
            sums = None
            for tile in range(tiles):
                cols = slice(tile * L, (tile + 1) * L)
                at = pl.ds(pl.multiple_of(s * 8, 8), 8)
                fields = [own_ref[k, at, cols] for k in range(4)]
                e, back, curv, grad, new = octet(
                    fields, depth3[tile, pl.ds(s, 1), :], coord_ref[tile, 0], coord_ref[tile, 1], rel, tr
                )
                slot = s * tiles + tile
                for j in range(6):
                    e_ref[slot, j] = e[j]
                part_ref[slot, 0] = back
                part_ref[slot, 1] = curv
                part_ref[slot, 2] = grad
                sums = new if sums is None else [a + b for a, b in zip(sums, new)]
            note(lane == s + RADIUS, sums, rel + tr, sum_ref, pair_ref)

        if part == 1:
            descend()


def far_pairs(
    own_ref, low_ref, high_ref, frame_ref, coord_ref, depth3, damp3, e_ref, part_ref, sum_ref, pair_ref,
    base_ref, inv_ref, zs, gram_ref, receive,
):
    tiles, f_dev = depth3.shape[:2]
    half = f_dev // 2
    row = iota((8, L), 0)
    lane = iota((8, L), 1)
    pair = iota((16, L), 0)
    size = 6 * WIN
    sum_ref[...] = jnp.zeros_like(sum_ref)
    pair_ref[...] = jnp.zeros_like(pair_ref)
    gram_ref[...] = jnp.zeros_like(gram_ref)
    zs[1][...] = jnp.zeros_like(zs[1])
    none = jnp.zeros((8, L), F32)

    def gram(which):
        z = zs[which][...]
        nt = (((1,), (1,)), ((), ()))
        gram_ref[...] += lax.dot_general(z, z[: size + 16], nt, preferred_element_type=F32)

    for part in range(2):
        receive(part)

        def per_source(i, which):
            s = i + part * half
            after = row >= i if part == 0 else row > i
            rel, tr = pair_pose(frame_ref, s, 0 if part == 0 else 16, after)
            if part == 0:
                slot = jnp.where(i == 0, 3, jnp.where(i < 4, i - 1, jnp.where(i == 4, 4, 7 - i)))
                shift = jnp.where(i >= 4, i, 0)
                keep = row >= i
                src = high_ref
            else:
                slot = jnp.where(i < 3, i, jnp.where(i == 3, 4, jnp.where(i == 7, 3, 6 - i)))
                shift = jnp.where((i > 3) & (i < 7), i + 1, 0)
                keep = row <= i
                src = low_ref
            sums = None
            for tile in range(tiles):
                cols = slice(tile * L, (tile + 1) * L)
                at = pl.ds(pl.multiple_of(f_dev * 8 + s * 8, 8), 8)
                fields = []
                for k in range(4):
                    got = src[tile, k, pl.ds(pl.multiple_of(slot * 8, 8), 8), :]
                    fields.append(jnp.where(keep, pltpu.roll(got, shift, 0), own_ref[k, at, cols]))
                e, back, curv, grad, new = octet(
                    fields, depth3[tile, pl.ds(s, 1), :], coord_ref[tile, 0], coord_ref[tile, 1], rel, tr
                )
                sums = new if sums is None else [a + b for a, b in zip(sums, new)]
                here = s * tiles + tile
                for j in range(6):
                    e_ref[here, 6 + j] = e[j]
                back = -(back + part_ref[here, 0])
                e_ref[here, 12] = back
                curv = jnp.sum(curv + part_ref[here, 1], axis=0, keepdims=True) + damp3[tile, pl.ds(s, 1), :]
                grad = -jnp.sum(grad + part_ref[here, 2], axis=0, keepdims=True)
                inv = 1.0 / curv
                scale = 1.0 / jnp.sqrt(curv)
                base_ref[tile, pl.ds(s, 1), :] = grad * inv
                inv_ref[tile, pl.ds(s, 1), :] = inv
                z = zs[which]
                skip = size + 16
                source = back * scale
                for j in range(6):
                    mine = e[j] * scale
                    other = e_ref[here, j] * scale
                    below, over = (mine, other) if part == 0 else (other, mine)
                    mid = jnp.where(row < i, below, jnp.where(row > i, over, source[j : j + 1, :]))
                    groups = [jnp.where(row >= i, below, 0.0), mid, jnp.where(row <= i, over, 0.0)]
                    groups = groups + [none] if part == 0 else [none] + groups
                    high, low = split(jnp.concatenate(groups, axis=0))
                    z[j * WIN : (j + 1) * WIN, cols] = high
                    z[skip + j * WIN : skip + (j + 1) * WIN, cols] = low
                y = grad * scale
                rest = y - y.astype(BF16).astype(F32)
                lines = jnp.where(pair == 0, y, jnp.where(pair == 1, rest, 0.0))
                z[size : size + 16, cols] = lines.astype(BF16)
            note(lane == s + RADIUS, sums, rel + tr, sum_ref, pair_ref)

        @pl.loop(0, half // 2)
        def per_two(k):
            gram(1)
            per_source(2 * k, 0)
            gram(0)
            per_source(2 * k + 1, 1)

    gram(1)


def assemble(near_sum, near_pair, far_sum, far_pair, gram_ref, matrix_ref, wide):
    size = 6 * WIN
    row = iota((8, L), 0)
    lane = iota((8, L), 1)
    i = lane & 7
    first = lane < 16

    def sides(near, far):
        return jnp.where(first, far, near), jnp.where(first, near, far)

    def expand(x):
        low, high = x
        mid = jnp.where(row < i, low, jnp.where(row > i, high, 0.0))
        start = jnp.where(row >= i, low, 0.0)
        end = jnp.where(row <= i, high, 0.0)
        return jnp.concatenate(
            [
                jnp.where(first, start, 0.0),
                jnp.where(first, mid, start),
                jnp.where(first, end, mid),
                jnp.where(first, 0.0, end),
            ],
            axis=0,
        )

    pose = [sides(near_pair[k], far_pair[k]) for k in range(12)]
    h = [[None] * 6 for _ in range(6)]
    wholes = [[None] * 6 for _ in range(6)]
    for n, (a, b) in enumerate(UPPER):
        pair = sides(near_sum[n], far_sum[n])
        h[a][b] = h[b][a] = pair if SIGNS[n] > 0 else tuple(-x for x in pair)
    count = len(UPPER)
    r = [tuple(-x for x in sides(near_sum[count + j], far_sum[count + j])) for j in range(6)]
    eye = iota((WIN, L), 0) == iota((WIN, L), 1)

    def total(terms):
        out = None
        for x, y in terms:
            if x is None or y is None:
                continue
            out = x * y if out is None else out + x * y
        return out

    had = [[[None, None] for _ in range(6)] for _ in range(6)]
    source = [[0.0] * 6 for _ in range(6)]
    lines = [0.0] * 6
    for side in range(2):
        rel = [pose[k][side] for k in range(9)]
        tr = [pose[9 + k][side] for k in range(3)]
        ad = [[None] * 6 for _ in range(6)]
        for c in range(3):
            corner = [
                tr[1] * rel[6 + c] - tr[2] * rel[3 + c],
                tr[2] * rel[c] - tr[0] * rel[6 + c],
                tr[0] * rel[3 + c] - tr[1] * rel[c],
            ]
            for a in range(3):
                ad[a][c] = ad[3 + a][3 + c] = rel[3 * a + c]
                ad[a][3 + c] = corner[a]
        for a in range(6):
            for b in range(6):
                had[a][b][side] = total(
                    [(None if h[a][k] is None else h[a][k][side], ad[k][b]) for k in range(6)]
                )
        for a in range(6):
            for b in range(6):
                source[a][b] = source[a][b] + total([(ad[k][a], had[k][b][side]) for k in range(6)])
        back = adj_t(rel, tr, [x[side] for x in r])
        lines = [x + y for x, y in zip(lines, back)]
    wide[...] = jnp.zeros_like(wide)
    matrix_ref[...] = jnp.zeros_like(matrix_ref)
    for a in range(6):
        rows = slice(a * WIN, (a + 1) * WIN)
        for b in range(6):
            cols = slice(b * WIN, (b + 1) * WIN)
            wide[rows, cols] = -expand(had[a][b])[:, :WIN]
            both = jnp.sum(source[a][b], axis=0, keepdims=True)
            if h[a][b] is not None:
                both = both + jnp.sum(expand(h[a][b]), axis=1, keepdims=True)
            matrix_ref[rows, cols] = jnp.where(eye, both, 0.0)[:, :WIN]
    high, low = gram_ref[:size, :], gram_ref[size + 16 :, :]
    wide[:size, :size] = wide[:size, :size] - low[:, :size]
    wide[:size, size : size + 1] = -(
        high[:, size : size + 1] + high[:, size + 1 : size + 2] + low[:, size : size + 1]
    )
    flipped = wide[...].T
    matrix_ref[:size, :size] = (
        matrix_ref[:size, :size] - high[:, :size] + wide[:size, :size] + flipped[:size, :size]
    )
    for j in range(6):
        cols = slice(j * WIN, (j + 1) * WIN)
        whole = jnp.sum(expand(r[j]), axis=1, keepdims=True)
        here = jnp.sum(jnp.where(eye, whole, 0.0), axis=0, keepdims=True)
        here = here - jnp.sum(lines[j], axis=0, keepdims=True)
        matrix_ref[size : size + 1, cols] = here[:, :WIN] + flipped[size : size + 1, cols]


def remote(src, dst, sems, phase, which, axis, peer):
    return pltpu.make_async_remote_copy(
        src_ref=src,
        dst_ref=dst,
        send_sem=sems.at[0, phase, which],
        recv_sem=sems.at[1, phase, which],
        device_id={axis: peer},
        device_id_type=pl.DeviceIdType.MESH,
    )


def peers(axis):
    count = lax.axis_size(axis)
    me = lax.axis_index(axis)
    return [lax.rem(me + step, count) for step in range(1, count)]


def pack(matrix_ref, packed_ref):
    size = 6 * WIN
    lane = iota((WIN, L), 1) % WIN
    row = iota((WIN, L), 0)
    inside = row + lane < WIN
    left = iota((BAND, L), 1) < L // 2
    packed_ref[...] = jnp.zeros_like(packed_ref)

    def skew(x):
        for bit in (1, 2, 4, 8, 16):
            x = jnp.where((lane & bit) != 0, pltpu.roll(x, WIN - bit, 0), x)
        return jnp.where(inside, x, 0.0)

    rest = []
    for j in range(6):
        rows = slice(j * WIN, (j + 1) * WIN)
        main = skew(matrix_ref[rows, :L])
        packed_ref[j * BAND : (j + 1) * BAND, :] = main[:BAND]
        packed_ref[6 * BAND + j : 6 * BAND + j + 1, :] = main[BAND : BAND + 1]
        rest.append(skew(matrix_ref[rows, L:]))
    base = 6 * BAND + 8
    for j in range(3):
        near = rest[j]
        far = pltpu.roll(rest[j + 3], L // 2, 1)
        packed_ref[base + j * BAND : base + (j + 1) * BAND, :] = jnp.where(left, near[:BAND], far[:BAND])
        at = base + 3 * BAND + j
        packed_ref[at : at + 1, :] = jnp.where(left[:1], near[BAND : BAND + 1], far[BAND : BAND + 1])
    packed_ref[6 * BAND + 6 : 6 * BAND + 7, :] = matrix_ref[size : size + 1, :L]
    packed_ref[base + 3 * BAND + 3 : base + 3 * BAND + 4, :] = jnp.where(
        left[:1], matrix_ref[size : size + 1, L:], 0.0
    )


def exchange(src, dst, sems, phase, axis):
    sent = []
    for peer in peers(axis):
        copy = remote(src(peer), dst, sems, phase, len(sent), axis, peer)
        copy.start()
        sent.append(copy)
    return sent


def operator(packed_ref, land, reduced_ref, gathered, diag_ref, ahead_ref, back_ref, far_ref, pix_sem, round_sem, mate_sem, f_dev, frames):
    zcount = lax.axis_size("pix")
    z = lax.axis_index("pix")
    count = lax.axis_size("frames")
    me = lax.axis_index("frames")
    chunk = land.shape[1]
    tiles = frames // L

    def piece(which):
        return pl.ds(pl.multiple_of(which * chunk, 8), chunk)

    sent = exchange(lambda peer: packed_ref.at[piece(peer)], land.at[z], pix_sem, 0, "pix")
    land[z] = packed_ref[piece(z), :]
    for copy in sent:
        copy.wait_recv()
    total = land[0]
    for k in range(1, zcount):
        total = total + land[k]
    reduced_ref[...] = total
    more = exchange(lambda peer: reduced_ref, gathered.at[me], round_sem, 0, "frames")
    gathered[me] = total
    for copy in more:
        copy.wait_recv()
    lane = iota((chunk, L), 1)
    sums = [[None] * tiles for _ in range(4)]
    for w in range(count):
        first = (w * f_dev - RADIUS) % frames
        start = first % L
        for k in range(4):
            part = pltpu.roll(gathered[w], (start - WIN * k) % L, 1)
            spans = [(first // L, start, min(start + WIN, L))]
            if start + WIN > L:
                spans.append(((first // L + 1) % tiles, 0, start + WIN - L))
            for tile, low, high in spans:
                term = jnp.where((lane >= low) & (lane < high), part, 0.0)
                sums[k][tile] = term if sums[k][tile] is None else sums[k][tile] + term
    for k in range(4):
        for tile in range(tiles):
            diag_ref[z, k, :, tile * L : (tile + 1) * L] = sums[k][tile]
    for copy in sent + more:
        copy.wait_send()
    mate = me + 1 - 2 * lax.rem(me, 2)
    mine = pl.ds(2 * lax.rem(me, 2), 2)
    half = diag_ref.at[z, mine]
    sent = exchange(lambda peer: half, half, pix_sem, 1, "pix")
    passed = []
    for n, (copy, step) in enumerate(zip(sent, range(zcount - 1, 0, -1))):
        copy.wait_recv()
        there = diag_ref.at[lax.rem(z + step, zcount), mine]
        handed = remote(there, there, mate_sem, 0, n, "frames", mate)
        handed.start()
        passed.append(handed)
    for copy in passed:
        copy.wait_recv()
    for copy in sent + passed:
        copy.wait_send()

    def block(k, at):
        return [
            diag_ref[at // chunk, k, at % chunk : at % chunk + 8, t * L : (t + 1) * L]
            for t in range(tiles)
        ]

    def entry(i, j, half):
        if i < 4:
            return block(i, BAND * j + 8 * half)
        return block(i - 4 + 2 * (j // 3), 6 * BAND + 8 + BAND * (j % 3) + 8 * half)

    row = iota((8, L), 0)
    lanes = iota((8, L), 1)

    def later(x, half):
        turned = [pltpu.roll(v, 8 * half, 1, stride=1, stride_axis=0) for v in x]
        if tiles == 1:
            return turned
        mine = lanes >= 8 * half + row
        return [jnp.where(mine, turned[t], turned[t - 1]) for t in range(tiles)]

    def flip(x):
        for bit in (4, 2, 1):
            x = jnp.where((row & bit) != 0, pltpu.roll(x, bit, 0), pltpu.roll(x, 8 - bit, 0))
        return x

    for i in range(6):
        for j in range(6):
            for half in range(2):
                front = entry(i, j, half)
                moved = later(entry(j, i, half), half)
                for t in range(tiles):
                    ahead_ref[i, 2 * j + half, :, t * L : (t + 1) * L] = flip(front[t])
                    value = jnp.where(row > 0, moved[t], 0.0) if half == 0 else moved[t]
                    back_ref[i, 2 * j + half, :, t * L : (t + 1) * L] = value
    edge = 6 * BAND
    last = edge + 8 + 3 * BAND
    for i in range(6):
        if i < 4:
            ends = block(i, edge)
        else:
            near, far = block(i - 4, last), block(i - 2, last)
            ends = [jnp.where(row < 3, a, pltpu.roll(b, 3, 0)) for a, b in zip(near, far)]
        for t in range(tiles):
            far_ref[i, :, t * L : (t + 1) * L] = jnp.where(row < 6, ends[t], 0.0)
    sources = [block(k, edge) for k in range(4)] + [block(k, last) for k in range(2)]
    rhs = []
    for t in range(tiles):
        out = jnp.zeros((8, L), F32)
        for i in range(6):
            at = 6 if i < 4 else 3
            out = jnp.where(row == i, sources[i][t][at : at + 1, :], out)
        rhs.append(out)
    return rhs, later


def conjugate(rhs, later, ahead_ref, back_ref, far_ref):
    tiles = len(rhs)
    row = iota((8, L), 0)
    lanes = iota((8, L), 1)

    def sooner(x, half):
        turned = [pltpu.roll(v, L - 8 * half - 7, 1, stride=1, stride_axis=0) for v in x]
        if tiles == 1:
            return turned
        mine = lanes + 8 * half + 7 - row < L
        return [jnp.where(mine, turned[t], turned[(t + 1) % tiles]) for t in range(tiles)]

    def moved(x, steps):
        turned = [pltpu.roll(v, steps % L, 1) for v in x]
        if tiles == 1:
            return turned
        if steps > 0:
            return [jnp.where(lanes >= steps, turned[t], turned[t - 1]) for t in range(tiles)]
        return [jnp.where(lanes < L + steps, turned[t], turned[(t + 1) % tiles]) for t in range(tiles)]

    def dot(x, y):
        total = x[0] * y[0]
        for t in range(1, tiles):
            total = total + x[t] * y[t]
        return jnp.sum(total, keepdims=True)

    def product(p):
        ahead = moved(p, -BAND)
        acc = [[far_ref[i, :, t * L : (t + 1) * L] * ahead[t] for t in range(tiles)] for i in range(6)]
        tail = [None] * tiles
        for j in range(6):
            wide = [jnp.broadcast_to(v[j : j + 1, :], (8, L)) for v in p]
            for t in range(tiles):
                term = far_ref[j, :, t * L : (t + 1) * L] * wide[t]
                tail[t] = term if tail[t] is None else tail[t] + term
            for half in range(2):
                plus = sooner(wide, half)
                minus = later(wide, half)
                for i in range(6):
                    for t in range(tiles):
                        acc[i][t] = (
                            acc[i][t]
                            + ahead_ref[i, 2 * j + half, :, t * L : (t + 1) * L] * plus[t]
                            + back_ref[i, 2 * j + half, :, t * L : (t + 1) * L] * minus[t]
                        )
        tail = moved(tail, BAND)
        out = []
        for t in range(tiles):
            y = tail[t] + REG * p[t]
            for i in range(6):
                y = y + jnp.where(row == i, jnp.sum(acc[i][t], axis=0, keepdims=True), 0.0)
            out.append(y)
        return out

    def step(_, carry):
        x, residual, direction, rr = carry
        image = product(direction)
        alpha = rr / dot(direction, image)
        x = [a + alpha * b for a, b in zip(x, direction)]
        residual = [a - alpha * b for a, b in zip(residual, image)]
        new = dot(residual, residual)
        beta = new / rr
        direction = [a + beta * b for a, b in zip(residual, direction)]
        return x, residual, direction, new

    zero = [jnp.zeros((8, L), F32)] * tiles
    return lax.fori_loop(0, ITERS, step, (zero, rhs, rhs, dot(rhs, rhs)))[0]


def finish(
    matrix_ref, e_ref, base_ref, inv_ref, pose_ref, step_ref, frames,
    cols_ref, step3, packed_ref, land, reduced_ref, gathered, diag_ref, ahead_ref, back_ref, far_ref, x_ref,
    pix_sem, round_sem, mate_sem,
):
    me = lax.axis_index("frames")
    tiles, f_dev = step3.shape[:2]
    half = f_dev // 2
    pack(matrix_ref, packed_ref)
    rhs, later = operator(
        packed_ref, land, reduced_ref, gathered, diag_ref, ahead_ref, back_ref, far_ref,
        pix_sem, round_sem, mate_sem, f_dev, frames,
    )
    x = conjugate(rhs, later, ahead_ref, back_ref, far_ref)
    for t, value in enumerate(x):
        x_ref[:, t * L : (t + 1) * L] = value
    mine = window(lambda at: x_ref[:, at], me, f_dev, frames)
    pose_ref[...] = mine[:6, RADIUS : RADIUS + f_dev]
    turned = spread_rows(mine)
    for i in range(6):
        cols_ref[i] = jnp.broadcast_to(turned[:WIN, i : i + 1], (WIN, L))
    row = iota((8, L), 0)
    lane = iota((8, L), 1)
    for part in range(2):

        @pl.loop(0, half)
        def per_source(i):
            s = i + part * half
            group = [[cols_ref[j, 8 * g : 8 * g + 8, :] for g in range(part, part + 3)] for j in range(6)]
            below = [jnp.where(row >= i, group[j][0], group[j][1]) for j in range(6)]
            over = [jnp.where(row > i, group[j][1], group[j][2]) for j in range(6)]
            near, far = (over, below) if part == 0 else (below, over)
            at = jnp.sum(jnp.where(lane == s + RADIUS, mine, 0.0), axis=1, keepdims=True)
            terms = near + far + [jnp.broadcast_to(at, (8, L))]
            for tile in range(tiles):
                slot = s * tiles + tile
                image = e_ref[slot, 0] * terms[0]
                for n in range(1, 13):
                    image = image + e_ref[slot, n] * terms[n]
                image = jnp.sum(image, axis=0, keepdims=True)
                here = (tile, pl.ds(s, 1), slice(None))
                step3[here] = base_ref[here] - inv_ref[here] * image

    for tile in range(tiles):
        step_ref[:, tile * L : (tile + 1) * L] = step3[tile]


def swap_edges(low_out, high_out, low_ref, high_ref, sems):
    count = lax.axis_size("frames")
    me = lax.axis_index("frames")
    below = lax.rem(me + count - 1, count)
    over = lax.rem(me + 1, count)
    tiles = low_out.shape[0]
    down = [remote(low_out.at[t, :, :SENT], low_ref.at[t, :, :SENT], sems, 0, t, "frames", below) for t in range(tiles)]
    up = [remote(high_out.at[t, :, :SENT], high_ref.at[t, :, :SENT], sems, 1, t, "frames", over) for t in range(tiles)]

    @pl.when(me < count - 1)
    def _():
        for copy in up:
            copy.start()

    def descend():
        @pl.when(me > 0)
        def _():
            for copy in down:
                copy.start()

    def receive(part):
        if part == 0:

            @pl.when(me > 0)
            def _():
                for copy in up:
                    copy.wait_recv()

            @pl.when(me == 0)
            def _():
                high_ref[...] = jnp.zeros_like(high_ref)

        else:

            @pl.when(me < count - 1)
            def _():
                for copy in down:
                    copy.wait_recv()

            @pl.when(me == count - 1)
            def _():
                low_ref[...] = jnp.zeros_like(low_ref)

    def drain():
        @pl.when(me > 0)
        def _():
            for copy in down:
                copy.wait_send()

        @pl.when(me < count - 1)
        def _():
            for copy in up:
                copy.wait_send()

    return descend, receive, drain


def solve(
    edge_ref, rot_ref, trans_ref, depth_ref, damp_ref, flow_ref, weight_ref, mask_ref,
    x_ref, step_ref, flow3, weight3, mask3, load_sem, pose_ref,
    own_ref, low_out, high_out, low_ref, high_ref, edge_sem,
    frame_ref, coord_ref, depth3, damp3, e_ref, part_ref, near_sum, near_pair, far_sum, far_pair,
    base_ref, inv_ref, z0, z1, gram_ref, matrix_ref, wide, *scratch,
):
    me = lax.axis_index("frames")
    f_dev, pix = depth_ref.shape
    frames = rot_ref.shape[1]
    loads = fetch(flow_ref, weight_ref, mask_ref, flow3, weight3, mask3, load_sem)
    barrier = pltpu.get_barrier_semaphore()
    total = 0
    for axis in ("frames", "pix"):
        for peer in peers(axis):
            pl.semaphore_signal(
                barrier, inc=1, device_id={axis: peer}, device_id_type=pl.DeviceIdType.MESH
            )
            total += 1
    poses = []
    for ref in (rot_ref, trans_ref):
        poses.append(window(lambda at: ref[:, at], me, f_dev, frames))
    turned = spread_rows(jnp.concatenate(poses, axis=0))
    for k in range(6):
        pose_ref[k] = jnp.broadcast_to(turned[:WIN, k : k + 1], (WIN, L))
    prepare(pose_ref, frame_ref, coord_ref, depth_ref, damp_ref, depth3, damp3)
    aggregate(edge_ref, loads, flow3, weight3, mask3, own_ref, low_out, high_out, me, f_dev)
    pl.semaphore_wait(barrier, total)
    descend, receive, drain = swap_edges(low_out, high_out, low_ref, high_ref, edge_sem)
    near_pairs(own_ref, frame_ref, coord_ref, depth3, e_ref, part_ref, near_sum, near_pair, descend)
    far_pairs(
        own_ref, low_ref, high_ref, frame_ref, coord_ref, depth3, damp3, e_ref, part_ref,
        far_sum, far_pair, base_ref, inv_ref, (z0, z1), gram_ref, receive,
    )
    assemble(near_sum, near_pair, far_sum, far_pair, gram_ref, matrix_ref, wide)
    finish(matrix_ref, e_ref, base_ref, inv_ref, x_ref, step_ref, frames, *scratch)
    drain()


def call(body, out, scratch, vmem, hbm, **params):
    vm = pl.BlockSpec(memory_space=pltpu.VMEM)
    far = pl.BlockSpec(memory_space=pl.ANY)
    return pl.pallas_call(
        body,
        out_shape=[jax.ShapeDtypeStruct(s, t) for s, t in out],
        in_specs=[vm] * vmem + [far] * hbm,
        out_specs=[vm] * len(out),
        scratch_shapes=scratch,
        compiler_params=pltpu.CompilerParams(vmem_limit_bytes=VMEM_LIMIT, **params),
    )


def per_device(edge_frames, rotvec, trans, inv_depth, depth_damping, flow, weight, mask):
    f_dev, pix = inv_depth.shape
    edges = mask.shape[0]
    frames = rotvec.shape[1]
    tiles = pix // L
    own_rows = f_dev * 16
    side = 40
    sums = len(UPPER) + 6
    width = 256
    size = 6 * WIN
    count = lax.axis_size("frames")
    zcount = lax.axis_size("pix")
    chunk = -(-PACKED // (8 * zcount)) * 8
    x, step = call(
        solve,
        [((6, f_dev), F32), ((f_dev, pix), F32)],
        [
            pltpu.VMEM((tiles, 2, edges, L), F32),
            pltpu.VMEM((tiles, 2, edges, L), F32),
            pltpu.VMEM((tiles, edges, L), jnp.int32),
            pltpu.SemaphoreType.DMA((tiles, 5)),
            pltpu.VMEM((6, WIN, L), F32),
            pltpu.VMEM((4, own_rows, pix), F32),
            pltpu.VMEM((tiles, 4, side, L), F32),
            pltpu.VMEM((tiles, 4, side, L), F32),
            pltpu.VMEM((tiles, 4, side, L), F32),
            pltpu.VMEM((tiles, 4, side, L), F32),
            pltpu.SemaphoreType.DMA((2, 2, tiles)),
            pltpu.VMEM((12, WIN, L), F32),
            pltpu.VMEM((tiles, 2, 8, L), F32),
            pltpu.VMEM((tiles, f_dev, L), F32),
            pltpu.VMEM((tiles, f_dev, L), F32),
            pltpu.VMEM((f_dev * tiles, 13, 8, L), F32),
            pltpu.VMEM((f_dev * tiles, 3, 8, L), F32),
            pltpu.VMEM((sums, 8, L), F32),
            pltpu.VMEM((12, 8, L), F32),
            pltpu.VMEM((sums, 8, L), F32),
            pltpu.VMEM((12, 8, L), F32),
            pltpu.VMEM((tiles, f_dev, L), F32),
            pltpu.VMEM((tiles, f_dev, L), F32),
            pltpu.VMEM((2 * size + 16, pix), BF16),
            pltpu.VMEM((2 * size + 16, pix), BF16),
            pltpu.VMEM((2 * size + 16, size + 16), F32),
            pltpu.VMEM((size + 8, width), F32),
            pltpu.VMEM((256, 256), F32),
            pltpu.VMEM((6, WIN, L), F32),
            pltpu.VMEM((tiles, f_dev, L), F32),
            pltpu.VMEM((chunk * zcount, L), F32),
            pltpu.VMEM((zcount, chunk, L), F32),
            pltpu.VMEM((chunk, L), F32),
            pltpu.VMEM((count, chunk, L), F32),
            pltpu.VMEM((zcount, 4, chunk, frames), F32),
            pltpu.VMEM((6, 12, 8, frames), F32),
            pltpu.VMEM((6, 12, 8, frames), F32),
            pltpu.VMEM((6, 8, frames), F32),
            pltpu.VMEM((8, frames), F32),
            pltpu.SemaphoreType.DMA((2, 2, zcount)),
            pltpu.SemaphoreType.DMA((2, 1, count)),
            pltpu.SemaphoreType.DMA((2, 1, zcount)),
        ],
        5, 3, collective_id=0, has_side_effects=True,
    )(edge_frames, rotvec, trans, inv_depth, depth_damping, flow, weight, mask)
    return x, step


def solution(mesh):
    return jax.shard_map(
        per_device,
        mesh=mesh,
        in_specs=(
            P(None, "frames"),
            P(),
            P(),
            P("frames", "pix"),
            P("frames", "pix"),
            P("frames", None, "pix"),
            P("frames", None, "pix"),
            P("frames", "pix"),
        ),
        out_specs=(P(None, "frames"), P("frames", "pix")),
        check_vma=False,
    )
```

```python
import jax
import jax.numpy as jnp
from jax import lax
from jax.experimental import pallas as pl
from jax.experimental.pallas import tpu as pltpu
from jax.sharding import PartitionSpec as P

ROWS = 48
COLS = 64
RADIUS = 8
ITERS = 6
REG = 100.0
F32 = jnp.float32
BF16 = jnp.bfloat16
L = 128
WIN = 32
BAND = 2 * RADIUS
PACKED = 160
SENT = RADIUS * (RADIUS + 1) // 2
VMEM_LIMIT = 60 * 1024 * 1024
UPPER = [(i, j) for i in range(6) for j in range(i, 6) if (i, j) != (0, 1)]


def split(x):
    high = x.astype(BF16)
    return high, (x - high.astype(F32)).astype(BF16)


def iota(shape, dim):
    return lax.broadcasted_iota(jnp.int32, shape, dim)


def destinations(edge_ref, own_rows, side, f_dev, me):
    start = me * f_dev
    source = edge_ref[0:1, :] - start + RADIUS
    target = edge_ref[1:2, :] - start + RADIUS
    s = source - RADIUS
    low = jnp.where(s < f_dev // 2, 1, 0)
    above = jnp.where(target > source, 1, 0)
    mine = jnp.where(low == above, 0, f_dev * 8) + s * 8 + (target & 7)
    q = target - RADIUS
    tile = jnp.where(source < 3, source, jnp.where(source == 3, 4, jnp.where(source == 7, 3, 6 - source)))
    line = jnp.where((source > 3) & (source < 7), q + 7 - source, q)
    lowest = own_rows + tile * 8 + line
    i = source - f_dev - RADIUS
    q = target - f_dev
    tile = jnp.where(i == 0, 3, jnp.where(i < 4, i - 1, jnp.where(i == 4, 4, 7 - i)))
    line = jnp.where(i >= 4, q - i, q)
    highest = own_rows + side + tile * 8 + line
    return jnp.where(source < RADIUS, lowest, jnp.where(source >= RADIUS + f_dev, highest, mine))


def fetch(flow_ref, weight_ref, mask_ref, flow3, weight3, mask3, sems):
    out = []
    for tile in range(flow3.shape[0]):
        cols = pl.ds(tile * L, L)
        pairs = [(mask_ref.at[:, cols], mask3.at[tile])]
        for comp in range(2):
            pairs.append((weight_ref.at[:, comp, cols], weight3.at[tile, comp]))
            pairs.append((flow_ref.at[:, comp, cols], flow3.at[tile, comp]))
        copies = [pltpu.make_async_copy(a, b, sems.at[tile, n]) for n, (a, b) in enumerate(pairs)]
        for copy in copies:
            copy.start()
        out.append(copies)
    return out


def aggregate(edge_ref, loads, flow3, weight3, mask3, own_ref, low_ref, high_ref, me, f_dev):
    edges = edge_ref.shape[1]
    own = own_ref.shape[1]
    side = low_ref.shape[2]
    rows = own + 2 * side
    dest = destinations(edge_ref, own, side, f_dev, me)
    pick = (iota((rows, edges), 0) == dest).astype(F32).astype(BF16)
    for tile in range(len(loads)):
        cols = slice(tile * L, (tile + 1) * L)
        if tile % 3 == 0:
            for copies in loads[tile : tile + 3]:
                for copy in copies:
                    copy.wait()
        live = mask3[tile].astype(F32)
        fields = []
        for comp in range(2):
            conf = weight3[tile, comp] * live
            fields += [conf, conf * flow3[tile, comp]]
        high, low = split(jnp.concatenate(fields, axis=1))
        out = jnp.dot(pick, high, preferred_element_type=F32) + jnp.dot(
            pick, low, preferred_element_type=F32
        )
        for field in range(4):
            part = out[:, field * L : (field + 1) * L]
            own_ref[field, :, cols] = part[:own]
            low_ref[tile, field] = part[own : own + side]
            high_ref[tile, field] = part[own + side :]


def window(load, me, f_dev, frames):
    tiles = frames // L
    first = lax.rem(me * f_dev - RADIUS + frames, frames)
    tile = first // L
    back = lax.rem(L - lax.rem(first, L), L)
    near = pltpu.roll(load(pl.ds(pl.multiple_of(tile * L, L), L)), back, 1)
    if tiles == 1:
        return near
    after = lax.rem(tile + 1, tiles)
    far = pltpu.roll(load(pl.ds(pl.multiple_of(after * L, L), L)), back, 1)
    return jnp.where(iota(near.shape, 1) + lax.rem(first, L) < L, near, far)


def spread_rows(x):
    return jnp.concatenate([x, jnp.zeros((L - x.shape[0], L), F32)], axis=0).T


def motion_sums(u, v, uu, vv, a, b, ds):
    va, ub = v * a, u * b
    e0, e1 = ds * a, ds * b
    return [e0, e1, -(u * e0 + v * e1), -(u * va + vv * b), uu * a + v * ub, ub - va]


def curvature_sums(u, v, uu, vv, uv, ds, wu, wv):
    a1, b1 = wu * v, wv * u
    a2, b2 = a1 * u, b1 * v
    a3, b3 = wu * uu, wv * vv
    h00, h11 = wu * ds * ds, wv * ds * ds
    h02, h12 = h00 * u, h11 * v
    x1, x2, x3 = ds * a1, ds * a2, ds * a3
    y1, y2, y3 = ds * b1, ds * b2, ds * b3
    return [
        h00, h02, x2, x3, x1,
        h11, h12, y3, y2, y1,
        h02 * u + h12 * v, u * x2 + v * y3, u * x3 + v * y2, x2 - y2,
        a2 * uv + b3 * vv, uv * (a3 + b3), a2 * v - b3 * u,
        a3 * uu + b2 * uv, b2 * u - a3 * v,
        a1 * v + b1 * u,
    ]


SIGNS = [1, -1, -1, 1, -1, 1, -1, -1, 1, 1, 1, 1, -1, 1, 1, -1, 1, 1, 1, 1]


def adj_t(rel, tr, vec):
    turn = [
        vec[3] - (tr[1] * vec[2] - tr[2] * vec[1]),
        vec[4] - (tr[2] * vec[0] - tr[0] * vec[2]),
        vec[5] - (tr[0] * vec[1] - tr[1] * vec[0]),
    ]
    out = [rel[j] * vec[0] + rel[3 + j] * vec[1] + rel[6 + j] * vec[2] for j in range(3)]
    return out + [rel[j] * turn[0] + rel[3 + j] * turn[1] + rel[6 + j] * turn[2] for j in range(3)]


def fold(x):
    row = iota((8, L), 0)

    def merge(a, b, bit):
        other = (row & bit) != 0
        return jnp.where(other, b, a) + pltpu.roll(jnp.where(other, a, b), bit, 0)

    first, second, third = merge(x[0], x[1], 1), merge(x[2], x[3], 1), merge(x[4], x[5], 1)
    return merge(merge(first, second, 2), third + pltpu.roll(third, 2, 0), 4)


def pair_pose(frame_ref, s, first, after):
    here = [frame_ref[k, pl.ds(s + RADIUS, 1), :] for k in range(12)]
    there = [
        jnp.where(after, frame_ref[k, first : first + 8, :], frame_ref[k, first + 8 : first + 16, :])
        for k in range(12)
    ]
    rel = [
        there[3 * r] * here[3 * c] + there[3 * r + 1] * here[3 * c + 1] + there[3 * r + 2] * here[3 * c + 2]
        for r in range(3)
        for c in range(3)
    ]
    tr = [
        there[9 + r] - (rel[3 * r] * here[9] + rel[3 * r + 1] * here[10] + rel[3 * r + 2] * here[11])
        for r in range(3)
    ]
    return rel, tr


def octet(fields, depth, col, rowc, rel, tr):
    wu, fu, wv, fv = fields
    point = [
        rel[3 * k] * col + rel[3 * k + 1] * rowc + rel[3 * k + 2] + depth * tr[k] for k in range(3)
    ]
    iz = 1.0 / point[2]
    u = point[0] * iz
    v = point[1] * iz
    ds = depth * iz
    su = iz * (tr[0] - u * tr[2])
    sv = iz * (tr[1] - v * tr[2])
    au = wu * su
    av = wv * sv
    gu = wu * (col - u) + fu
    gv = wv * (rowc - v) + fv
    uu = 1.0 + u * u
    vv = 1.0 + v * v
    uv = u * v
    e = motion_sums(u, v, uu, vv, au, av, ds)
    back = adj_t(rel, tr, e)
    sums = curvature_sums(u, v, uu, vv, uv, ds, wu, wv) + motion_sums(u, v, uu, vv, gu, gv, ds)
    return e, back, au * su + av * sv, su * gu + sv * gv, sums


def prepare(pose_ref, frame_ref, coord_ref, depth_ref, damp_ref, depth3, damp3):
    tiles = depth3.shape[0]
    ox, oy, oz = pose_ref[0], pose_ref[1], pose_ref[2]
    zero = jnp.zeros_like(ox)
    cross = [[zero, -oz, oy], [oz, zero, -ox], [-oy, ox, zero]]
    sq = ox * ox + oy * oy + oz * oz
    c1 = 1.0 - sq / 6.0 + sq * sq / 120.0
    c2 = 0.5 - sq / 24.0 + sq * sq / 720.0
    for r in range(3):
        for c in range(3):
            square = cross[r][0] * cross[0][c] + cross[r][1] * cross[1][c] + cross[r][2] * cross[2][c]
            frame_ref[3 * r + c] = float(r == c) + c1 * cross[r][c] + c2 * square
        frame_ref[9 + r] = pose_ref[3 + r]
    first = lax.axis_index("pix") * (tiles * L)
    for tile in range(tiles):
        depth3[tile] = depth_ref[:, tile * L : (tile + 1) * L]
        damp3[tile] = damp_ref[:, tile * L : (tile + 1) * L]
        pixel = first + tile * L + iota((8, L), 1)
        prow = pixel // COLS
        pcol = pixel - prow * COLS
        coord_ref[tile, 0] = (pcol.astype(F32) - 0.5 * (COLS - 1)) / COLS
        coord_ref[tile, 1] = (prow.astype(F32) - 0.5 * (ROWS - 1)) / COLS


def note(at, sums, pose, sum_ref, pair_ref):
    for n, x in enumerate(sums):
        sum_ref[n] = jnp.where(at, jnp.sum(x, axis=1, keepdims=True), sum_ref[n])
    for n, x in enumerate(pose):
        pair_ref[n] = jnp.where(at, x, pair_ref[n])


def near_pairs(own_ref, frame_ref, coord_ref, depth3, e_ref, part_ref, sum_ref, pair_ref, descend):
    tiles, f_dev = depth3.shape[:2]
    half = f_dev // 2
    row = iota((8, L), 0)
    lane = iota((8, L), 1)
    sum_ref[...] = jnp.zeros_like(sum_ref)
    pair_ref[...] = jnp.zeros_like(pair_ref)
    for part in range(2):

        @pl.loop(0, half)
        def per_source(i):
            s = i + part * half
            rel, tr = pair_pose(frame_ref, s, 8, row > i if part == 0 else row >= i)
            sums = None
            for tile in range(tiles):
                cols = slice(tile * L, (tile + 1) * L)
                at = pl.ds(pl.multiple_of(s * 8, 8), 8)
                fields = [own_ref[k, at, cols] for k in range(4)]
                e, back, curv, grad, new = octet(
                    fields, depth3[tile, pl.ds(s, 1), :], coord_ref[tile, 0], coord_ref[tile, 1], rel, tr
                )
                slot = s * tiles + tile
                for j in range(6):
                    e_ref[slot, j] = e[j]
                for j in range(6):
                    part_ref[slot, j] = back[j]
                part_ref[slot, 6] = curv
                part_ref[slot, 7] = grad
                sums = new if sums is None else [a + b for a, b in zip(sums, new)]
            note(lane == s + RADIUS, sums, rel + tr, sum_ref, pair_ref)

        if part == 1:
            descend()


def far_pairs(
    own_ref, low_ref, high_ref, frame_ref, coord_ref, depth3, damp3, e_ref, part_ref, sum_ref, pair_ref,
    base_ref, inv_ref, zs, gram_ref, receive,
):
    tiles, f_dev = depth3.shape[:2]
    half = f_dev // 2
    row = iota((8, L), 0)
    lane = iota((8, L), 1)
    pair = iota((16, L), 0)
    size = 6 * WIN
    sum_ref[...] = jnp.zeros_like(sum_ref)
    pair_ref[...] = jnp.zeros_like(pair_ref)
    gram_ref[...] = jnp.zeros_like(gram_ref)
    zs[1][...] = jnp.zeros_like(zs[1])
    none = jnp.zeros((8, L), F32)

    def gram(which):
        z = zs[which][...]
        nt = (((1,), (1,)), ((), ()))
        gram_ref[...] += lax.dot_general(z, z[: size + 16], nt, preferred_element_type=F32)

    for part in range(2):
        receive(part)

        def per_source(i, which):
            s = i + part * half
            after = row >= i if part == 0 else row > i
            rel, tr = pair_pose(frame_ref, s, 0 if part == 0 else 16, after)
            if part == 0:
                slot = jnp.where(i == 0, 3, jnp.where(i < 4, i - 1, jnp.where(i == 4, 4, 7 - i)))
                shift = jnp.where(i >= 4, i, 0)
                keep = row >= i
                src = high_ref
            else:
                slot = jnp.where(i < 3, i, jnp.where(i == 3, 4, jnp.where(i == 7, 3, 6 - i)))
                shift = jnp.where((i > 3) & (i < 7), i + 1, 0)
                keep = row <= i
                src = low_ref
            sums = None
            for tile in range(tiles):
                cols = slice(tile * L, (tile + 1) * L)
                at = pl.ds(pl.multiple_of(f_dev * 8 + s * 8, 8), 8)
                fields = []
                for k in range(4):
                    got = src[tile, k, pl.ds(pl.multiple_of(slot * 8, 8), 8), :]
                    fields.append(jnp.where(keep, pltpu.roll(got, shift, 0), own_ref[k, at, cols]))
                e, back, curv, grad, new = octet(
                    fields, depth3[tile, pl.ds(s, 1), :], coord_ref[tile, 0], coord_ref[tile, 1], rel, tr
                )
                sums = new if sums is None else [a + b for a, b in zip(sums, new)]
                here = s * tiles + tile
                for j in range(6):
                    e_ref[here, 6 + j] = e[j]
                back = -fold([x + part_ref[here, j] for j, x in enumerate(back)])
                e_ref[here, 12] = back
                curv = jnp.sum(curv + part_ref[here, 6], axis=0, keepdims=True) + damp3[tile, pl.ds(s, 1), :]
                grad = -jnp.sum(grad + part_ref[here, 7], axis=0, keepdims=True)
                inv = 1.0 / curv
                scale = 1.0 / jnp.sqrt(curv)
                base_ref[tile, pl.ds(s, 1), :] = grad * inv
                inv_ref[tile, pl.ds(s, 1), :] = inv
                z = zs[which]
                skip = size + 16
                source = back * scale
                for j in range(6):
                    mine = e[j] * scale
                    other = e_ref[here, j] * scale
                    below, over = (mine, other) if part == 0 else (other, mine)
                    mid = jnp.where(row < i, below, jnp.where(row > i, over, source[j : j + 1, :]))
                    groups = [jnp.where(row >= i, below, 0.0), mid, jnp.where(row <= i, over, 0.0)]
                    groups = groups + [none] if part == 0 else [none] + groups
                    high, low = split(jnp.concatenate(groups, axis=0))
                    z[j * WIN : (j + 1) * WIN, cols] = high
                    z[skip + j * WIN : skip + (j + 1) * WIN, cols] = low
                y = grad * scale
                rest = y - y.astype(BF16).astype(F32)
                lines = jnp.where(pair == 0, y, jnp.where(pair == 1, rest, 0.0))
                z[size : size + 16, cols] = lines.astype(BF16)
            note(lane == s + RADIUS, sums, rel + tr, sum_ref, pair_ref)

        @pl.loop(0, half // 2)
        def per_two(k):
            gram(1)
            per_source(2 * k, 0)
            gram(0)
            per_source(2 * k + 1, 1)

    gram(1)


def assemble(near_sum, near_pair, far_sum, far_pair, gram_ref, matrix_ref, wide):
    size = 6 * WIN
    row = iota((8, L), 0)
    lane = iota((8, L), 1)
    i = lane & 7
    first = lane < 16

    def sides(near, far):
        return jnp.where(first, far, near), jnp.where(first, near, far)

    def expand(x):
        low, high = x
        mid = jnp.where(row < i, low, jnp.where(row > i, high, 0.0))
        start = jnp.where(row >= i, low, 0.0)
        end = jnp.where(row <= i, high, 0.0)
        return jnp.concatenate(
            [
                jnp.where(first, start, 0.0),
                jnp.where(first, mid, start),
                jnp.where(first, end, mid),
                jnp.where(first, 0.0, end),
            ],
            axis=0,
        )

    pose = [sides(near_pair[k], far_pair[k]) for k in range(12)]
    h = [[None] * 6 for _ in range(6)]
    wholes = [[None] * 6 for _ in range(6)]
    for n, (a, b) in enumerate(UPPER):
        pair = sides(near_sum[n], far_sum[n])
        h[a][b] = h[b][a] = pair if SIGNS[n] > 0 else tuple(-x for x in pair)
    count = len(UPPER)
    r = [tuple(-x for x in sides(near_sum[count + j], far_sum[count + j])) for j in range(6)]
    eye = iota((WIN, L), 0) == iota((WIN, L), 1)

    def total(terms):
        out = None
        for x, y in terms:
            if x is None or y is None:
                continue
            out = x * y if out is None else out + x * y
        return out

    had = [[[None, None] for _ in range(6)] for _ in range(6)]
    source = [[0.0] * 6 for _ in range(6)]
    lines = [0.0] * 6
    for side in range(2):
        rel = [pose[k][side] for k in range(9)]
        tr = [pose[9 + k][side] for k in range(3)]
        ad = [[None] * 6 for _ in range(6)]
        for c in range(3):
            corner = [
                tr[1] * rel[6 + c] - tr[2] * rel[3 + c],
                tr[2] * rel[c] - tr[0] * rel[6 + c],
                tr[0] * rel[3 + c] - tr[1] * rel[c],
            ]
            for a in range(3):
                ad[a][c] = ad[3 + a][3 + c] = rel[3 * a + c]
                ad[a][3 + c] = corner[a]
        for a in range(6):
            for b in range(6):
                had[a][b][side] = total(
                    [(None if h[a][k] is None else h[a][k][side], ad[k][b]) for k in range(6)]
                )
        for a in range(6):
            for b in range(6):
                source[a][b] = source[a][b] + total([(ad[k][a], had[k][b][side]) for k in range(6)])
        back = adj_t(rel, tr, [x[side] for x in r])
        lines = [x + y for x, y in zip(lines, back)]
    wide[...] = jnp.zeros_like(wide)
    matrix_ref[...] = jnp.zeros_like(matrix_ref)
    for a in range(6):
        rows = slice(a * WIN, (a + 1) * WIN)
        for b in range(6):
            cols = slice(b * WIN, (b + 1) * WIN)
            wide[rows, cols] = -expand(had[a][b])[:, :WIN]
            both = jnp.sum(source[a][b], axis=0, keepdims=True)
            if h[a][b] is not None:
                both = both + jnp.sum(expand(h[a][b]), axis=1, keepdims=True)
            matrix_ref[rows, cols] = jnp.where(eye, both, 0.0)[:, :WIN]
    high, low = gram_ref[:size, :], gram_ref[size + 16 :, :]
    wide[:size, :size] = wide[:size, :size] - low[:, :size]
    wide[:size, size : size + 1] = -(
        high[:, size : size + 1] + high[:, size + 1 : size + 2] + low[:, size : size + 1]
    )
    flipped = wide[...].T
    matrix_ref[:size, :size] = (
        matrix_ref[:size, :size] - high[:, :size] + wide[:size, :size] + flipped[:size, :size]
    )
    for j in range(6):
        cols = slice(j * WIN, (j + 1) * WIN)
        whole = jnp.sum(expand(r[j]), axis=1, keepdims=True)
        here = jnp.sum(jnp.where(eye, whole, 0.0), axis=0, keepdims=True)
        here = here - jnp.sum(lines[j], axis=0, keepdims=True)
        matrix_ref[size : size + 1, cols] = here[:, :WIN] + flipped[size : size + 1, cols]


def remote(src, dst, sems, phase, which, axis, peer):
    return pltpu.make_async_remote_copy(
        src_ref=src,
        dst_ref=dst,
        send_sem=sems.at[0, phase, which],
        recv_sem=sems.at[1, phase, which],
        device_id={axis: peer},
        device_id_type=pl.DeviceIdType.MESH,
    )


def peers(axis):
    count = lax.axis_size(axis)
    me = lax.axis_index(axis)
    return [lax.rem(me + step, count) for step in range(1, count)]


def pack(matrix_ref, packed_ref):
    size = 6 * WIN
    lane = iota((WIN, L), 1) % WIN
    row = iota((WIN, L), 0)
    inside = row + lane < WIN
    left = iota((BAND, L), 1) < L // 2
    packed_ref[...] = jnp.zeros_like(packed_ref)

    def skew(x):
        for bit in (1, 2, 4, 8, 16):
            x = jnp.where((lane & bit) != 0, pltpu.roll(x, WIN - bit, 0), x)
        return jnp.where(inside, x, 0.0)

    rest = []
    for j in range(6):
        rows = slice(j * WIN, (j + 1) * WIN)
        main = skew(matrix_ref[rows, :L])
        packed_ref[j * BAND : (j + 1) * BAND, :] = main[:BAND]
        packed_ref[6 * BAND + j : 6 * BAND + j + 1, :] = main[BAND : BAND + 1]
        rest.append(skew(matrix_ref[rows, L:]))
    base = 6 * BAND + 8
    for j in range(3):
        near = rest[j]
        far = pltpu.roll(rest[j + 3], L // 2, 1)
        packed_ref[base + j * BAND : base + (j + 1) * BAND, :] = jnp.where(left, near[:BAND], far[:BAND])
        at = base + 3 * BAND + j
        packed_ref[at : at + 1, :] = jnp.where(left[:1], near[BAND : BAND + 1], far[BAND : BAND + 1])
    packed_ref[6 * BAND + 6 : 6 * BAND + 7, :] = matrix_ref[size : size + 1, :L]
    packed_ref[base + 3 * BAND + 3 : base + 3 * BAND + 4, :] = jnp.where(
        left[:1], matrix_ref[size : size + 1, L:], 0.0
    )


def exchange(src, dst, sems, phase, axis):
    sent = []
    for peer in peers(axis):
        copy = remote(src(peer), dst, sems, phase, len(sent), axis, peer)
        copy.start()
        sent.append(copy)
    return sent


def operator(packed_ref, land, reduced_ref, gathered, diag_ref, ahead_ref, back_ref, far_ref, pix_sem, round_sem, mate_sem, f_dev, frames):
    zcount = lax.axis_size("pix")
    z = lax.axis_index("pix")
    count = lax.axis_size("frames")
    me = lax.axis_index("frames")
    chunk = land.shape[1]
    tiles = frames // L

    def piece(which):
        return pl.ds(pl.multiple_of(which * chunk, 8), chunk)

    sent = exchange(lambda peer: packed_ref.at[piece(peer)], land.at[z], pix_sem, 0, "pix")
    land[z] = packed_ref[piece(z), :]
    for copy in sent:
        copy.wait_recv()
    total = land[0]
    for k in range(1, zcount):
        total = total + land[k]
    reduced_ref[...] = total
    more = exchange(lambda peer: reduced_ref, gathered.at[me], round_sem, 0, "frames")
    gathered[me] = total
    for copy in more:
        copy.wait_recv()
    lane = iota((chunk, L), 1)
    sums = [[None] * tiles for _ in range(4)]
    for w in range(count):
        first = (w * f_dev - RADIUS) % frames
        start = first % L
        for k in range(4):
            part = pltpu.roll(gathered[w], (start - WIN * k) % L, 1)
            spans = [(first // L, start, min(start + WIN, L))]
            if start + WIN > L:
                spans.append(((first // L + 1) % tiles, 0, start + WIN - L))
            for tile, low, high in spans:
                term = jnp.where((lane >= low) & (lane < high), part, 0.0)
                sums[k][tile] = term if sums[k][tile] is None else sums[k][tile] + term
    for k in range(4):
        for tile in range(tiles):
            diag_ref[z, k, :, tile * L : (tile + 1) * L] = sums[k][tile]
    for copy in sent + more:
        copy.wait_send()
    mate = me + 1 - 2 * lax.rem(me, 2)
    mine = pl.ds(2 * lax.rem(me, 2), 2)
    half = diag_ref.at[z, mine]
    sent = exchange(lambda peer: half, half, pix_sem, 1, "pix")
    passed = []
    for n, (copy, step) in enumerate(zip(sent, range(zcount - 1, 0, -1))):
        copy.wait_recv()
        there = diag_ref.at[lax.rem(z + step, zcount), mine]
        handed = remote(there, there, mate_sem, 0, n, "frames", mate)
        handed.start()
        passed.append(handed)
    for copy in passed:
        copy.wait_recv()
    for copy in sent + passed:
        copy.wait_send()

    def block(k, at):
        return [
            diag_ref[at // chunk, k, at % chunk : at % chunk + 8, t * L : (t + 1) * L]
            for t in range(tiles)
        ]

    def entry(i, j, half):
        if i < 4:
            return block(i, BAND * j + 8 * half)
        return block(i - 4 + 2 * (j // 3), 6 * BAND + 8 + BAND * (j % 3) + 8 * half)

    row = iota((8, L), 0)
    lanes = iota((8, L), 1)

    def later(x, half):
        turned = [pltpu.roll(v, 8 * half, 1, stride=1, stride_axis=0) for v in x]
        if tiles == 1:
            return turned
        mine = lanes >= 8 * half + row
        return [jnp.where(mine, turned[t], turned[t - 1]) for t in range(tiles)]

    def flip(x):
        for bit in (4, 2, 1):
            x = jnp.where((row & bit) != 0, pltpu.roll(x, bit, 0), pltpu.roll(x, 8 - bit, 0))
        return x

    for i in range(6):
        for j in range(6):
            for half in range(2):
                front = entry(i, j, half)
                moved = later(entry(j, i, half), half)
                for t in range(tiles):
                    ahead_ref[i, 2 * j + half, :, t * L : (t + 1) * L] = flip(front[t])
                    value = jnp.where(row > 0, moved[t], 0.0) if half == 0 else moved[t]
                    back_ref[i, 2 * j + half, :, t * L : (t + 1) * L] = value
    edge = 6 * BAND
    last = edge + 8 + 3 * BAND
    for i in range(6):
        if i < 4:
            ends = block(i, edge)
        else:
            near, far = block(i - 4, last), block(i - 2, last)
            ends = [jnp.where(row < 3, a, pltpu.roll(b, 3, 0)) for a, b in zip(near, far)]
        for t in range(tiles):
            far_ref[i, :, t * L : (t + 1) * L] = jnp.where(row < 6, ends[t], 0.0)
    sources = [block(k, edge) for k in range(4)] + [block(k, last) for k in range(2)]
    rhs = []
    for t in range(tiles):
        out = jnp.zeros((8, L), F32)
        for i in range(6):
            at = 6 if i < 4 else 3
            out = jnp.where(row == i, sources[i][t][at : at + 1, :], out)
        rhs.append(out)
    return rhs, later


def conjugate(rhs, later, ahead_ref, back_ref, far_ref):
    tiles = len(rhs)
    row = iota((8, L), 0)
    lanes = iota((8, L), 1)

    def sooner(x, half):
        turned = [pltpu.roll(v, L - 8 * half - 7, 1, stride=1, stride_axis=0) for v in x]
        if tiles == 1:
            return turned
        mine = lanes + 8 * half + 7 - row < L
        return [jnp.where(mine, turned[t], turned[(t + 1) % tiles]) for t in range(tiles)]

    def moved(x, steps):
        turned = [pltpu.roll(v, steps % L, 1) for v in x]
        if tiles == 1:
            return turned
        if steps > 0:
            return [jnp.where(lanes >= steps, turned[t], turned[t - 1]) for t in range(tiles)]
        return [jnp.where(lanes < L + steps, turned[t], turned[(t + 1) % tiles]) for t in range(tiles)]

    def dot(x, y):
        total = x[0] * y[0]
        for t in range(1, tiles):
            total = total + x[t] * y[t]
        return jnp.sum(total, keepdims=True)

    def product(p):
        ahead = moved(p, -BAND)
        acc = [[far_ref[i, :, t * L : (t + 1) * L] * ahead[t] for t in range(tiles)] for i in range(6)]
        tail = [None] * tiles
        for j in range(6):
            wide = [jnp.broadcast_to(v[j : j + 1, :], (8, L)) for v in p]
            for t in range(tiles):
                term = far_ref[j, :, t * L : (t + 1) * L] * wide[t]
                tail[t] = term if tail[t] is None else tail[t] + term
            for half in range(2):
                plus = sooner(wide, half)
                minus = later(wide, half)
                for i in range(6):
                    for t in range(tiles):
                        acc[i][t] = (
                            acc[i][t]
                            + ahead_ref[i, 2 * j + half, :, t * L : (t + 1) * L] * plus[t]
                            + back_ref[i, 2 * j + half, :, t * L : (t + 1) * L] * minus[t]
                        )
        tail = moved(tail, BAND)
        out = []
        for t in range(tiles):
            y = tail[t] + REG * p[t]
            for i in range(6):
                y = y + jnp.where(row == i, jnp.sum(acc[i][t], axis=0, keepdims=True), 0.0)
            out.append(y)
        return out

    def step(_, carry):
        x, residual, direction, rr = carry
        image = product(direction)
        alpha = rr / dot(direction, image)
        x = [a + alpha * b for a, b in zip(x, direction)]
        residual = [a - alpha * b for a, b in zip(residual, image)]
        new = dot(residual, residual)
        beta = new / rr
        direction = [a + beta * b for a, b in zip(residual, direction)]
        return x, residual, direction, new

    zero = [jnp.zeros((8, L), F32)] * tiles
    return lax.fori_loop(0, ITERS, step, (zero, rhs, rhs, dot(rhs, rhs)))[0]


def finish(
    matrix_ref, e_ref, base_ref, inv_ref, pose_ref, step_ref, frames,
    cols_ref, step3, packed_ref, land, reduced_ref, gathered, diag_ref, ahead_ref, back_ref, far_ref, x_ref,
    pix_sem, round_sem, mate_sem,
):
    me = lax.axis_index("frames")
    tiles, f_dev = step3.shape[:2]
    half = f_dev // 2
    pack(matrix_ref, packed_ref)
    rhs, later = operator(
        packed_ref, land, reduced_ref, gathered, diag_ref, ahead_ref, back_ref, far_ref,
        pix_sem, round_sem, mate_sem, f_dev, frames,
    )
    x = conjugate(rhs, later, ahead_ref, back_ref, far_ref)
    for t, value in enumerate(x):
        x_ref[:, t * L : (t + 1) * L] = value
    mine = window(lambda at: x_ref[:, at], me, f_dev, frames)
    pose_ref[...] = mine[:6, RADIUS : RADIUS + f_dev]
    turned = spread_rows(mine)
    for i in range(6):
        cols_ref[i] = jnp.broadcast_to(turned[:WIN, i : i + 1], (WIN, L))
    row = iota((8, L), 0)
    lane = iota((8, L), 1)
    for part in range(2):

        @pl.loop(0, half)
        def per_source(i):
            s = i + part * half
            group = [[cols_ref[j, 8 * g : 8 * g + 8, :] for g in range(part, part + 3)] for j in range(6)]
            below = [jnp.where(row >= i, group[j][0], group[j][1]) for j in range(6)]
            over = [jnp.where(row > i, group[j][1], group[j][2]) for j in range(6)]
            near, far = (over, below) if part == 0 else (below, over)
            at = jnp.sum(jnp.where(lane == s + RADIUS, mine, 0.0), axis=1, keepdims=True)
            terms = near + far + [jnp.broadcast_to(at, (8, L))]
            for tile in range(tiles):
                slot = s * tiles + tile
                image = e_ref[slot, 0] * terms[0]
                for n in range(1, 13):
                    image = image + e_ref[slot, n] * terms[n]
                image = jnp.sum(image, axis=0, keepdims=True)
                here = (tile, pl.ds(s, 1), slice(None))
                step3[here] = base_ref[here] - inv_ref[here] * image

    for tile in range(tiles):
        step_ref[:, tile * L : (tile + 1) * L] = step3[tile]


def swap_edges(low_out, high_out, low_ref, high_ref, sems):
    count = lax.axis_size("frames")
    me = lax.axis_index("frames")
    below = lax.rem(me + count - 1, count)
    over = lax.rem(me + 1, count)
    tiles = low_out.shape[0]
    down = [remote(low_out.at[t, :, :SENT], low_ref.at[t, :, :SENT], sems, 0, t, "frames", below) for t in range(tiles)]
    up = [remote(high_out.at[t, :, :SENT], high_ref.at[t, :, :SENT], sems, 1, t, "frames", over) for t in range(tiles)]

    @pl.when(me < count - 1)
    def _():
        for copy in up:
            copy.start()

    def descend():
        @pl.when(me > 0)
        def _():
            for copy in down:
                copy.start()

    def receive(part):
        if part == 0:

            @pl.when(me > 0)
            def _():
                for copy in up:
                    copy.wait_recv()

            @pl.when(me == 0)
            def _():
                high_ref[...] = jnp.zeros_like(high_ref)

        else:

            @pl.when(me < count - 1)
            def _():
                for copy in down:
                    copy.wait_recv()

            @pl.when(me == count - 1)
            def _():
                low_ref[...] = jnp.zeros_like(low_ref)

    def drain():
        @pl.when(me > 0)
        def _():
            for copy in down:
                copy.wait_send()

        @pl.when(me < count - 1)
        def _():
            for copy in up:
                copy.wait_send()

    return descend, receive, drain


def solve(
    edge_ref, rot_ref, trans_ref, depth_ref, damp_ref, flow_ref, weight_ref, mask_ref,
    x_ref, step_ref, flow3, weight3, mask3, load_sem, pose_ref,
    own_ref, low_out, high_out, low_ref, high_ref, edge_sem,
    frame_ref, coord_ref, depth3, damp3, e_ref, part_ref, near_sum, near_pair, far_sum, far_pair,
    base_ref, inv_ref, z0, z1, gram_ref, matrix_ref, wide, *scratch,
):
    me = lax.axis_index("frames")
    f_dev, pix = depth_ref.shape
    frames = rot_ref.shape[1]
    loads = fetch(flow_ref, weight_ref, mask_ref, flow3, weight3, mask3, load_sem)
    barrier = pltpu.get_barrier_semaphore()
    total = 0
    for axis in ("frames", "pix"):
        for peer in peers(axis):
            pl.semaphore_signal(
                barrier, inc=1, device_id={axis: peer}, device_id_type=pl.DeviceIdType.MESH
            )
            total += 1
    poses = []
    for ref in (rot_ref, trans_ref):
        poses.append(window(lambda at: ref[:, at], me, f_dev, frames))
    turned = spread_rows(jnp.concatenate(poses, axis=0))
    for k in range(6):
        pose_ref[k] = jnp.broadcast_to(turned[:WIN, k : k + 1], (WIN, L))
    prepare(pose_ref, frame_ref, coord_ref, depth_ref, damp_ref, depth3, damp3)
    aggregate(edge_ref, loads, flow3, weight3, mask3, own_ref, low_out, high_out, me, f_dev)
    pl.semaphore_wait(barrier, total)
    descend, receive, drain = swap_edges(low_out, high_out, low_ref, high_ref, edge_sem)
    near_pairs(own_ref, frame_ref, coord_ref, depth3, e_ref, part_ref, near_sum, near_pair, descend)
    far_pairs(
        own_ref, low_ref, high_ref, frame_ref, coord_ref, depth3, damp3, e_ref, part_ref,
        far_sum, far_pair, base_ref, inv_ref, (z0, z1), gram_ref, receive,
    )
    assemble(near_sum, near_pair, far_sum, far_pair, gram_ref, matrix_ref, wide)
    finish(matrix_ref, e_ref, base_ref, inv_ref, x_ref, step_ref, frames, *scratch)
    drain()


def call(body, out, scratch, vmem, hbm, **params):
    vm = pl.BlockSpec(memory_space=pltpu.VMEM)
    far = pl.BlockSpec(memory_space=pl.ANY)
    return pl.pallas_call(
        body,
        out_shape=[pltpu.VMEM(s, t) for s, t in out],
        in_specs=[vm] * vmem + [far] * hbm,
        out_specs=[vm] * len(out),
        scratch_shapes=scratch,
        compiler_params=pltpu.CompilerParams(vmem_limit_bytes=VMEM_LIMIT, **params),
    )


def per_device(edge_frames, rotvec, trans, inv_depth, depth_damping, flow, weight, mask):
    f_dev, pix = inv_depth.shape
    edges = mask.shape[0]
    frames = rotvec.shape[1]
    tiles = pix // L
    own_rows = f_dev * 16
    side = 40
    sums = len(UPPER) + 6
    width = 256
    size = 6 * WIN
    count = lax.axis_size("frames")
    zcount = lax.axis_size("pix")
    chunk = -(-PACKED // (8 * zcount)) * 8
    x, step = call(
        solve,
        [((6, f_dev), F32), ((f_dev, pix), F32)],
        [
            pltpu.VMEM((tiles, 2, edges, L), F32),
            pltpu.VMEM((tiles, 2, edges, L), F32),
            pltpu.VMEM((tiles, edges, L), jnp.int32),
            pltpu.SemaphoreType.DMA((tiles, 5)),
            pltpu.VMEM((6, WIN, L), F32),
            pltpu.VMEM((4, own_rows, pix), F32),
            pltpu.VMEM((tiles, 4, side, L), F32),
            pltpu.VMEM((tiles, 4, side, L), F32),
            pltpu.VMEM((tiles, 4, side, L), F32),
            pltpu.VMEM((tiles, 4, side, L), F32),
            pltpu.SemaphoreType.DMA((2, 2, tiles)),
            pltpu.VMEM((12, WIN, L), F32),
            pltpu.VMEM((tiles, 2, 8, L), F32),
            pltpu.VMEM((tiles, f_dev, L), F32),
            pltpu.VMEM((tiles, f_dev, L), F32),
            pltpu.VMEM((f_dev * tiles, 13, 8, L), F32),
            pltpu.VMEM((f_dev * tiles, 8, 8, L), F32),
            pltpu.VMEM((sums, 8, L), F32),
            pltpu.VMEM((12, 8, L), F32),
            pltpu.VMEM((sums, 8, L), F32),
            pltpu.VMEM((12, 8, L), F32),
            pltpu.VMEM((tiles, f_dev, L), F32),
            pltpu.VMEM((tiles, f_dev, L), F32),
            pltpu.VMEM((2 * size + 16, pix), BF16),
            pltpu.VMEM((2 * size + 16, pix), BF16),
            pltpu.VMEM((2 * size + 16, size + 16), F32),
            pltpu.VMEM((size + 8, width), F32),
            pltpu.VMEM((256, 256), F32),
            pltpu.VMEM((6, WIN, L), F32),
            pltpu.VMEM((tiles, f_dev, L), F32),
            pltpu.VMEM((chunk * zcount, L), F32),
            pltpu.VMEM((zcount, chunk, L), F32),
            pltpu.VMEM((chunk, L), F32),
            pltpu.VMEM((count, chunk, L), F32),
            pltpu.VMEM((zcount, 4, chunk, frames), F32),
            pltpu.VMEM((6, 12, 8, frames), F32),
            pltpu.VMEM((6, 12, 8, frames), F32),
            pltpu.VMEM((6, 8, frames), F32),
            pltpu.VMEM((8, frames), F32),
            pltpu.SemaphoreType.DMA((2, 2, zcount)),
            pltpu.SemaphoreType.DMA((2, 1, count)),
            pltpu.SemaphoreType.DMA((2, 1, zcount)),
        ],
        5, 3, collective_id=0, has_side_effects=True,
    )(edge_frames, rotvec, trans, inv_depth, depth_damping, flow, weight, mask)
    return x, step


def solution(mesh):
    return jax.shard_map(
        per_device,
        mesh=mesh,
        in_specs=(
            P(None, "frames"),
            P(),
            P(),
            P("frames", "pix"),
            P("frames", "pix"),
            P("frames", None, "pix"),
            P("frames", None, "pix"),
            P("frames", "pix"),
        ),
        out_specs=(P(None, "frames"), P("frames", "pix")),
        check_vma=False,
    )
```

```python
import jax
import jax.numpy as jnp
from jax import lax
from jax.experimental import pallas as pl
from jax.experimental.pallas import tpu as pltpu
from jax.sharding import PartitionSpec as P

ROWS = 48
COLS = 64
RADIUS = 8
ITERS = 6
REG = 100.0
F32 = jnp.float32
BF16 = jnp.bfloat16
L = 128
WIN = 32
BAND = 2 * RADIUS
PACKED = 160
SENT = RADIUS * (RADIUS + 1) // 2
VMEM_LIMIT = 60 * 1024 * 1024
UPPER = [(i, j) for i in range(6) for j in range(i, 6) if (i, j) != (0, 1)]


def split(x):
    high = x.astype(BF16)
    return high, (x - high.astype(F32)).astype(BF16)


def iota(shape, dim):
    return lax.broadcasted_iota(jnp.int32, shape, dim)


def destinations(edge_ref, own_rows, side, f_dev, me):
    start = me * f_dev
    source = edge_ref[0:1, :] - start + RADIUS
    target = edge_ref[1:2, :] - start + RADIUS
    s = source - RADIUS
    low = jnp.where(s < f_dev // 2, 1, 0)
    above = jnp.where(target > source, 1, 0)
    mine = jnp.where(low == above, 0, f_dev * 8) + s * 8 + (target & 7)
    q = target - RADIUS
    tile = jnp.where(source < 3, source, jnp.where(source == 3, 4, jnp.where(source == 7, 3, 6 - source)))
    line = jnp.where((source > 3) & (source < 7), q + 7 - source, q)
    lowest = own_rows + tile * 8 + line
    i = source - f_dev - RADIUS
    q = target - f_dev
    tile = jnp.where(i == 0, 3, jnp.where(i < 4, i - 1, jnp.where(i == 4, 4, 7 - i)))
    line = jnp.where(i >= 4, q - i, q)
    highest = own_rows + side + tile * 8 + line
    return jnp.where(source < RADIUS, lowest, jnp.where(source >= RADIUS + f_dev, highest, mine))


def fetch(flow_ref, weight_ref, mask_ref, flow3, weight3, mask3, sems):
    out = []
    for tile in range(flow3.shape[0]):
        cols = pl.ds(tile * L, L)
        pairs = [(mask_ref.at[:, cols], mask3.at[tile])]
        for comp in range(2):
            pairs.append((weight_ref.at[:, comp, cols], weight3.at[tile, comp]))
            pairs.append((flow_ref.at[:, comp, cols], flow3.at[tile, comp]))
        copies = [pltpu.make_async_copy(a, b, sems.at[tile, n]) for n, (a, b) in enumerate(pairs)]
        for copy in copies:
            copy.start()
        out.append(copies)
    return out


def aggregate(edge_ref, loads, flow3, weight3, mask3, own_ref, low_ref, high_ref, me, f_dev, ready):
    edges = edge_ref.shape[1]
    own = own_ref.shape[1]
    side = low_ref.shape[2]
    rows = own + 2 * side
    dest = destinations(edge_ref, own, side, f_dev, me)
    pick = (iota((rows, edges), 0) == dest).astype(F32).astype(BF16)
    for tile in range(len(loads)):
        cols = slice(tile * L, (tile + 1) * L)
        if tile % 3 == 0:
            for copies in loads[tile : tile + 3]:
                for copy in copies:
                    copy.wait()
        live = mask3[tile].astype(F32)
        fields = []
        for comp in range(2):
            conf = weight3[tile, comp] * live
            fields += [conf, conf * flow3[tile, comp]]
        high, low = split(jnp.concatenate(fields, axis=1))
        out = jnp.dot(pick, high, preferred_element_type=F32) + jnp.dot(
            pick, low, preferred_element_type=F32
        )
        for field in range(4):
            part = out[:, field * L : (field + 1) * L]
            own_ref[field, :, cols] = part[:own]
            low_ref[tile, field] = part[own : own + side]
            high_ref[tile, field] = part[own + side :]
        if tile % 3 == 2 or tile == len(loads) - 1:
            ready(range(tile - tile % 3, tile + 1))


def window(load, me, f_dev, frames):
    tiles = frames // L
    first = lax.rem(me * f_dev - RADIUS + frames, frames)
    tile = first // L
    back = lax.rem(L - lax.rem(first, L), L)
    near = pltpu.roll(load(pl.ds(pl.multiple_of(tile * L, L), L)), back, 1)
    if tiles == 1:
        return near
    after = lax.rem(tile + 1, tiles)
    far = pltpu.roll(load(pl.ds(pl.multiple_of(after * L, L), L)), back, 1)
    return jnp.where(iota(near.shape, 1) + lax.rem(first, L) < L, near, far)


def spread_rows(x):
    return jnp.concatenate([x, jnp.zeros((L - x.shape[0], L), F32)], axis=0).T


def motion_sums(u, v, uu, vv, a, b, ds):
    va, ub = v * a, u * b
    e0, e1 = ds * a, ds * b
    return [e0, e1, -(u * e0 + v * e1), -(u * va + vv * b), uu * a + v * ub, ub - va]


def curvature_sums(u, v, uu, vv, uv, ds, wu, wv):
    a1, b1 = wu * v, wv * u
    a2, b2 = a1 * u, b1 * v
    a3, b3 = wu * uu, wv * vv
    h00, h11 = wu * ds * ds, wv * ds * ds
    h02, h12 = h00 * u, h11 * v
    x1, x2, x3 = ds * a1, ds * a2, ds * a3
    y1, y2, y3 = ds * b1, ds * b2, ds * b3
    return [
        h00, h02, x2, x3, x1,
        h11, h12, y3, y2, y1,
        h02 * u + h12 * v, u * x2 + v * y3, u * x3 + v * y2, x2 - y2,
        a2 * uv + b3 * vv, uv * (a3 + b3), a2 * v - b3 * u,
        a3 * uu + b2 * uv, b2 * u - a3 * v,
        a1 * v + b1 * u,
    ]


SIGNS = [1, -1, -1, 1, -1, 1, -1, -1, 1, 1, 1, 1, -1, 1, 1, -1, 1, 1, 1, 1]


def adj_t(rel, tr, vec):
    turn = [
        vec[3] - (tr[1] * vec[2] - tr[2] * vec[1]),
        vec[4] - (tr[2] * vec[0] - tr[0] * vec[2]),
        vec[5] - (tr[0] * vec[1] - tr[1] * vec[0]),
    ]
    out = [rel[j] * vec[0] + rel[3 + j] * vec[1] + rel[6 + j] * vec[2] for j in range(3)]
    return out + [rel[j] * turn[0] + rel[3 + j] * turn[1] + rel[6 + j] * turn[2] for j in range(3)]


def fold(x):
    row = iota((8, L), 0)

    def merge(a, b, bit):
        other = (row & bit) != 0
        return jnp.where(other, b, a) + pltpu.roll(jnp.where(other, a, b), bit, 0)

    first, second, third = merge(x[0], x[1], 1), merge(x[2], x[3], 1), merge(x[4], x[5], 1)
    return merge(merge(first, second, 2), third + pltpu.roll(third, 2, 0), 4)


def pair_pose(frame_ref, s, first, after):
    here = [frame_ref[k, pl.ds(s + RADIUS, 1), :] for k in range(12)]
    there = [
        jnp.where(after, frame_ref[k, first : first + 8, :], frame_ref[k, first + 8 : first + 16, :])
        for k in range(12)
    ]
    rel = [
        there[3 * r] * here[3 * c] + there[3 * r + 1] * here[3 * c + 1] + there[3 * r + 2] * here[3 * c + 2]
        for r in range(3)
        for c in range(3)
    ]
    tr = [
        there[9 + r] - (rel[3 * r] * here[9] + rel[3 * r + 1] * here[10] + rel[3 * r + 2] * here[11])
        for r in range(3)
    ]
    return rel, tr


def octet(fields, depth, col, rowc, rel, tr):
    wu, fu, wv, fv = fields
    point = [
        rel[3 * k] * col + rel[3 * k + 1] * rowc + rel[3 * k + 2] + depth * tr[k] for k in range(3)
    ]
    iz = 1.0 / point[2]
    u = point[0] * iz
    v = point[1] * iz
    ds = depth * iz
    su = iz * (tr[0] - u * tr[2])
    sv = iz * (tr[1] - v * tr[2])
    au = wu * su
    av = wv * sv
    gu = wu * (col - u) + fu
    gv = wv * (rowc - v) + fv
    uu = 1.0 + u * u
    vv = 1.0 + v * v
    uv = u * v
    e = motion_sums(u, v, uu, vv, au, av, ds)
    back = adj_t(rel, tr, e)
    sums = curvature_sums(u, v, uu, vv, uv, ds, wu, wv) + motion_sums(u, v, uu, vv, gu, gv, ds)
    return e, back, au * su + av * sv, su * gu + sv * gv, sums


def prepare(pose_ref, frame_ref, coord_ref, depth_ref, damp_ref, depth3, damp3):
    tiles = depth3.shape[0]
    ox, oy, oz = pose_ref[0], pose_ref[1], pose_ref[2]
    zero = jnp.zeros_like(ox)
    cross = [[zero, -oz, oy], [oz, zero, -ox], [-oy, ox, zero]]
    sq = ox * ox + oy * oy + oz * oz
    c1 = 1.0 - sq / 6.0 + sq * sq / 120.0
    c2 = 0.5 - sq / 24.0 + sq * sq / 720.0
    for r in range(3):
        for c in range(3):
            square = cross[r][0] * cross[0][c] + cross[r][1] * cross[1][c] + cross[r][2] * cross[2][c]
            frame_ref[3 * r + c] = float(r == c) + c1 * cross[r][c] + c2 * square
        frame_ref[9 + r] = pose_ref[3 + r]
    first = lax.axis_index("pix") * (tiles * L)
    for tile in range(tiles):
        depth3[tile] = depth_ref[:, tile * L : (tile + 1) * L]
        damp3[tile] = damp_ref[:, tile * L : (tile + 1) * L]
        pixel = first + tile * L + iota((8, L), 1)
        prow = pixel // COLS
        pcol = pixel - prow * COLS
        coord_ref[tile, 0] = (pcol.astype(F32) - 0.5 * (COLS - 1)) / COLS
        coord_ref[tile, 1] = (prow.astype(F32) - 0.5 * (ROWS - 1)) / COLS


def note(at, sums, pose, sum_ref, pair_ref):
    for n, x in enumerate(sums):
        sum_ref[n] = jnp.where(at, jnp.sum(x, axis=1, keepdims=True), sum_ref[n])
    for n, x in enumerate(pose):
        pair_ref[n] = jnp.where(at, x, pair_ref[n])


def near_pairs(own_ref, frame_ref, coord_ref, depth3, e_ref, part_ref, sum_ref, pair_ref, descend):
    tiles, f_dev = depth3.shape[:2]
    half = f_dev // 2
    row = iota((8, L), 0)
    lane = iota((8, L), 1)
    sum_ref[...] = jnp.zeros_like(sum_ref)
    pair_ref[...] = jnp.zeros_like(pair_ref)
    for part in range(2):

        @pl.loop(0, half)
        def per_source(i):
            s = i + part * half
            rel, tr = pair_pose(frame_ref, s, 8, row > i if part == 0 else row >= i)
            sums = None
            for tile in range(tiles):
                cols = slice(tile * L, (tile + 1) * L)
                at = pl.ds(pl.multiple_of(s * 8, 8), 8)
                fields = [own_ref[k, at, cols] for k in range(4)]
                e, back, curv, grad, new = octet(
                    fields, depth3[tile, pl.ds(s, 1), :], coord_ref[tile, 0], coord_ref[tile, 1], rel, tr
                )
                slot = s * tiles + tile
                for j in range(6):
                    e_ref[slot, j] = e[j]
                for j in range(6):
                    part_ref[slot, j] = back[j]
                part_ref[slot, 6] = curv
                part_ref[slot, 7] = grad
                sums = new if sums is None else [a + b for a, b in zip(sums, new)]
            note(lane == s + RADIUS, sums, rel + tr, sum_ref, pair_ref)

        if part == 1:
            descend()


def far_pairs(
    own_ref, low_ref, high_ref, frame_ref, coord_ref, depth3, damp3, e_ref, part_ref, sum_ref, pair_ref,
    base_ref, inv_ref, zs, gram_ref, receive,
):
    tiles, f_dev = depth3.shape[:2]
    half = f_dev // 2
    row = iota((8, L), 0)
    lane = iota((8, L), 1)
    pair = iota((16, L), 0)
    size = 6 * WIN
    sum_ref[...] = jnp.zeros_like(sum_ref)
    pair_ref[...] = jnp.zeros_like(pair_ref)
    gram_ref[...] = jnp.zeros_like(gram_ref)
    zs[1][...] = jnp.zeros_like(zs[1])
    none = jnp.zeros((8, L), F32)

    def gram(which):
        z = zs[which][...]
        nt = (((1,), (1,)), ((), ()))
        gram_ref[...] += lax.dot_general(z, z[: size + 16], nt, preferred_element_type=F32)

    for part in range(2):
        receive(part)

        def per_source(i, which):
            s = i + part * half
            after = row >= i if part == 0 else row > i
            rel, tr = pair_pose(frame_ref, s, 0 if part == 0 else 16, after)
            if part == 0:
                slot = jnp.where(i == 0, 3, jnp.where(i < 4, i - 1, jnp.where(i == 4, 4, 7 - i)))
                shift = jnp.where(i >= 4, i, 0)
                keep = row >= i
                src = high_ref
            else:
                slot = jnp.where(i < 3, i, jnp.where(i == 3, 4, jnp.where(i == 7, 3, 6 - i)))
                shift = jnp.where((i > 3) & (i < 7), i + 1, 0)
                keep = row <= i
                src = low_ref
            sums = None
            for tile in range(tiles):
                cols = slice(tile * L, (tile + 1) * L)
                at = pl.ds(pl.multiple_of(f_dev * 8 + s * 8, 8), 8)
                fields = []
                for k in range(4):
                    got = src[tile, k, pl.ds(pl.multiple_of(slot * 8, 8), 8), :]
                    fields.append(jnp.where(keep, pltpu.roll(got, shift, 0), own_ref[k, at, cols]))
                e, back, curv, grad, new = octet(
                    fields, depth3[tile, pl.ds(s, 1), :], coord_ref[tile, 0], coord_ref[tile, 1], rel, tr
                )
                sums = new if sums is None else [a + b for a, b in zip(sums, new)]
                here = s * tiles + tile
                for j in range(6):
                    e_ref[here, 6 + j] = e[j]
                back = -fold([x + part_ref[here, j] for j, x in enumerate(back)])
                e_ref[here, 12] = back
                curv = jnp.sum(curv + part_ref[here, 6], axis=0, keepdims=True) + damp3[tile, pl.ds(s, 1), :]
                grad = -jnp.sum(grad + part_ref[here, 7], axis=0, keepdims=True)
                inv = 1.0 / curv
                scale = 1.0 / jnp.sqrt(curv)
                base_ref[tile, pl.ds(s, 1), :] = grad * inv
                inv_ref[tile, pl.ds(s, 1), :] = inv
                z = zs[which]
                skip = size + 16
                source = back * scale
                for j in range(6):
                    mine = e[j] * scale
                    other = e_ref[here, j] * scale
                    below, over = (mine, other) if part == 0 else (other, mine)
                    mid = jnp.where(row < i, below, jnp.where(row > i, over, source[j : j + 1, :]))
                    groups = [jnp.where(row >= i, below, 0.0), mid, jnp.where(row <= i, over, 0.0)]
                    groups = groups + [none] if part == 0 else [none] + groups
                    high, low = split(jnp.concatenate(groups, axis=0))
                    z[j * WIN : (j + 1) * WIN, cols] = high
                    z[skip + j * WIN : skip + (j + 1) * WIN, cols] = low
                y = grad * scale
                rest = y - y.astype(BF16).astype(F32)
                lines = jnp.where(pair == 0, y, jnp.where(pair == 1, rest, 0.0))
                z[size : size + 16, cols] = lines.astype(BF16)
            note(lane == s + RADIUS, sums, rel + tr, sum_ref, pair_ref)

        @pl.loop(0, half // 2)
        def per_two(k):
            gram(1)
            per_source(2 * k, 0)
            gram(0)
            per_source(2 * k + 1, 1)

    gram(1)


def assemble(near_sum, near_pair, far_sum, far_pair, gram_ref, matrix_ref, wide):
    size = 6 * WIN
    row = iota((8, L), 0)
    lane = iota((8, L), 1)
    i = lane & 7
    first = lane < 16

    def sides(near, far):
        return jnp.where(first, far, near), jnp.where(first, near, far)

    def expand(x):
        low, high = x
        mid = jnp.where(row < i, low, jnp.where(row > i, high, 0.0))
        start = jnp.where(row >= i, low, 0.0)
        end = jnp.where(row <= i, high, 0.0)
        return jnp.concatenate(
            [
                jnp.where(first, start, 0.0),
                jnp.where(first, mid, start),
                jnp.where(first, end, mid),
                jnp.where(first, 0.0, end),
            ],
            axis=0,
        )

    pose = [sides(near_pair[k], far_pair[k]) for k in range(12)]
    h = [[None] * 6 for _ in range(6)]
    wholes = [[None] * 6 for _ in range(6)]
    for n, (a, b) in enumerate(UPPER):
        pair = sides(near_sum[n], far_sum[n])
        h[a][b] = h[b][a] = pair if SIGNS[n] > 0 else tuple(-x for x in pair)
    count = len(UPPER)
    r = [tuple(-x for x in sides(near_sum[count + j], far_sum[count + j])) for j in range(6)]
    eye = iota((WIN, L), 0) == iota((WIN, L), 1)

    def total(terms):
        out = None
        for x, y in terms:
            if x is None or y is None:
                continue
            out = x * y if out is None else out + x * y
        return out

    had = [[[None, None] for _ in range(6)] for _ in range(6)]
    source = [[0.0] * 6 for _ in range(6)]
    lines = [0.0] * 6
    for side in range(2):
        rel = [pose[k][side] for k in range(9)]
        tr = [pose[9 + k][side] for k in range(3)]
        ad = [[None] * 6 for _ in range(6)]
        for c in range(3):
            corner = [
                tr[1] * rel[6 + c] - tr[2] * rel[3 + c],
                tr[2] * rel[c] - tr[0] * rel[6 + c],
                tr[0] * rel[3 + c] - tr[1] * rel[c],
            ]
            for a in range(3):
                ad[a][c] = ad[3 + a][3 + c] = rel[3 * a + c]
                ad[a][3 + c] = corner[a]
        for a in range(6):
            for b in range(6):
                had[a][b][side] = total(
                    [(None if h[a][k] is None else h[a][k][side], ad[k][b]) for k in range(6)]
                )
        for a in range(6):
            for b in range(6):
                source[a][b] = source[a][b] + total([(ad[k][a], had[k][b][side]) for k in range(6)])
        back = adj_t(rel, tr, [x[side] for x in r])
        lines = [x + y for x, y in zip(lines, back)]
    wide[...] = jnp.zeros_like(wide)
    matrix_ref[...] = jnp.zeros_like(matrix_ref)
    for a in range(6):
        rows = slice(a * WIN, (a + 1) * WIN)
        for b in range(6):
            cols = slice(b * WIN, (b + 1) * WIN)
            wide[rows, cols] = -expand(had[a][b])[:, :WIN]
            both = jnp.sum(source[a][b], axis=0, keepdims=True)
            if h[a][b] is not None:
                both = both + jnp.sum(expand(h[a][b]), axis=1, keepdims=True)
            matrix_ref[rows, cols] = jnp.where(eye, both, 0.0)[:, :WIN]
    high, low = gram_ref[:size, :], gram_ref[size + 16 :, :]
    wide[:size, :size] = wide[:size, :size] - low[:, :size]
    wide[:size, size : size + 1] = -(
        high[:, size : size + 1] + high[:, size + 1 : size + 2] + low[:, size : size + 1]
    )
    flipped = wide[...].T
    matrix_ref[:size, :size] = (
        matrix_ref[:size, :size] - high[:, :size] + wide[:size, :size] + flipped[:size, :size]
    )
    for j in range(6):
        cols = slice(j * WIN, (j + 1) * WIN)
        whole = jnp.sum(expand(r[j]), axis=1, keepdims=True)
        here = jnp.sum(jnp.where(eye, whole, 0.0), axis=0, keepdims=True)
        here = here - jnp.sum(lines[j], axis=0, keepdims=True)
        matrix_ref[size : size + 1, cols] = here[:, :WIN] + flipped[size : size + 1, cols]


def remote(src, dst, sems, phase, which, axis, peer):
    return pltpu.make_async_remote_copy(
        src_ref=src,
        dst_ref=dst,
        send_sem=sems.at[0, phase, which],
        recv_sem=sems.at[1, phase, which],
        device_id={axis: peer},
        device_id_type=pl.DeviceIdType.MESH,
    )


def peers(axis):
    count = lax.axis_size(axis)
    me = lax.axis_index(axis)
    return [lax.rem(me + step, count) for step in range(1, count)]


def pack(matrix_ref, packed_ref):
    size = 6 * WIN
    lane = iota((WIN, L), 1) % WIN
    row = iota((WIN, L), 0)
    inside = row + lane < WIN
    left = iota((BAND, L), 1) < L // 2
    packed_ref[...] = jnp.zeros_like(packed_ref)

    def skew(x):
        for bit in (1, 2, 4, 8, 16):
            x = jnp.where((lane & bit) != 0, pltpu.roll(x, WIN - bit, 0), x)
        return jnp.where(inside, x, 0.0)

    rest = []
    for j in range(6):
        rows = slice(j * WIN, (j + 1) * WIN)
        main = skew(matrix_ref[rows, :L])
        packed_ref[j * BAND : (j + 1) * BAND, :] = main[:BAND]
        packed_ref[6 * BAND + j : 6 * BAND + j + 1, :] = main[BAND : BAND + 1]
        rest.append(skew(matrix_ref[rows, L:]))
    base = 6 * BAND + 8
    for j in range(3):
        near = rest[j]
        far = pltpu.roll(rest[j + 3], L // 2, 1)
        packed_ref[base + j * BAND : base + (j + 1) * BAND, :] = jnp.where(left, near[:BAND], far[:BAND])
        at = base + 3 * BAND + j
        packed_ref[at : at + 1, :] = jnp.where(left[:1], near[BAND : BAND + 1], far[BAND : BAND + 1])
    packed_ref[6 * BAND + 6 : 6 * BAND + 7, :] = matrix_ref[size : size + 1, :L]
    packed_ref[base + 3 * BAND + 3 : base + 3 * BAND + 4, :] = jnp.where(
        left[:1], matrix_ref[size : size + 1, L:], 0.0
    )


def exchange(src, dst, sems, phase, axis):
    sent = []
    for peer in peers(axis):
        copy = remote(src(peer), dst, sems, phase, len(sent), axis, peer)
        copy.start()
        sent.append(copy)
    return sent


def operator(packed_ref, land, reduced_ref, gathered, diag_ref, ahead_ref, back_ref, far_ref, pix_sem, round_sem, mate_sem, f_dev, frames):
    zcount = lax.axis_size("pix")
    z = lax.axis_index("pix")
    count = lax.axis_size("frames")
    me = lax.axis_index("frames")
    chunk = land.shape[1]
    tiles = frames // L

    def piece(which):
        return pl.ds(pl.multiple_of(which * chunk, 8), chunk)

    sent = exchange(lambda peer: packed_ref.at[piece(peer)], land.at[z], pix_sem, 0, "pix")
    land[z] = packed_ref[piece(z), :]
    for copy in sent:
        copy.wait_recv()
    total = land[0]
    for k in range(1, zcount):
        total = total + land[k]
    reduced_ref[...] = total
    more = exchange(lambda peer: reduced_ref, gathered.at[me], round_sem, 0, "frames")
    gathered[me] = total
    for copy in more:
        copy.wait_recv()
    lane = iota((chunk, L), 1)
    sums = [[None] * tiles for _ in range(4)]
    for w in range(count):
        first = (w * f_dev - RADIUS) % frames
        start = first % L
        for k in range(4):
            part = pltpu.roll(gathered[w], (start - WIN * k) % L, 1)
            spans = [(first // L, start, min(start + WIN, L))]
            if start + WIN > L:
                spans.append(((first // L + 1) % tiles, 0, start + WIN - L))
            for tile, low, high in spans:
                term = jnp.where((lane >= low) & (lane < high), part, 0.0)
                sums[k][tile] = term if sums[k][tile] is None else sums[k][tile] + term
    for k in range(4):
        for tile in range(tiles):
            diag_ref[z, k, :, tile * L : (tile + 1) * L] = sums[k][tile]
    for copy in sent + more:
        copy.wait_send()
    mate = me + 1 - 2 * lax.rem(me, 2)
    mine = pl.ds(2 * lax.rem(me, 2), 2)
    half = diag_ref.at[z, mine]
    sent = exchange(lambda peer: half, half, pix_sem, 1, "pix")
    passed = []
    for n, (copy, step) in enumerate(zip(sent, range(zcount - 1, 0, -1))):
        copy.wait_recv()
        there = diag_ref.at[lax.rem(z + step, zcount), mine]
        handed = remote(there, there, mate_sem, 0, n, "frames", mate)
        handed.start()
        passed.append(handed)
    for copy in passed:
        copy.wait_recv()
    for copy in sent + passed:
        copy.wait_send()

    def block(k, at):
        return [
            diag_ref[at // chunk, k, at % chunk : at % chunk + 8, t * L : (t + 1) * L]
            for t in range(tiles)
        ]

    def entry(i, j, half):
        if i < 4:
            return block(i, BAND * j + 8 * half)
        return block(i - 4 + 2 * (j // 3), 6 * BAND + 8 + BAND * (j % 3) + 8 * half)

    row = iota((8, L), 0)
    lanes = iota((8, L), 1)

    def later(x, half):
        turned = [pltpu.roll(v, 8 * half, 1, stride=1, stride_axis=0) for v in x]
        if tiles == 1:
            return turned
        mine = lanes >= 8 * half + row
        return [jnp.where(mine, turned[t], turned[t - 1]) for t in range(tiles)]

    def flip(x):
        for bit in (4, 2, 1):
            x = jnp.where((row & bit) != 0, pltpu.roll(x, bit, 0), pltpu.roll(x, 8 - bit, 0))
        return x

    for i in range(6):
        for j in range(6):
            for half in range(2):
                front = entry(i, j, half)
                moved = later(entry(j, i, half), half)
                for t in range(tiles):
                    ahead_ref[i, 2 * j + half, :, t * L : (t + 1) * L] = flip(front[t])
                    value = jnp.where(row > 0, moved[t], 0.0) if half == 0 else moved[t]
                    back_ref[i, 2 * j + half, :, t * L : (t + 1) * L] = value
    edge = 6 * BAND
    last = edge + 8 + 3 * BAND
    for i in range(6):
        if i < 4:
            ends = block(i, edge)
        else:
            near, far = block(i - 4, last), block(i - 2, last)
            ends = [jnp.where(row < 3, a, pltpu.roll(b, 3, 0)) for a, b in zip(near, far)]
        for t in range(tiles):
            far_ref[i, :, t * L : (t + 1) * L] = jnp.where(row < 6, ends[t], 0.0)
    sources = [block(k, edge) for k in range(4)] + [block(k, last) for k in range(2)]
    rhs = []
    for t in range(tiles):
        out = jnp.zeros((8, L), F32)
        for i in range(6):
            at = 6 if i < 4 else 3
            out = jnp.where(row == i, sources[i][t][at : at + 1, :], out)
        rhs.append(out)
    return rhs, later


def conjugate(rhs, later, ahead_ref, back_ref, far_ref):
    tiles = len(rhs)
    row = iota((8, L), 0)
    lanes = iota((8, L), 1)

    def sooner(x, half):
        turned = [pltpu.roll(v, L - 8 * half - 7, 1, stride=1, stride_axis=0) for v in x]
        if tiles == 1:
            return turned
        mine = lanes + 8 * half + 7 - row < L
        return [jnp.where(mine, turned[t], turned[(t + 1) % tiles]) for t in range(tiles)]

    def moved(x, steps):
        turned = [pltpu.roll(v, steps % L, 1) for v in x]
        if tiles == 1:
            return turned
        if steps > 0:
            return [jnp.where(lanes >= steps, turned[t], turned[t - 1]) for t in range(tiles)]
        return [jnp.where(lanes < L + steps, turned[t], turned[(t + 1) % tiles]) for t in range(tiles)]

    def dot(x, y):
        total = x[0] * y[0]
        for t in range(1, tiles):
            total = total + x[t] * y[t]
        return jnp.sum(total, keepdims=True)

    def product(p):
        ahead = moved(p, -BAND)
        acc = [[far_ref[i, :, t * L : (t + 1) * L] * ahead[t] for t in range(tiles)] for i in range(6)]
        tail = [None] * tiles
        for j in range(6):
            wide = [jnp.broadcast_to(v[j : j + 1, :], (8, L)) for v in p]
            for t in range(tiles):
                term = far_ref[j, :, t * L : (t + 1) * L] * wide[t]
                tail[t] = term if tail[t] is None else tail[t] + term
            for half in range(2):
                plus = sooner(wide, half)
                minus = later(wide, half)
                for i in range(6):
                    for t in range(tiles):
                        acc[i][t] = (
                            acc[i][t]
                            + ahead_ref[i, 2 * j + half, :, t * L : (t + 1) * L] * plus[t]
                            + back_ref[i, 2 * j + half, :, t * L : (t + 1) * L] * minus[t]
                        )
        tail = moved(tail, BAND)
        out = []
        for t in range(tiles):
            y = tail[t] + REG * p[t]
            for i in range(6):
                y = y + jnp.where(row == i, jnp.sum(acc[i][t], axis=0, keepdims=True), 0.0)
            out.append(y)
        return out

    def step(_, carry):
        x, residual, direction, rr = carry
        image = product(direction)
        alpha = rr / dot(direction, image)
        x = [a + alpha * b for a, b in zip(x, direction)]
        residual = [a - alpha * b for a, b in zip(residual, image)]
        new = dot(residual, residual)
        beta = new / rr
        direction = [a + beta * b for a, b in zip(residual, direction)]
        return x, residual, direction, new

    zero = [jnp.zeros((8, L), F32)] * tiles
    return lax.fori_loop(0, ITERS, step, (zero, rhs, rhs, dot(rhs, rhs)))[0]


def finish(
    matrix_ref, e_ref, base_ref, inv_ref, pose_ref, step_ref, frames,
    cols_ref, step3, packed_ref, land, reduced_ref, gathered, diag_ref, ahead_ref, back_ref, far_ref, x_ref,
    pix_sem, round_sem, mate_sem,
):
    me = lax.axis_index("frames")
    tiles, f_dev = step3.shape[:2]
    half = f_dev // 2
    pack(matrix_ref, packed_ref)
    rhs, later = operator(
        packed_ref, land, reduced_ref, gathered, diag_ref, ahead_ref, back_ref, far_ref,
        pix_sem, round_sem, mate_sem, f_dev, frames,
    )
    x = conjugate(rhs, later, ahead_ref, back_ref, far_ref)
    for t, value in enumerate(x):
        x_ref[:, t * L : (t + 1) * L] = value
    mine = window(lambda at: x_ref[:, at], me, f_dev, frames)
    pose_ref[...] = mine[:6, RADIUS : RADIUS + f_dev]
    turned = spread_rows(mine)
    for i in range(6):
        cols_ref[i] = jnp.broadcast_to(turned[:WIN, i : i + 1], (WIN, L))
    row = iota((8, L), 0)
    lane = iota((8, L), 1)
    for part in range(2):

        @pl.loop(0, half)
        def per_source(i):
            s = i + part * half
            group = [[cols_ref[j, 8 * g : 8 * g + 8, :] for g in range(part, part + 3)] for j in range(6)]
            below = [jnp.where(row >= i, group[j][0], group[j][1]) for j in range(6)]
            over = [jnp.where(row > i, group[j][1], group[j][2]) for j in range(6)]
            near, far = (over, below) if part == 0 else (below, over)
            at = jnp.sum(jnp.where(lane == s + RADIUS, mine, 0.0), axis=1, keepdims=True)
            terms = near + far + [jnp.broadcast_to(at, (8, L))]
            for tile in range(tiles):
                slot = s * tiles + tile
                image = e_ref[slot, 0] * terms[0]
                for n in range(1, 13):
                    image = image + e_ref[slot, n] * terms[n]
                image = jnp.sum(image, axis=0, keepdims=True)
                here = (tile, pl.ds(s, 1), slice(None))
                step3[here] = base_ref[here] - inv_ref[here] * image

    for tile in range(tiles):
        step_ref[:, tile * L : (tile + 1) * L] = step3[tile]


def swap_edges(low_out, high_out, low_ref, high_ref, sems):
    count = lax.axis_size("frames")
    me = lax.axis_index("frames")
    below = lax.rem(me + count - 1, count)
    over = lax.rem(me + 1, count)
    tiles = low_out.shape[0]
    down = [remote(low_out.at[t, :, :SENT], low_ref.at[t, :, :SENT], sems, 0, t, "frames", below) for t in range(tiles)]
    up = [remote(high_out.at[t, :, :SENT], high_ref.at[t, :, :SENT], sems, 1, t, "frames", over) for t in range(tiles)]

    def ascend(span):
        @pl.when(me < count - 1)
        def _():
            for t in span:
                up[t].start()

    def descend():
        @pl.when(me > 0)
        def _():
            for copy in down:
                copy.start()

    def receive(part):
        if part == 0:

            @pl.when(me > 0)
            def _():
                for copy in up:
                    copy.wait_recv()

            @pl.when(me == 0)
            def _():
                high_ref[...] = jnp.zeros_like(high_ref)

        else:

            @pl.when(me < count - 1)
            def _():
                for copy in down:
                    copy.wait_recv()

            @pl.when(me == count - 1)
            def _():
                low_ref[...] = jnp.zeros_like(low_ref)

    def drain():
        @pl.when(me > 0)
        def _():
            for copy in down:
                copy.wait_send()

        @pl.when(me < count - 1)
        def _():
            for copy in up:
                copy.wait_send()

    return ascend, descend, receive, drain


def solve(
    edge_ref, rot_ref, trans_ref, depth_ref, damp_ref, flow_ref, weight_ref, mask_ref,
    x_ref, step_ref, flow3, weight3, mask3, load_sem, pose_ref,
    own_ref, low_out, high_out, low_ref, high_ref, edge_sem,
    frame_ref, coord_ref, depth3, damp3, e_ref, part_ref, near_sum, near_pair, far_sum, far_pair,
    base_ref, inv_ref, z0, z1, gram_ref, matrix_ref, wide, *scratch,
):
    me = lax.axis_index("frames")
    f_dev, pix = depth_ref.shape
    frames = rot_ref.shape[1]
    loads = fetch(flow_ref, weight_ref, mask_ref, flow3, weight3, mask3, load_sem)
    barrier = pltpu.get_barrier_semaphore()
    total = 0
    for axis in ("frames", "pix"):
        for peer in peers(axis):
            pl.semaphore_signal(
                barrier, inc=1, device_id={axis: peer}, device_id_type=pl.DeviceIdType.MESH
            )
            total += 1
    poses = []
    for ref in (rot_ref, trans_ref):
        poses.append(window(lambda at: ref[:, at], me, f_dev, frames))
    turned = spread_rows(jnp.concatenate(poses, axis=0))
    for k in range(6):
        pose_ref[k] = jnp.broadcast_to(turned[:WIN, k : k + 1], (WIN, L))
    prepare(pose_ref, frame_ref, coord_ref, depth_ref, damp_ref, depth3, damp3)
    ascend, descend, receive, drain = swap_edges(low_out, high_out, low_ref, high_ref, edge_sem)

    def ready(span):
        if span[0] == 0:
            pl.semaphore_wait(barrier, total)
        ascend(span)

    aggregate(edge_ref, loads, flow3, weight3, mask3, own_ref, low_out, high_out, me, f_dev, ready)
    near_pairs(own_ref, frame_ref, coord_ref, depth3, e_ref, part_ref, near_sum, near_pair, descend)
    far_pairs(
        own_ref, low_ref, high_ref, frame_ref, coord_ref, depth3, damp3, e_ref, part_ref,
        far_sum, far_pair, base_ref, inv_ref, (z0, z1), gram_ref, receive,
    )
    assemble(near_sum, near_pair, far_sum, far_pair, gram_ref, matrix_ref, wide)
    finish(matrix_ref, e_ref, base_ref, inv_ref, x_ref, step_ref, frames, *scratch)
    drain()


def call(body, out, scratch, vmem, hbm, **params):
    vm = pl.BlockSpec(memory_space=pltpu.VMEM)
    far = pl.BlockSpec(memory_space=pl.ANY)
    return pl.pallas_call(
        body,
        out_shape=[pltpu.VMEM(s, t) for s, t in out],
        in_specs=[vm] * vmem + [far] * hbm,
        out_specs=[vm] * len(out),
        scratch_shapes=scratch,
        compiler_params=pltpu.CompilerParams(vmem_limit_bytes=VMEM_LIMIT, **params),
    )


def per_device(edge_frames, rotvec, trans, inv_depth, depth_damping, flow, weight, mask):
    f_dev, pix = inv_depth.shape
    edges = mask.shape[0]
    frames = rotvec.shape[1]
    tiles = pix // L
    own_rows = f_dev * 16
    side = 40
    sums = len(UPPER) + 6
    width = 256
    size = 6 * WIN
    count = lax.axis_size("frames")
    zcount = lax.axis_size("pix")
    chunk = -(-PACKED // (8 * zcount)) * 8
    x, step = call(
        solve,
        [((6, f_dev), F32), ((f_dev, pix), F32)],
        [
            pltpu.VMEM((tiles, 2, edges, L), F32),
            pltpu.VMEM((tiles, 2, edges, L), F32),
            pltpu.VMEM((tiles, edges, L), jnp.int32),
            pltpu.SemaphoreType.DMA((tiles, 5)),
            pltpu.VMEM((6, WIN, L), F32),
            pltpu.VMEM((4, own_rows, pix), F32),
            pltpu.VMEM((tiles, 4, side, L), F32),
            pltpu.VMEM((tiles, 4, side, L), F32),
            pltpu.VMEM((tiles, 4, side, L), F32),
            pltpu.VMEM((tiles, 4, side, L), F32),
            pltpu.SemaphoreType.DMA((2, 2, tiles)),
            pltpu.VMEM((12, WIN, L), F32),
            pltpu.VMEM((tiles, 2, 8, L), F32),
            pltpu.VMEM((tiles, f_dev, L), F32),
            pltpu.VMEM((tiles, f_dev, L), F32),
            pltpu.VMEM((f_dev * tiles, 13, 8, L), F32),
            pltpu.VMEM((f_dev * tiles, 8, 8, L), F32),
            pltpu.VMEM((sums, 8, L), F32),
            pltpu.VMEM((12, 8, L), F32),
            pltpu.VMEM((sums, 8, L), F32),
            pltpu.VMEM((12, 8, L), F32),
            pltpu.VMEM((tiles, f_dev, L), F32),
            pltpu.VMEM((tiles, f_dev, L), F32),
            pltpu.VMEM((2 * size + 16, pix), BF16),
            pltpu.VMEM((2 * size + 16, pix), BF16),
            pltpu.VMEM((2 * size + 16, size + 16), F32),
            pltpu.VMEM((size + 8, width), F32),
            pltpu.VMEM((256, 256), F32),
            pltpu.VMEM((6, WIN, L), F32),
            pltpu.VMEM((tiles, f_dev, L), F32),
            pltpu.VMEM((chunk * zcount, L), F32),
            pltpu.VMEM((zcount, chunk, L), F32),
            pltpu.VMEM((chunk, L), F32),
            pltpu.VMEM((count, chunk, L), F32),
            pltpu.VMEM((zcount, 4, chunk, frames), F32),
            pltpu.VMEM((6, 12, 8, frames), F32),
            pltpu.VMEM((6, 12, 8, frames), F32),
            pltpu.VMEM((6, 8, frames), F32),
            pltpu.VMEM((8, frames), F32),
            pltpu.SemaphoreType.DMA((2, 2, zcount)),
            pltpu.SemaphoreType.DMA((2, 1, count)),
            pltpu.SemaphoreType.DMA((2, 1, zcount)),
        ],
        5, 3, collective_id=0, has_side_effects=True,
    )(edge_frames, rotvec, trans, inv_depth, depth_damping, flow, weight, mask)
    return x, step


def solution(mesh):
    return jax.shard_map(
        per_device,
        mesh=mesh,
        in_specs=(
            P(None, "frames"),
            P(),
            P(),
            P("frames", "pix"),
            P("frames", "pix"),
            P("frames", None, "pix"),
            P("frames", None, "pix"),
            P("frames", "pix"),
        ),
        out_specs=(P(None, "frames"), P("frames", "pix")),
        check_vma=False,
    )
```

```python
import jax
import jax.numpy as jnp
from jax import lax
from jax.experimental import pallas as pl
from jax.experimental.pallas import tpu as pltpu
from jax.sharding import PartitionSpec as P

ROWS = 48
COLS = 64
RADIUS = 8
ITERS = 6
REG = 100.0
F32 = jnp.float32
BF16 = jnp.bfloat16
L = 128
WIN = 32
BAND = 2 * RADIUS
PACKED = 160
SENT = RADIUS * (RADIUS + 1) // 2
VMEM_LIMIT = 60 * 1024 * 1024
UPPER = [(i, j) for i in range(6) for j in range(i, 6) if (i, j) != (0, 1)]


def split(x):
    high = x.astype(BF16)
    return high, (x - high.astype(F32)).astype(BF16)


def iota(shape, dim):
    return lax.broadcasted_iota(jnp.int32, shape, dim)


def destinations(edge_ref, own_rows, side, f_dev, me):
    start = me * f_dev
    source = edge_ref[0:1, :] - start + RADIUS
    target = edge_ref[1:2, :] - start + RADIUS
    s = source - RADIUS
    low = jnp.where(s < f_dev // 2, 1, 0)
    above = jnp.where(target > source, 1, 0)
    mine = jnp.where(low == above, 0, f_dev * 8) + s * 8 + (target & 7)
    q = target - RADIUS
    tile = jnp.where(source < 3, source, jnp.where(source == 3, 4, jnp.where(source == 7, 3, 6 - source)))
    line = jnp.where((source > 3) & (source < 7), q + 7 - source, q)
    lowest = own_rows + tile * 8 + line
    i = source - f_dev - RADIUS
    q = target - f_dev
    tile = jnp.where(i == 0, 3, jnp.where(i < 4, i - 1, jnp.where(i == 4, 4, 7 - i)))
    line = jnp.where(i >= 4, q - i, q)
    highest = own_rows + side + tile * 8 + line
    return jnp.where(source < RADIUS, lowest, jnp.where(source >= RADIUS + f_dev, highest, mine))


def fetch(flow_ref, weight_ref, mask_ref, flow3, weight3, mask3, sems):
    out = []
    for tile in range(flow3.shape[0]):
        cols = pl.ds(tile * L, L)
        pairs = [(mask_ref.at[:, cols], mask3.at[tile])]
        for comp in range(2):
            pairs.append((weight_ref.at[:, comp, cols], weight3.at[tile, comp]))
            pairs.append((flow_ref.at[:, comp, cols], flow3.at[tile, comp]))
        copies = [pltpu.make_async_copy(a, b, sems.at[tile, n]) for n, (a, b) in enumerate(pairs)]
        for copy in copies:
            copy.start()
        out.append(copies)
    return out


def aggregate(edge_ref, loads, flow3, weight3, mask3, own_ref, low_ref, high_ref, me, f_dev, ready):
    edges = edge_ref.shape[1]
    own = own_ref.shape[1]
    side = low_ref.shape[2]
    rows = own + 2 * side
    dest = destinations(edge_ref, own, side, f_dev, me)
    pick = (iota((rows, edges), 0) == dest).astype(F32).astype(BF16)
    for tile in range(len(loads)):
        cols = slice(tile * L, (tile + 1) * L)
        if tile % 3 == 0:
            for copies in loads[tile : tile + 3]:
                for copy in copies:
                    copy.wait()
        live = mask3[tile].astype(F32)
        fields = []
        for comp in range(2):
            conf = weight3[tile, comp] * live
            fields += [conf, conf * flow3[tile, comp]]
        high, low = split(jnp.concatenate(fields, axis=1))
        out = jnp.dot(pick, high, preferred_element_type=F32) + jnp.dot(
            pick, low, preferred_element_type=F32
        )
        for field in range(4):
            part = out[:, field * L : (field + 1) * L]
            own_ref[field, :, cols] = part[:own]
            low_ref[tile, field] = part[own : own + side]
            high_ref[tile, field] = part[own + side :]
        if tile % 3 == 2 or tile == len(loads) - 1:
            ready(range(tile - tile % 3, tile + 1))


def window(load, me, f_dev, frames):
    tiles = frames // L
    first = lax.rem(me * f_dev - RADIUS + frames, frames)
    tile = first // L
    back = lax.rem(L - lax.rem(first, L), L)
    near = pltpu.roll(load(pl.ds(pl.multiple_of(tile * L, L), L)), back, 1)
    if tiles == 1:
        return near
    after = lax.rem(tile + 1, tiles)
    far = pltpu.roll(load(pl.ds(pl.multiple_of(after * L, L), L)), back, 1)
    return jnp.where(iota(near.shape, 1) + lax.rem(first, L) < L, near, far)


def spread_rows(x):
    return jnp.concatenate([x, jnp.zeros((L - x.shape[0], L), F32)], axis=0).T


def motion_sums(u, v, uu, vv, a, b, ds):
    va, ub = v * a, u * b
    e0, e1 = ds * a, ds * b
    return [e0, e1, -(u * e0 + v * e1), -(u * va + vv * b), uu * a + v * ub, ub - va]


def curvature_sums(u, v, uu, vv, uv, ds, wu, wv):
    a1, b1 = wu * v, wv * u
    a2, b2 = a1 * u, b1 * v
    a3, b3 = wu * uu, wv * vv
    h00, h11 = wu * ds * ds, wv * ds * ds
    h02, h12 = h00 * u, h11 * v
    x1, x2, x3 = ds * a1, ds * a2, ds * a3
    y1, y2, y3 = ds * b1, ds * b2, ds * b3
    return [
        h00, h02, x2, x3, x1,
        h11, h12, y3, y2, y1,
        h02 * u + h12 * v, u * x2 + v * y3, u * x3 + v * y2, x2 - y2,
        a2 * uv + b3 * vv, uv * (a3 + b3), a2 * v - b3 * u,
        a3 * uu + b2 * uv, b2 * u - a3 * v,
        a1 * v + b1 * u,
    ]


SIGNS = [1, -1, -1, 1, -1, 1, -1, -1, 1, 1, 1, 1, -1, 1, 1, -1, 1, 1, 1, 1]


def adj_t(rel, tr, vec):
    turn = [
        vec[3] - (tr[1] * vec[2] - tr[2] * vec[1]),
        vec[4] - (tr[2] * vec[0] - tr[0] * vec[2]),
        vec[5] - (tr[0] * vec[1] - tr[1] * vec[0]),
    ]
    out = [rel[j] * vec[0] + rel[3 + j] * vec[1] + rel[6 + j] * vec[2] for j in range(3)]
    return out + [rel[j] * turn[0] + rel[3 + j] * turn[1] + rel[6 + j] * turn[2] for j in range(3)]


def fold(x):
    row = iota((8, L), 0)

    def merge(a, b, bit):
        other = (row & bit) != 0
        return jnp.where(other, b, a) + pltpu.roll(jnp.where(other, a, b), bit, 0)

    first, second, third = merge(x[0], x[1], 1), merge(x[2], x[3], 1), merge(x[4], x[5], 1)
    return merge(merge(first, second, 2), third + pltpu.roll(third, 2, 0), 4)


def pair_pose(frame_ref, s, first, after):
    here = [frame_ref[k, pl.ds(s + RADIUS, 1), :] for k in range(12)]
    there = [
        jnp.where(after, frame_ref[k, first : first + 8, :], frame_ref[k, first + 8 : first + 16, :])
        for k in range(12)
    ]
    rel = [
        there[3 * r] * here[3 * c] + there[3 * r + 1] * here[3 * c + 1] + there[3 * r + 2] * here[3 * c + 2]
        for r in range(3)
        for c in range(3)
    ]
    tr = [
        there[9 + r] - (rel[3 * r] * here[9] + rel[3 * r + 1] * here[10] + rel[3 * r + 2] * here[11])
        for r in range(3)
    ]
    return rel, tr


def octet(fields, depth, col, rowc, rel, tr):
    wu, fu, wv, fv = fields
    point = [
        rel[3 * k] * col + rel[3 * k + 1] * rowc + rel[3 * k + 2] + depth * tr[k] for k in range(3)
    ]
    iz = 1.0 / point[2]
    u = point[0] * iz
    v = point[1] * iz
    ds = depth * iz
    su = iz * (tr[0] - u * tr[2])
    sv = iz * (tr[1] - v * tr[2])
    au = wu * su
    av = wv * sv
    gu = wu * (col - u) + fu
    gv = wv * (rowc - v) + fv
    uu = 1.0 + u * u
    vv = 1.0 + v * v
    uv = u * v
    e = motion_sums(u, v, uu, vv, au, av, ds)
    back = adj_t(rel, tr, e)
    sums = curvature_sums(u, v, uu, vv, uv, ds, wu, wv) + motion_sums(u, v, uu, vv, gu, gv, ds)
    return e, back, au * su + av * sv, su * gu + sv * gv, sums


def prepare(pose_ref, frame_ref, coord_ref, depth_ref, damp_ref, depth3, damp3):
    tiles = depth3.shape[0]
    ox, oy, oz = pose_ref[0], pose_ref[1], pose_ref[2]
    zero = jnp.zeros_like(ox)
    cross = [[zero, -oz, oy], [oz, zero, -ox], [-oy, ox, zero]]
    sq = ox * ox + oy * oy + oz * oz
    c1 = 1.0 - sq / 6.0 + sq * sq / 120.0
    c2 = 0.5 - sq / 24.0 + sq * sq / 720.0
    for r in range(3):
        for c in range(3):
            square = cross[r][0] * cross[0][c] + cross[r][1] * cross[1][c] + cross[r][2] * cross[2][c]
            frame_ref[3 * r + c] = float(r == c) + c1 * cross[r][c] + c2 * square
        frame_ref[9 + r] = pose_ref[3 + r]
    first = lax.axis_index("pix") * (tiles * L)
    for tile in range(tiles):
        depth3[tile] = depth_ref[:, tile * L : (tile + 1) * L]
        damp3[tile] = damp_ref[:, tile * L : (tile + 1) * L]
        pixel = first + tile * L + iota((8, L), 1)
        prow = pixel // COLS
        pcol = pixel - prow * COLS
        coord_ref[tile, 0] = (pcol.astype(F32) - 0.5 * (COLS - 1)) / COLS
        coord_ref[tile, 1] = (prow.astype(F32) - 0.5 * (ROWS - 1)) / COLS


def note(at, sums, pose, sum_ref, pair_ref):
    for n, x in enumerate(sums):
        sum_ref[n] = jnp.where(at, jnp.sum(x, axis=1, keepdims=True), sum_ref[n])
    for n, x in enumerate(pose):
        pair_ref[n] = jnp.where(at, x, pair_ref[n])


def near_pairs(own_ref, frame_ref, coord_ref, depth3, e_ref, part_ref, sum_ref, pair_ref, descend):
    tiles, f_dev = depth3.shape[:2]
    half = f_dev // 2
    row = iota((8, L), 0)
    lane = iota((8, L), 1)
    sum_ref[...] = jnp.zeros_like(sum_ref)
    pair_ref[...] = jnp.zeros_like(pair_ref)
    for part in range(2):

        @pl.loop(0, half)
        def per_source(i):
            s = i + part * half
            rel, tr = pair_pose(frame_ref, s, 8, row > i if part == 0 else row >= i)
            sums = None
            for tile in range(tiles):
                cols = slice(tile * L, (tile + 1) * L)
                at = pl.ds(pl.multiple_of(s * 8, 8), 8)
                fields = [own_ref[k, at, cols] for k in range(4)]
                e, back, curv, grad, new = octet(
                    fields, depth3[tile, pl.ds(s, 1), :], coord_ref[tile, 0], coord_ref[tile, 1], rel, tr
                )
                slot = s * tiles + tile
                for j in range(6):
                    e_ref[slot, j] = e[j]
                for j in range(6):
                    part_ref[slot, j] = back[j]
                part_ref[slot, 6] = curv
                part_ref[slot, 7] = grad
                sums = new if sums is None else [a + b for a, b in zip(sums, new)]
            note(lane == s + RADIUS, sums, rel + tr, sum_ref, pair_ref)

        if part == 1:
            descend()


def far_pairs(
    own_ref, low_ref, high_ref, frame_ref, coord_ref, depth3, damp3, e_ref, part_ref, sum_ref, pair_ref,
    base_ref, inv_ref, zs, gram_ref, receive,
):
    tiles, f_dev = depth3.shape[:2]
    half = f_dev // 2
    row = iota((8, L), 0)
    lane = iota((8, L), 1)
    pair = iota((16, L), 0)
    size = 6 * WIN
    sum_ref[...] = jnp.zeros_like(sum_ref)
    pair_ref[...] = jnp.zeros_like(pair_ref)
    gram_ref[...] = jnp.zeros_like(gram_ref)
    zs[1][...] = jnp.zeros_like(zs[1])
    none = jnp.zeros((8, L), F32)

    def gram(which):
        z = zs[which][...]
        nt = (((1,), (1,)), ((), ()))
        gram_ref[...] += lax.dot_general(z, z[: size + 16], nt, preferred_element_type=F32)

    for part in range(2):
        receive(part)

        def per_source(i, which):
            s = i + part * half
            after = row >= i if part == 0 else row > i
            rel, tr = pair_pose(frame_ref, s, 0 if part == 0 else 16, after)
            if part == 0:
                slot = jnp.where(i == 0, 3, jnp.where(i < 4, i - 1, jnp.where(i == 4, 4, 7 - i)))
                shift = jnp.where(i >= 4, i, 0)
                keep = row >= i
                src = high_ref
            else:
                slot = jnp.where(i < 3, i, jnp.where(i == 3, 4, jnp.where(i == 7, 3, 6 - i)))
                shift = jnp.where((i > 3) & (i < 7), i + 1, 0)
                keep = row <= i
                src = low_ref
            sums = None
            for tile in range(tiles):
                cols = slice(tile * L, (tile + 1) * L)
                at = pl.ds(pl.multiple_of(f_dev * 8 + s * 8, 8), 8)
                fields = []
                for k in range(4):
                    got = src[tile, k, pl.ds(pl.multiple_of(slot * 8, 8), 8), :]
                    fields.append(jnp.where(keep, pltpu.roll(got, shift, 0), own_ref[k, at, cols]))
                e, back, curv, grad, new = octet(
                    fields, depth3[tile, pl.ds(s, 1), :], coord_ref[tile, 0], coord_ref[tile, 1], rel, tr
                )
                sums = new if sums is None else [a + b for a, b in zip(sums, new)]
                here = s * tiles + tile
                for j in range(6):
                    e_ref[here, 6 + j] = e[j]
                back = -fold([x + part_ref[here, j] for j, x in enumerate(back)])
                e_ref[here, 12] = back
                curv = jnp.sum(curv + part_ref[here, 6], axis=0, keepdims=True) + damp3[tile, pl.ds(s, 1), :]
                grad = -jnp.sum(grad + part_ref[here, 7], axis=0, keepdims=True)
                inv = 1.0 / curv
                scale = 1.0 / jnp.sqrt(curv)
                base_ref[tile, pl.ds(s, 1), :] = grad * inv
                inv_ref[tile, pl.ds(s, 1), :] = inv
                z = zs[which]
                skip = size + 16
                source = back * scale
                for j in range(6):
                    mine = e[j] * scale
                    other = e_ref[here, j] * scale
                    below, over = (mine, other) if part == 0 else (other, mine)
                    mid = jnp.where(row < i, below, jnp.where(row > i, over, source[j : j + 1, :]))
                    groups = [jnp.where(row >= i, below, 0.0), mid, jnp.where(row <= i, over, 0.0)]
                    groups = groups + [none] if part == 0 else [none] + groups
                    high, low = split(jnp.concatenate(groups, axis=0))
                    z[j * WIN : (j + 1) * WIN, cols] = high
                    z[skip + j * WIN : skip + (j + 1) * WIN, cols] = low
                y = grad * scale
                rest = y - y.astype(BF16).astype(F32)
                lines = jnp.where(pair == 0, y, jnp.where(pair == 1, rest, 0.0))
                z[size : size + 16, cols] = lines.astype(BF16)
            note(lane == s + RADIUS, sums, rel + tr, sum_ref, pair_ref)

        @pl.loop(0, half // 2)
        def per_two(k):
            gram(1)
            per_source(2 * k, 0)
            gram(0)
            per_source(2 * k + 1, 1)

    gram(1)


def assemble(near_sum, near_pair, far_sum, far_pair, gram_ref, matrix_ref, wide):
    size = 6 * WIN
    row = iota((8, L), 0)
    lane = iota((8, L), 1)
    i = lane & 7
    first = lane < 16

    def sides(near, far):
        return jnp.where(first, far, near), jnp.where(first, near, far)

    def expand(x):
        low, high = x
        mid = jnp.where(row < i, low, jnp.where(row > i, high, 0.0))
        start = jnp.where(row >= i, low, 0.0)
        end = jnp.where(row <= i, high, 0.0)
        return jnp.concatenate(
            [
                jnp.where(first, start, 0.0),
                jnp.where(first, mid, start),
                jnp.where(first, end, mid),
                jnp.where(first, 0.0, end),
            ],
            axis=0,
        )

    pose = [sides(near_pair[k], far_pair[k]) for k in range(12)]
    h = [[None] * 6 for _ in range(6)]
    wholes = [[None] * 6 for _ in range(6)]
    for n, (a, b) in enumerate(UPPER):
        pair = sides(near_sum[n], far_sum[n])
        h[a][b] = h[b][a] = pair if SIGNS[n] > 0 else tuple(-x for x in pair)
    count = len(UPPER)
    r = [tuple(-x for x in sides(near_sum[count + j], far_sum[count + j])) for j in range(6)]
    eye = iota((WIN, L), 0) == iota((WIN, L), 1)

    def total(terms):
        out = None
        for x, y in terms:
            if x is None or y is None:
                continue
            out = x * y if out is None else out + x * y
        return out

    had = [[[None, None] for _ in range(6)] for _ in range(6)]
    source = [[0.0] * 6 for _ in range(6)]
    lines = [0.0] * 6
    for side in range(2):
        rel = [pose[k][side] for k in range(9)]
        tr = [pose[9 + k][side] for k in range(3)]
        ad = [[None] * 6 for _ in range(6)]
        for c in range(3):
            corner = [
                tr[1] * rel[6 + c] - tr[2] * rel[3 + c],
                tr[2] * rel[c] - tr[0] * rel[6 + c],
                tr[0] * rel[3 + c] - tr[1] * rel[c],
            ]
            for a in range(3):
                ad[a][c] = ad[3 + a][3 + c] = rel[3 * a + c]
                ad[a][3 + c] = corner[a]
        for a in range(6):
            for b in range(6):
                had[a][b][side] = total(
                    [(None if h[a][k] is None else h[a][k][side], ad[k][b]) for k in range(6)]
                )
        for a in range(6):
            for b in range(6):
                source[a][b] = source[a][b] + total([(ad[k][a], had[k][b][side]) for k in range(6)])
        back = adj_t(rel, tr, [x[side] for x in r])
        lines = [x + y for x, y in zip(lines, back)]
    wide[...] = jnp.zeros_like(wide)
    matrix_ref[...] = jnp.zeros_like(matrix_ref)
    for a in range(6):
        rows = slice(a * WIN, (a + 1) * WIN)
        for b in range(6):
            cols = slice(b * WIN, (b + 1) * WIN)
            wide[rows, cols] = -expand(had[a][b])[:, :WIN]
            both = jnp.sum(source[a][b], axis=0, keepdims=True)
            if h[a][b] is not None:
                both = both + jnp.sum(expand(h[a][b]), axis=1, keepdims=True)
            matrix_ref[rows, cols] = jnp.where(eye, both, 0.0)[:, :WIN]
    high, low = gram_ref[:size, :], gram_ref[size + 16 :, :]
    wide[:size, :size] = wide[:size, :size] - low[:, :size]
    wide[:size, size : size + 1] = -(
        high[:, size : size + 1] + high[:, size + 1 : size + 2] + low[:, size : size + 1]
    )
    flipped = wide[...].T
    matrix_ref[:size, :size] = (
        matrix_ref[:size, :size] - high[:, :size] + wide[:size, :size] + flipped[:size, :size]
    )
    for j in range(6):
        cols = slice(j * WIN, (j + 1) * WIN)
        whole = jnp.sum(expand(r[j]), axis=1, keepdims=True)
        here = jnp.sum(jnp.where(eye, whole, 0.0), axis=0, keepdims=True)
        here = here - jnp.sum(lines[j], axis=0, keepdims=True)
        matrix_ref[size : size + 1, cols] = here[:, :WIN] + flipped[size : size + 1, cols]


def remote(src, dst, sems, phase, which, axis, peer):
    return pltpu.make_async_remote_copy(
        src_ref=src,
        dst_ref=dst,
        send_sem=sems.at[0, phase, which],
        recv_sem=sems.at[1, phase, which],
        device_id={axis: peer},
        device_id_type=pl.DeviceIdType.MESH,
    )


def peers(axis):
    count = lax.axis_size(axis)
    me = lax.axis_index(axis)
    return [lax.rem(me + step, count) for step in range(1, count)]


def pack(matrix_ref, packed_ref):
    size = 6 * WIN
    lane = iota((WIN, L), 1) % WIN
    row = iota((WIN, L), 0)
    inside = row + lane < WIN
    left = iota((BAND, L), 1) < L // 2
    packed_ref[...] = jnp.zeros_like(packed_ref)

    def skew(x):
        for bit in (1, 2, 4, 8, 16):
            x = jnp.where((lane & bit) != 0, pltpu.roll(x, WIN - bit, 0), x)
        return jnp.where(inside, x, 0.0)

    rest = []
    for j in range(6):
        rows = slice(j * WIN, (j + 1) * WIN)
        main = skew(matrix_ref[rows, :L])
        packed_ref[j * BAND : (j + 1) * BAND, :] = main[:BAND]
        packed_ref[6 * BAND + j : 6 * BAND + j + 1, :] = main[BAND : BAND + 1]
        rest.append(skew(matrix_ref[rows, L:]))
    base = 6 * BAND + 8
    for j in range(3):
        near = rest[j]
        far = pltpu.roll(rest[j + 3], L // 2, 1)
        packed_ref[base + j * BAND : base + (j + 1) * BAND, :] = jnp.where(left, near[:BAND], far[:BAND])
        at = base + 3 * BAND + j
        packed_ref[at : at + 1, :] = jnp.where(left[:1], near[BAND : BAND + 1], far[BAND : BAND + 1])
    packed_ref[6 * BAND + 6 : 6 * BAND + 7, :] = matrix_ref[size : size + 1, :L]
    packed_ref[base + 3 * BAND + 3 : base + 3 * BAND + 4, :] = jnp.where(
        left[:1], matrix_ref[size : size + 1, L:], 0.0
    )


def exchange(src, dst, sems, phase, axis):
    sent = []
    for peer in peers(axis):
        copy = remote(src(peer), dst, sems, phase, len(sent), axis, peer)
        copy.start()
        sent.append(copy)
    return sent


def operator(packed_ref, land, reduced_ref, gathered, diag_ref, ahead_ref, back_ref, far_ref, pix_sem, round_sem, mate_sem, f_dev, frames):
    zcount = lax.axis_size("pix")
    z = lax.axis_index("pix")
    count = lax.axis_size("frames")
    me = lax.axis_index("frames")
    chunk = land.shape[1]
    tiles = frames // L

    def piece(which):
        return pl.ds(pl.multiple_of(which * chunk, 8), chunk)

    sent = exchange(lambda peer: packed_ref.at[piece(peer)], land.at[z], pix_sem, 0, "pix")
    land[z] = packed_ref[piece(z), :]
    for copy in sent:
        copy.wait_recv()
    total = land[0]
    for k in range(1, zcount):
        total = total + land[k]
    reduced_ref[...] = total
    more = exchange(lambda peer: reduced_ref, gathered.at[me], round_sem, 0, "frames")
    gathered[me] = total
    for copy in more:
        copy.wait_recv()
    lane = iota((chunk, L), 1)
    sums = [[None] * tiles for _ in range(4)]
    for w in range(count):
        first = (w * f_dev - RADIUS) % frames
        start = first % L
        for k in range(4):
            part = pltpu.roll(gathered[w], (start - WIN * k) % L, 1)
            spans = [(first // L, start, min(start + WIN, L))]
            if start + WIN > L:
                spans.append(((first // L + 1) % tiles, 0, start + WIN - L))
            for tile, low, high in spans:
                term = jnp.where((lane >= low) & (lane < high), part, 0.0)
                sums[k][tile] = term if sums[k][tile] is None else sums[k][tile] + term
    for k in range(4):
        for tile in range(tiles):
            diag_ref[z, k, :, tile * L : (tile + 1) * L] = sums[k][tile]
    pending = sent + more
    mate = me + 1 - 2 * lax.rem(me, 2)
    mine = pl.ds(2 * lax.rem(me, 2), 2)
    half = diag_ref.at[z, mine]
    sent = exchange(lambda peer: half, half, pix_sem, 1, "pix")
    passed = []
    for n, (copy, step) in enumerate(zip(sent, range(zcount - 1, 0, -1))):
        copy.wait_recv()
        there = diag_ref.at[lax.rem(z + step, zcount), mine]
        handed = remote(there, there, mate_sem, 0, n, "frames", mate)
        handed.start()
        passed.append(handed)
    for copy in passed:
        copy.wait_recv()
    pending = pending + sent + passed

    def block(k, at):
        return [
            diag_ref[at // chunk, k, at % chunk : at % chunk + 8, t * L : (t + 1) * L]
            for t in range(tiles)
        ]

    def entry(i, j, half):
        if i < 4:
            return block(i, BAND * j + 8 * half)
        return block(i - 4 + 2 * (j // 3), 6 * BAND + 8 + BAND * (j % 3) + 8 * half)

    row = iota((8, L), 0)
    lanes = iota((8, L), 1)

    def later(x, half):
        turned = [pltpu.roll(v, 8 * half, 1, stride=1, stride_axis=0) for v in x]
        if tiles == 1:
            return turned
        mine = lanes >= 8 * half + row
        return [jnp.where(mine, turned[t], turned[t - 1]) for t in range(tiles)]

    def flip(x):
        for bit in (4, 2, 1):
            x = jnp.where((row & bit) != 0, pltpu.roll(x, bit, 0), pltpu.roll(x, 8 - bit, 0))
        return x

    for i in range(6):
        for j in range(6):
            for half in range(2):
                front = entry(i, j, half)
                moved = later(entry(j, i, half), half)
                for t in range(tiles):
                    ahead_ref[i, 2 * j + half, :, t * L : (t + 1) * L] = flip(front[t])
                    value = jnp.where(row > 0, moved[t], 0.0) if half == 0 else moved[t]
                    back_ref[i, 2 * j + half, :, t * L : (t + 1) * L] = value
    edge = 6 * BAND
    last = edge + 8 + 3 * BAND
    for i in range(6):
        if i < 4:
            ends = block(i, edge)
        else:
            near, far = block(i - 4, last), block(i - 2, last)
            ends = [jnp.where(row < 3, a, pltpu.roll(b, 3, 0)) for a, b in zip(near, far)]
        for t in range(tiles):
            far_ref[i, :, t * L : (t + 1) * L] = jnp.where(row < 6, ends[t], 0.0)
    sources = [block(k, edge) for k in range(4)] + [block(k, last) for k in range(2)]
    rhs = []
    for t in range(tiles):
        out = jnp.zeros((8, L), F32)
        for i in range(6):
            at = 6 if i < 4 else 3
            out = jnp.where(row == i, sources[i][t][at : at + 1, :], out)
        rhs.append(out)
    return rhs, later, pending


def conjugate(rhs, later, ahead_ref, back_ref, far_ref):
    tiles = len(rhs)
    row = iota((8, L), 0)
    lanes = iota((8, L), 1)

    def sooner(x, half):
        turned = [pltpu.roll(v, L - 8 * half - 7, 1, stride=1, stride_axis=0) for v in x]
        if tiles == 1:
            return turned
        mine = lanes + 8 * half + 7 - row < L
        return [jnp.where(mine, turned[t], turned[(t + 1) % tiles]) for t in range(tiles)]

    def moved(x, steps):
        turned = [pltpu.roll(v, steps % L, 1) for v in x]
        if tiles == 1:
            return turned
        if steps > 0:
            return [jnp.where(lanes >= steps, turned[t], turned[t - 1]) for t in range(tiles)]
        return [jnp.where(lanes < L + steps, turned[t], turned[(t + 1) % tiles]) for t in range(tiles)]

    def dot(x, y):
        total = x[0] * y[0]
        for t in range(1, tiles):
            total = total + x[t] * y[t]
        return jnp.sum(total, keepdims=True)

    def product(p):
        ahead = moved(p, -BAND)
        acc = [[far_ref[i, :, t * L : (t + 1) * L] * ahead[t] for t in range(tiles)] for i in range(6)]
        tail = [None] * tiles
        for j in range(6):
            wide = [jnp.broadcast_to(v[j : j + 1, :], (8, L)) for v in p]
            for t in range(tiles):
                term = far_ref[j, :, t * L : (t + 1) * L] * wide[t]
                tail[t] = term if tail[t] is None else tail[t] + term
            for half in range(2):
                plus = sooner(wide, half)
                minus = later(wide, half)
                for i in range(6):
                    for t in range(tiles):
                        acc[i][t] = (
                            acc[i][t]
                            + ahead_ref[i, 2 * j + half, :, t * L : (t + 1) * L] * plus[t]
                            + back_ref[i, 2 * j + half, :, t * L : (t + 1) * L] * minus[t]
                        )
        tail = moved(tail, BAND)
        out = []
        for t in range(tiles):
            y = tail[t] + REG * p[t]
            for i in range(6):
                y = y + jnp.where(row == i, jnp.sum(acc[i][t], axis=0, keepdims=True), 0.0)
            out.append(y)
        return out

    def step(_, carry):
        x, residual, direction, rr = carry
        image = product(direction)
        alpha = rr / dot(direction, image)
        x = [a + alpha * b for a, b in zip(x, direction)]
        residual = [a - alpha * b for a, b in zip(residual, image)]
        new = dot(residual, residual)
        beta = new / rr
        direction = [a + beta * b for a, b in zip(residual, direction)]
        return x, residual, direction, new

    zero = [jnp.zeros((8, L), F32)] * tiles
    return lax.fori_loop(0, ITERS, step, (zero, rhs, rhs, dot(rhs, rhs)))[0]


def finish(
    matrix_ref, e_ref, base_ref, inv_ref, pose_ref, step_ref, frames,
    cols_ref, step3, packed_ref, land, reduced_ref, gathered, diag_ref, ahead_ref, back_ref, far_ref, x_ref,
    pix_sem, round_sem, mate_sem,
):
    me = lax.axis_index("frames")
    tiles, f_dev = step3.shape[:2]
    half = f_dev // 2
    pack(matrix_ref, packed_ref)
    rhs, later, pending = operator(
        packed_ref, land, reduced_ref, gathered, diag_ref, ahead_ref, back_ref, far_ref,
        pix_sem, round_sem, mate_sem, f_dev, frames,
    )
    x = conjugate(rhs, later, ahead_ref, back_ref, far_ref)
    for t, value in enumerate(x):
        x_ref[:, t * L : (t + 1) * L] = value
    mine = window(lambda at: x_ref[:, at], me, f_dev, frames)
    pose_ref[...] = mine[:6, RADIUS : RADIUS + f_dev]
    turned = spread_rows(mine)
    for i in range(6):
        cols_ref[i] = jnp.broadcast_to(turned[:WIN, i : i + 1], (WIN, L))
    row = iota((8, L), 0)
    lane = iota((8, L), 1)
    for part in range(2):

        @pl.loop(0, half)
        def per_source(i):
            s = i + part * half
            group = [[cols_ref[j, 8 * g : 8 * g + 8, :] for g in range(part, part + 3)] for j in range(6)]
            below = [jnp.where(row >= i, group[j][0], group[j][1]) for j in range(6)]
            over = [jnp.where(row > i, group[j][1], group[j][2]) for j in range(6)]
            near, far = (over, below) if part == 0 else (below, over)
            at = jnp.sum(jnp.where(lane == s + RADIUS, mine, 0.0), axis=1, keepdims=True)
            terms = near + far + [jnp.broadcast_to(at, (8, L))]
            for tile in range(tiles):
                slot = s * tiles + tile
                image = e_ref[slot, 0] * terms[0]
                for n in range(1, 13):
                    image = image + e_ref[slot, n] * terms[n]
                image = jnp.sum(image, axis=0, keepdims=True)
                here = (tile, pl.ds(s, 1), slice(None))
                step3[here] = base_ref[here] - inv_ref[here] * image

    for tile in range(tiles):
        step_ref[:, tile * L : (tile + 1) * L] = step3[tile]
    for copy in pending:
        copy.wait_send()


def swap_edges(low_out, high_out, low_ref, high_ref, sems):
    count = lax.axis_size("frames")
    me = lax.axis_index("frames")
    below = lax.rem(me + count - 1, count)
    over = lax.rem(me + 1, count)
    tiles = low_out.shape[0]
    down = [remote(low_out.at[t, :, :SENT], low_ref.at[t, :, :SENT], sems, 0, t, "frames", below) for t in range(tiles)]
    up = [remote(high_out.at[t, :, :SENT], high_ref.at[t, :, :SENT], sems, 1, t, "frames", over) for t in range(tiles)]

    def ascend(span):
        @pl.when(me < count - 1)
        def _():
            for t in span:
                up[t].start()

    def descend():
        @pl.when(me > 0)
        def _():
            for copy in down:
                copy.start()

    def receive(part):
        if part == 0:

            @pl.when(me > 0)
            def _():
                for copy in up:
                    copy.wait_recv()

            @pl.when(me == 0)
            def _():
                high_ref[...] = jnp.zeros_like(high_ref)

        else:

            @pl.when(me < count - 1)
            def _():
                for copy in down:
                    copy.wait_recv()

            @pl.when(me == count - 1)
            def _():
                low_ref[...] = jnp.zeros_like(low_ref)

    def drain():
        @pl.when(me > 0)
        def _():
            for copy in down:
                copy.wait_send()

        @pl.when(me < count - 1)
        def _():
            for copy in up:
                copy.wait_send()

    return ascend, descend, receive, drain


def solve(
    edge_ref, rot_ref, trans_ref, depth_ref, damp_ref, flow_ref, weight_ref, mask_ref,
    x_ref, step_ref, flow3, weight3, mask3, load_sem, pose_ref,
    own_ref, low_out, high_out, low_ref, high_ref, edge_sem,
    frame_ref, coord_ref, depth3, damp3, e_ref, part_ref, near_sum, near_pair, far_sum, far_pair,
    base_ref, inv_ref, z0, z1, gram_ref, matrix_ref, wide, *scratch,
):
    me = lax.axis_index("frames")
    f_dev, pix = depth_ref.shape
    frames = rot_ref.shape[1]
    loads = fetch(flow_ref, weight_ref, mask_ref, flow3, weight3, mask3, load_sem)
    barrier = pltpu.get_barrier_semaphore()
    total = 0
    for axis in ("frames", "pix"):
        for peer in peers(axis):
            pl.semaphore_signal(
                barrier, inc=1, device_id={axis: peer}, device_id_type=pl.DeviceIdType.MESH
            )
            total += 1
    poses = []
    for ref in (rot_ref, trans_ref):
        poses.append(window(lambda at: ref[:, at], me, f_dev, frames))
    turned = spread_rows(jnp.concatenate(poses, axis=0))
    for k in range(6):
        pose_ref[k] = jnp.broadcast_to(turned[:WIN, k : k + 1], (WIN, L))
    prepare(pose_ref, frame_ref, coord_ref, depth_ref, damp_ref, depth3, damp3)
    ascend, descend, receive, drain = swap_edges(low_out, high_out, low_ref, high_ref, edge_sem)

    def ready(span):
        if span[0] == 0:
            pl.semaphore_wait(barrier, total)
        ascend(span)

    aggregate(edge_ref, loads, flow3, weight3, mask3, own_ref, low_out, high_out, me, f_dev, ready)
    near_pairs(own_ref, frame_ref, coord_ref, depth3, e_ref, part_ref, near_sum, near_pair, descend)
    far_pairs(
        own_ref, low_ref, high_ref, frame_ref, coord_ref, depth3, damp3, e_ref, part_ref,
        far_sum, far_pair, base_ref, inv_ref, (z0, z1), gram_ref, receive,
    )
    assemble(near_sum, near_pair, far_sum, far_pair, gram_ref, matrix_ref, wide)
    finish(matrix_ref, e_ref, base_ref, inv_ref, x_ref, step_ref, frames, *scratch)
    drain()


def call(body, out, scratch, vmem, hbm, **params):
    vm = pl.BlockSpec(memory_space=pltpu.VMEM)
    far = pl.BlockSpec(memory_space=pl.ANY)
    return pl.pallas_call(
        body,
        out_shape=[pltpu.VMEM(s, t) for s, t in out],
        in_specs=[vm] * vmem + [far] * hbm,
        out_specs=[vm] * len(out),
        scratch_shapes=scratch,
        compiler_params=pltpu.CompilerParams(vmem_limit_bytes=VMEM_LIMIT, **params),
    )


def per_device(edge_frames, rotvec, trans, inv_depth, depth_damping, flow, weight, mask):
    f_dev, pix = inv_depth.shape
    edges = mask.shape[0]
    frames = rotvec.shape[1]
    tiles = pix // L
    own_rows = f_dev * 16
    side = 40
    sums = len(UPPER) + 6
    width = 256
    size = 6 * WIN
    count = lax.axis_size("frames")
    zcount = lax.axis_size("pix")
    chunk = -(-PACKED // (8 * zcount)) * 8
    x, step = call(
        solve,
        [((6, f_dev), F32), ((f_dev, pix), F32)],
        [
            pltpu.VMEM((tiles, 2, edges, L), F32),
            pltpu.VMEM((tiles, 2, edges, L), F32),
            pltpu.VMEM((tiles, edges, L), jnp.int32),
            pltpu.SemaphoreType.DMA((tiles, 5)),
            pltpu.VMEM((6, WIN, L), F32),
            pltpu.VMEM((4, own_rows, pix), F32),
            pltpu.VMEM((tiles, 4, side, L), F32),
            pltpu.VMEM((tiles, 4, side, L), F32),
            pltpu.VMEM((tiles, 4, side, L), F32),
            pltpu.VMEM((tiles, 4, side, L), F32),
            pltpu.SemaphoreType.DMA((2, 2, tiles)),
            pltpu.VMEM((12, WIN, L), F32),
            pltpu.VMEM((tiles, 2, 8, L), F32),
            pltpu.VMEM((tiles, f_dev, L), F32),
            pltpu.VMEM((tiles, f_dev, L), F32),
            pltpu.VMEM((f_dev * tiles, 13, 8, L), F32),
            pltpu.VMEM((f_dev * tiles, 8, 8, L), F32),
            pltpu.VMEM((sums, 8, L), F32),
            pltpu.VMEM((12, 8, L), F32),
            pltpu.VMEM((sums, 8, L), F32),
            pltpu.VMEM((12, 8, L), F32),
            pltpu.VMEM((tiles, f_dev, L), F32),
            pltpu.VMEM((tiles, f_dev, L), F32),
            pltpu.VMEM((2 * size + 16, pix), BF16),
            pltpu.VMEM((2 * size + 16, pix), BF16),
            pltpu.VMEM((2 * size + 16, size + 16), F32),
            pltpu.VMEM((size + 8, width), F32),
            pltpu.VMEM((256, 256), F32),
            pltpu.VMEM((6, WIN, L), F32),
            pltpu.VMEM((tiles, f_dev, L), F32),
            pltpu.VMEM((chunk * zcount, L), F32),
            pltpu.VMEM((zcount, chunk, L), F32),
            pltpu.VMEM((chunk, L), F32),
            pltpu.VMEM((count, chunk, L), F32),
            pltpu.VMEM((zcount, 4, chunk, frames), F32),
            pltpu.VMEM((6, 12, 8, frames), F32),
            pltpu.VMEM((6, 12, 8, frames), F32),
            pltpu.VMEM((6, 8, frames), F32),
            pltpu.VMEM((8, frames), F32),
            pltpu.SemaphoreType.DMA((2, 2, zcount)),
            pltpu.SemaphoreType.DMA((2, 1, count)),
            pltpu.SemaphoreType.DMA((2, 1, zcount)),
        ],
        5, 3, collective_id=0, has_side_effects=True,
    )(edge_frames, rotvec, trans, inv_depth, depth_damping, flow, weight, mask)
    return x, step


def solution(mesh):
    return jax.shard_map(
        per_device,
        mesh=mesh,
        in_specs=(
            P(None, "frames"),
            P(),
            P(),
            P("frames", "pix"),
            P("frames", "pix"),
            P("frames", None, "pix"),
            P("frames", None, "pix"),
            P("frames", "pix"),
        ),
        out_specs=(P(None, "frames"), P("frames", "pix")),
        check_vma=False,
    )
```
